32 devices in a mesh: dp: 32 (over z, y, x, core).
Axes of the slice: x: 2, y: 2, z: 4, core: 2. Of those that a mesh axis runs over, the one named last changes fastest.
Arguments:
- features: bfloat16 [64, 256, 256], P('dp'), may hold values from -6 to 6
- frame_lens: int32 [64], P('dp'), may hold values from 128 to 256
- labels: int32 [64, 48], P('dp'), may hold values from 1 to 255
- label_lens: int32 [64], P('dp'), may hold values from 1 to 48
- w_up: float32 [262144], P('dp'), may hold values from -0.375 to 0.375
- w_down: float32 [262144], P('dp'), may hold values from -0.1875 to 0.1875
- w_out: float32 [65536], P('dp'), may hold values from -1.125 to 1.125
- first_up: float32 [262144], P('dp'), may hold values from -0.00018 to 0.00018
- first_down: float32 [262144], P('dp'), may hold values from -0.00018 to 0.00018
- first_out: float32 [65536], P('dp'), may hold values from -0.00018 to 0.00018
- second_up: float32 [262144], P('dp'), may hold values from 1e-10 to 1e-08
- second_down: float32 [262144], P('dp'), may hold values from 1e-10 to 1e-08
- second_out: float32 [65536], P('dp'), may hold values from 1e-10 to 1e-08
Outputs:
- new_up: float32 [262144], P('dp')
- new_down: float32 [262144], P('dp')
- new_out: float32 [65536], P('dp')
- new_first_up: float32 [262144], P('dp')
- new_first_down: float32 [262144], P('dp')
- new_first_out: float32 [65536], P('dp')
- new_second_up: float32 [262144], P('dp')
- new_second_down: float32 [262144], P('dp')
- new_second_out: float32 [65536], P('dp')
The draws below stay inside these ranges and needn't reach their ends.
Inputs may be any that keep to these rules, and one draw needn't show every extreme that they name: `labels`: 0 is the blank and is not a label.
All inputs are finite; a program needn't handle non-finite values.
Results may differ from the reference program's by a relative error of at most 0.002.
The reference program's roundings to bfloat16 on the way (of `normalized`, `hidden`, `block_out`, `logit_grad`, `ff_grad` and `act_grad`) count: a program that leaves them out, or rounds other values in their place, can miss the bound.
Values may be sent and summed in bfloat16 or wider, within the bound.
A program may use at most 64 MiB of HBM per device.

```python
import math
import jax
import jax.numpy as jnp
from jax import lax

D = 256
FF = 1024
VOCAB = 256
UTT = 2
FRAMES = 256
LABELS = 48
UTTERANCES = 64
N_DP = 32


def set_ends(result, rng, smallest, largest):
    longest = result.shape.index(max(result.shape))
    spots = []
    for shift in (0, 1):
        where = [jax.random.randint(jax.random.fold_in(rng, axis), (), 0, length) for axis, length in enumerate(result.shape)]
        where[longest] = (where[longest] + shift) % result.shape[longest]
        spots.append(tuple(where))
    return result.at[spots[0]].set(smallest).at[spots[1]].set(largest)


def shard_levels(rng, shape, cuts, smallest, top_value):
    def one(axis_at, blocks):
        heights = jax.random.uniform(jax.random.fold_in(jax.random.fold_in(rng, 6), axis_at), (blocks,), jnp.float32, smallest / len(cuts), top_value / len(cuts))
        return jnp.repeat(jnp.exp(heights), shape[axis_at] // blocks).reshape((-1,) + (1,) * (len(shape) - axis_at - 1))

    gain = one(*cuts[0])
    for cut in cuts[1:]:
        gain = gain * one(*cut)
    return gain


def gaussian(own_key, dims, deviation, reach, pieces=(), kind=jnp.bfloat16):
    values = jax.random.normal(own_key, dims, jnp.float32) * deviation
    if len(pieces) > 0:
        values = shard_levels(own_key, dims, pieces, -0.22, 0.18) * values
    return jnp.clip(values, min=-reach, max=reach).astype(kind)


def setup_inputs(seed: int = 0) -> dict:
    key_list = jax.random.split(jax.random.key(seed), 14)
    return {
        "features": gaussian(key_list[0], (UTTERANCES, FRAMES, D), 1.0, 6.0, ((0, 32),)),
        "frame_lens": set_ends(jax.random.randint(key_list[1], (UTTERANCES,), FRAMES // 2, FRAMES + 1), jax.random.fold_in(key_list[1], 1), FRAMES // 2, FRAMES).astype(jnp.int32),
        "labels": set_ends(jax.random.randint(key_list[2], (UTTERANCES, LABELS), 1, VOCAB), jax.random.fold_in(key_list[2], 1), 1, VOCAB - 1).astype(jnp.int32),
        "label_lens": set_ends(jax.random.randint(key_list[3], (UTTERANCES,), 1, LABELS + 1), jax.random.fold_in(key_list[3], 1), 1, LABELS).astype(jnp.int32),
        "w_up": gaussian(key_list[4], (D * FF,), D ** -0.5, 0.375, ((0, 32),), jnp.float32),
        "w_down": gaussian(key_list[5], (FF * D,), FF ** -0.5, 0.1875, ((0, 32),), jnp.float32),
        "w_out": gaussian(key_list[6], (D * VOCAB,), (3.0 / D ** 0.5), 1.125, ((0, 32),), jnp.float32),
        "first_up": gaussian(key_list[7], (D * FF,), (3e-5), 0.00018, ((0, 32),), jnp.float32),
        "first_down": gaussian(key_list[8], (FF * D,), (3e-5), 0.00018, ((0, 32),), jnp.float32),
        "first_out": gaussian(key_list[9], (D * VOCAB,), (3e-5), 0.00018, ((0, 32),), jnp.float32),
        "second_up": jnp.clip(jnp.exp(math.log(9.99999993922529e-09) - 4.6051702 * jax.random.uniform(key_list[10], (D * FF,), jnp.float32) ** shard_levels(key_list[10], (D * FF,), ((0, 32),), -0.2, 0.2)), 1.000000013351432e-10, 9.99999993922529e-09),
        "second_down": jnp.clip(jnp.exp(math.log(9.99999993922529e-09) - 4.6051702 * jax.random.uniform(key_list[11], (FF * D,), jnp.float32) ** shard_levels(key_list[11], (FF * D,), ((0, 32),), -0.2, 0.2)), 1.000000013351432e-10, 9.99999993922529e-09),
        "second_out": jnp.clip(jnp.exp(math.log(9.99999993922529e-09) - 4.6051702 * jax.random.uniform(key_list[12], (D * VOCAB,), jnp.float32) ** shard_levels(key_list[12], (D * VOCAB,), ((0, 32),), -0.2, 0.2)), 1.000000013351432e-10, 9.99999993922529e-09),
    }


first_correction = 1.0 - (0.9 ** 10) ** 10
second_correction = 1.0 - (0.999 ** 10) ** 10

def ctc_losses(log_probs, labels, frame_lens, label_lens):
    batch, frames, vocab = log_probs.shape
    label_count = labels.shape[1]
    states = 2 * label_count + 1
    blanks = jnp.zeros_like(labels)
    extended = jnp.concatenate([jnp.stack([blanks, labels], axis=2).reshape(batch, 2 * label_count), blanks[:, :1]], axis=1)
    earlier = jnp.concatenate([jnp.full((batch, 2), -1, jnp.int32), extended[:, :-2]], axis=1)
    may_skip = (extended != 0) & (extended != earlier)
    onehot = (extended[:, :, None] == jnp.arange(vocab, dtype=jnp.int32)[None, None, :]).astype(log_probs.dtype)
    emitted = jnp.einsum('btv,bsv->tbs', log_probs, onehot, precision=lax.Precision.HIGHEST)
    state_ids = jnp.arange(states, dtype=jnp.int32)
    start = jnp.where(state_ids[None, :] < 2, emitted[0], -1e+30)
    frame_ids = jnp.arange(1, frames, dtype=jnp.int32)

    def advance(alpha, inputs):
        emit_row, frame_id = inputs
        lowest = jnp.full((batch, 1), -1e+30, alpha.dtype)
        from_one = jnp.concatenate([lowest, alpha[:, :-1]], axis=1)
        from_two = jnp.concatenate([lowest, lowest, alpha[:, :-2]], axis=1)
        from_two = jnp.where(may_skip, from_two, -1e+30)
        merged = jnp.logaddexp(jnp.logaddexp(alpha, from_one), from_two) + emit_row
        alive = frame_id < frame_lens[:, None]
        return (jnp.where(alive, merged, alpha), None)
    alpha, _ = lax.scan(advance, start, (emitted[1:], frame_ids))
    last_state = 2 * label_lens
    pick_end = lax.optimization_barrier(jnp.sum(jnp.where(state_ids[None, :] == last_state[:, None], alpha, 0.0), axis=1))
    pick_label = lax.optimization_barrier(jnp.sum(jnp.where(state_ids[None, :] == last_state[:, None] - 1, alpha, 0.0), axis=1))
    return -jnp.logaddexp(pick_end, pick_label)

def shard_gradients(features, frame_lens, labels, label_lens, up_mat, down_mat, out_mat, loss_scale):
    batch, frames, width = features.shape
    vocab = out_mat.shape[1]
    flat_in = features.reshape(batch * frames, width).astype(jnp.float32)
    centre = lax.optimization_barrier(jnp.mean(flat_in, axis=1, keepdims=True))
    spread = lax.optimization_barrier(jnp.mean((flat_in - centre) ** 2, axis=1, keepdims=True))
    normalized = ((flat_in - centre) * lax.rsqrt(spread + 1e-05)).astype(jnp.bfloat16)
    activation = jnp.dot(normalized, up_mat, preferred_element_type=jnp.float32)
    hidden = jax.nn.silu(activation).astype(jnp.bfloat16)
    block_out = (flat_in + 0.5 * jnp.dot(hidden, down_mat, preferred_element_type=jnp.float32)).astype(jnp.bfloat16)
    logits = jnp.dot(block_out, out_mat, preferred_element_type=jnp.float32)

    def loss_of(logit_rows):
        log_probs = jax.nn.log_softmax(logit_rows.reshape(batch, frames, vocab), axis=-1)
        return loss_scale * jnp.sum(ctc_losses(log_probs, labels, frame_lens, label_lens))
    loss_value, pullback = jax.vjp(loss_of, logits)
    logit_grad = pullback(jnp.ones((), loss_value.dtype))[0].astype(jnp.bfloat16)
    grad_out = jnp.dot(block_out.T, logit_grad, preferred_element_type=jnp.float32)
    ff_grad = (0.5 * jnp.dot(logit_grad, out_mat.T, preferred_element_type=jnp.float32)).astype(jnp.bfloat16)
    grad_down = jnp.dot(hidden.T, ff_grad, preferred_element_type=jnp.float32)
    sigmoid = jax.nn.sigmoid(activation)
    slope = sigmoid * (1.0 + activation * (1.0 - sigmoid))
    act_grad = (jnp.dot(ff_grad, down_mat.T, preferred_element_type=jnp.float32) * slope).astype(jnp.bfloat16)
    grad_up = jnp.dot(normalized.T, act_grad, preferred_element_type=jnp.float32)
    return (grad_up, grad_down, grad_out)

def adam_update(weight, first, second, grad, clip):
    scaled = clip * grad
    new_first = 0.9 * first + 0.1 * scaled
    new_second = 0.999 * second + 0.001 * scaled * scaled
    ratio = new_first / first_correction / (jnp.sqrt(new_second / second_correction) + 1e-08)
    return (weight - 0.001 * ratio, new_first, new_second)

def reference(features, frame_lens, labels, label_lens, w_up, w_down, w_out, first_up, first_down, first_out, second_up, second_down, second_out):
    up_mat = w_up.astype(jnp.bfloat16).reshape(D, FF)
    down_mat = w_down.astype(jnp.bfloat16).reshape(FF, D)
    out_mat = w_out.astype(jnp.bfloat16).reshape(D, VOCAB)
    loss_scale = 1.0 / (UTT * N_DP)
    shards = (features.reshape(N_DP, UTT, FRAMES, D), frame_lens.reshape(N_DP, UTT), labels.reshape(N_DP, UTT, LABELS), label_lens.reshape(N_DP, UTT))

    def accumulate(carry, item):
        terms = shard_gradients(item[0], item[1], item[2], item[3], up_mat, down_mat, out_mat, loss_scale)
        return ((carry[0] + terms[0], carry[1] + terms[1], carry[2] + terms[2]), None)
    start = (jnp.zeros((D, FF), jnp.float32), jnp.zeros((FF, D), jnp.float32), jnp.zeros((D, VOCAB), jnp.float32))
    sums, _ = lax.scan(accumulate, start, shards)
    grad_up = sums[0].reshape(-1)
    grad_down = sums[1].reshape(-1)
    grad_out = sums[2].reshape(-1)
    total = jnp.sum(grad_up * grad_up) + jnp.sum(grad_down * grad_down) + jnp.sum(grad_out * grad_out)
    clip = 1.0 / jnp.maximum(jnp.sqrt(total), 1.0)
    new_up, new_first_up, new_second_up = adam_update(w_up, first_up, second_up, grad_up, clip)
    new_down, new_first_down, new_second_down = adam_update(w_down, first_down, second_down, grad_down, clip)
    new_out, new_first_out, new_second_out = adam_update(w_out, first_out, second_out, grad_out, clip)
    return (new_up, new_down, new_out, new_first_up, new_first_down, new_first_out, new_second_up, new_second_down, new_second_out)
```

```python
import functools

import jax
import jax.numpy as jnp
from jax import lax
from jax.experimental import pallas as pl
from jax.experimental.pallas import tpu as pltpu
from jax.sharding import PartitionSpec as P

D = 256
FF = 1024
VOCAB = 256
LANES = 128
MESH = pl.DeviceIdType.MESH

first_correction = 1.0 - (0.9**10) ** 10
second_correction = 1.0 - (0.999**10) ** 10
negative = -1e30
VMEM = pl.BlockSpec(memory_space=pltpu.VMEM)
SMEM = pl.BlockSpec(memory_space=pltpu.SMEM)
HBM = pl.BlockSpec(memory_space=pltpu.HBM)


def flip(me, bit):
    return me + bit - 2 * bit * ((me // bit) % 2)


def bit_orders(devices):
    bits = [1 << k for k in range(devices.bit_length() - 1)]
    core, rest = bits[:1], bits[1:]
    down = rest[::-1]
    swapped = down[:-2] + down[-2:][::-1]
    turned = down[-2:] + down[:-2]
    return (down + core, swapped + core, turned + core)


def subsets(bits):
    offsets = [0]
    for bit in bits:
        offsets = offsets + [offset + bit for offset in offsets]
    return offsets


def place_with(me, free, pattern):
    place = me
    for bit in free:
        if pattern & bit:
            place = flip(place, bit)
    return place


class Gather:
    def __init__(self, me, devices, fulls, send_sem, recv_sem):
        self.me, self.fulls = me, fulls
        self.send_sem, self.recv_sem = send_sem, recv_sem
        self.orders = bit_orders(devices)
        self.steps = len(self.orders[0])
        self.copies = [{}, {}, {}]

    def fill(self, shards):
        for shard, full in zip(shards, self.fulls):
            rows, width = full.shape[1:]
            parts = width // LANES
            for part in range(parts):
                full[self.me, :, part * LANES : (part + 1) * LANES] = shard[
                    pl.ds(part, rows, stride=parts), :
                ].astype(jnp.bfloat16)

    def send(self, which, pattern, stage):
        order, full = self.orders[which], self.fulls[which]
        owner = place_with(self.me, order[:stage], pattern)
        slot = pattern + order[stage]
        copy = pltpu.make_async_remote_copy(
            src_ref=full.at[owner],
            dst_ref=full.at[owner],
            send_sem=self.send_sem.at[which, slot],
            recv_sem=self.recv_sem.at[which, slot],
            device_id=(flip(self.me, order[stage]),),
            device_id_type=MESH,
        )
        copy.start()
        self.copies[which][slot] = copy

    def pass_on(self):
        for which in range(3):
            for stage in range(self.steps):
                self.send(which, 0, stage)
        for stage in range(self.steps - 1):
            for at in range(1 << stage):
                for which in range(3):
                    order = self.orders[which]
                    pattern = subsets(order[:stage])[at] + order[stage]
                    self.copies[which][pattern].wait_recv()
                    for later in range(stage + 1, self.steps):
                        self.send(which, pattern, later)

    def arrive(self, which):
        order = self.orders[which]
        for pattern in subsets(order[:-1]):
            self.copies[which][pattern + order[-1]].wait_recv()

    def close(self):
        for copies in self.copies:
            for copy in copies.values():
                copy.wait_send()


def drain(ref, blocks, send_sem, recv_sem, peer):
    return pltpu.make_async_remote_copy(
        src_ref=ref.at[pl.ds(0, blocks)],
        dst_ref=ref.at[pl.ds(0, blocks)],
        send_sem=send_sem,
        recv_sem=recv_sem,
        device_id=(peer,),
        device_id_type=MESH,
    )


class GroupGather:
    def __init__(self, me, devices, fulls, send_sem, recv_sem):
        self.me, self.devices, self.fulls = me, devices, fulls
        self.send_sem, self.recv_sem = send_sem, recv_sem
        self.orders = bit_orders(devices)
        self.steps = len(self.orders[0])

    def fill(self, shards):
        for shard, full in zip(shards, self.fulls):
            rows, width = full.shape[1:]
            parts = width // LANES
            for part in range(parts):
                full[self.me, :, part * LANES : (part + 1) * LANES] = shard[
                    pl.ds(part, rows, stride=parts), :
                ].astype(jnp.bfloat16)

    def sem_at(self, stage, group):
        return stage * (stage + 1) // 2 + (group if stage < self.steps - 1 else 0)

    def send(self, which, patterns, stage, group):
        order, full = self.orders[which], self.fulls[which]
        for pattern in patterns:
            owner = place_with(self.me, order[:stage], pattern)
            pltpu.make_async_remote_copy(
                src_ref=full.at[owner],
                dst_ref=full.at[owner],
                send_sem=self.send_sem.at[which],
                recv_sem=self.recv_sem.at[which, self.sem_at(stage, group)],
                device_id=(flip(self.me, order[stage]),),
                device_id_type=MESH,
            ).start()

    def drain(self, which, blocks, at):
        return drain(
            self.fulls[which], blocks, self.send_sem.at[which], self.recv_sem.at[which, at],
            flip(self.me, 1),
        )

    def pass_on(self):
        for which in range(3):
            for stage in range(self.steps):
                self.send(which, [0], stage, 0)
        for stage in range(self.steps - 1):
            for group in range(stage + 1):
                for which in range(3):
                    order = self.orders[which]
                    patterns = [0]
                    if group:
                        patterns = [at + order[group - 1] for at in subsets(order[: group - 1])]
                    self.drain(which, len(patterns), self.sem_at(stage, group)).wait_recv()
                    patterns = [pattern + order[stage] for pattern in patterns]
                    for later in range(stage + 1, self.steps):
                        self.send(which, patterns, later, stage + 1)

    def arrive(self, which):
        last = self.steps - 1
        self.drain(which, 1 << last, self.sem_at(last, 0)).wait_recv()

    def close(self):
        for which in range(3):
            self.drain(which, self.devices - 1, 0).wait_send()


def gather_sems(devices):
    steps = devices.bit_length() - 1
    return (steps - 1) * steps // 2 + 1


def greet_partners(me, devices, barrier):
    for step in range(devices.bit_length() - 1):
        pl.semaphore_signal(
            barrier, inc=1, device_id=(flip(me, 1 << step),), device_id_type=MESH
        )


def greet(me, devices, barrier):
    @pl.loop(1, devices)
    def _(shift):
        pl.semaphore_signal(
            barrier, inc=1, device_id=((me + shift) % devices,), device_id_type=MESH
        )


def gather_kernel(devices, w_up, w_down, w_out, full_up, full_down, full_out, send_sem, recv_sem):
    me = lax.axis_index("dp")
    barrier = pltpu.get_barrier_semaphore()
    greet(me, devices, barrier)
    gather = Gather(me, devices, (full_up, full_down, full_out), send_sem, recv_sem)
    gather.fill((w_up, w_down, w_out))
    pl.semaphore_wait(barrier, devices - 1)
    gather.pass_on()
    for which in range(3):
        gather.arrive(which)
    gather.close()


def gather_weights(devices, w_up, w_down, w_out):
    shapes = []
    for shard, width in ((w_up, FF), (w_down, D), (w_out, VOCAB)):
        shapes.append(
            jax.ShapeDtypeStruct((devices, shard.size // width, width), jnp.bfloat16)
        )
    return pl.pallas_call(
        functools.partial(gather_kernel, devices),
        out_shape=shapes,
        in_specs=[VMEM] * 3,
        out_specs=[VMEM] * 3,
        scratch_shapes=[
            pltpu.SemaphoreType.DMA((3, devices)),
            pltpu.SemaphoreType.DMA((3, devices)),
        ],
        compiler_params=pltpu.CompilerParams(collective_id=0, has_side_effects=True),
        name="gather_weights",
    )(w_up, w_down, w_out)


def dot_rows(left, right):
    return jnp.dot(left, right, preferred_element_type=jnp.float32)


def dot_last(left, right, precision=None):
    return lax.dot_general(
        left, right, (((1,), (1,)), ((), ())), precision=precision,
        preferred_element_type=jnp.float32,
    )


def dot_first(left, right):
    return lax.dot_general(
        left, right, (((0,), (0,)), ((), ())), preferred_element_type=jnp.float32
    )


def row_blocks(total, body):
    block = min(128, total)

    @pl.loop(0, total // block)
    def _(step):
        body(pl.ds(pl.multiple_of(step * block, block), block))


def normalize(features, normalized):
    def body(rows):
        flat_in = features[rows, :].astype(jnp.float32)
        centre = jnp.mean(flat_in, axis=1, keepdims=True)
        shifted = flat_in - centre
        spread = jnp.mean(shifted * shifted, axis=1, keepdims=True)
        normalized[rows, :] = (shifted * lax.rsqrt(spread + 1e-05)).astype(jnp.bfloat16)

    row_blocks(features.shape[0], body)


def project_up(normalized, up_mat, activation, hidden):
    def body(rows):
        act = dot_rows(normalized[rows, :], up_mat[...].reshape(D, FF))
        activation[rows, :] = act
        hidden[rows, :] = (act * (1.0 / (1.0 + jnp.exp(-act)))).astype(jnp.bfloat16)

    row_blocks(normalized.shape[0], body)


def project_down(features, hidden, down_mat, out_mat, block_out, log_probs):
    def body(rows):
        flat_in = features[rows, :].astype(jnp.float32)
        out_rows = (flat_in + 0.5 * dot_rows(hidden[rows, :], down_mat[...].reshape(FF, D))).astype(
            jnp.bfloat16
        )
        block_out[rows, :] = out_rows
        logits = dot_rows(out_rows, out_mat[...].reshape(D, VOCAB))
        top = jnp.max(logits, axis=1, keepdims=True)
        low = logits - top
        log_probs[rows, :] = low - jnp.log(jnp.sum(jnp.exp(low), axis=1, keepdims=True))

    row_blocks(features.shape[0], body)


def ctc_grad(
    loss_scale,
    frame_lens,
    label_lens,
    labels,
    log_probs,
    emitted,
    alpha_rows,
    beta_rows,
    logit_grad,
):
    utterances, label_count = labels.shape
    frames = log_probs.shape[0] // utterances
    states = 2 * label_count + 1

    label_ids = lax.broadcasted_iota(jnp.int32, (label_count, LANES), 0)
    state_at = lax.broadcasted_iota(jnp.int32, (label_count, LANES), 1)
    spread_now = (state_at == 2 * label_ids + 1).astype(jnp.bfloat16)
    spread_back = (state_at == 2 * label_ids + 3).astype(jnp.bfloat16)
    spread_ahead = (state_at == 2 * label_ids - 1).astype(jnp.bfloat16)
    label_rows = jnp.concatenate(
        [
            labels[...].astype(jnp.float32),
            jnp.zeros((8 - utterances, label_count), jnp.float32),
        ],
        axis=0,
    ).astype(jnp.bfloat16)
    extended = dot_rows(label_rows, spread_now)
    earlier = dot_rows(label_rows, spread_back)
    later = dot_rows(label_rows, spread_ahead)
    row_ids = lax.broadcasted_iota(jnp.int32, (8, LANES), 0)
    lane_ids = lax.broadcasted_iota(jnp.int32, (8, LANES), 1)
    may_skip = (extended > 0.5) & (extended != earlier)
    skip_later = (later > 0.5) & (later != extended)
    skip_add = jnp.where(may_skip, 0.0, negative)
    later_add = jnp.where(skip_later, 0.0, negative)
    ends = jnp.full((8, LANES), -9, jnp.int32)
    first_frame = jnp.full((8, LANES), -9, jnp.int32)
    for utterance in range(utterances):
        ends = jnp.where(row_ids == utterance, 2 * label_lens[utterance], ends)
        first_frame = jnp.where(row_ids == utterance, frame_lens[utterance] - 1, first_frame)
    finish = jnp.where((lane_ids == ends) | (lane_ids == ends - 1), 0.0, negative)

    emitted[...] = jnp.full(emitted.shape, negative, jnp.float32)
    vocab_ids = lax.broadcasted_iota(jnp.int32, (VOCAB, LANES), 0).astype(jnp.float32)
    lanes_wide = lax.broadcasted_iota(jnp.int32, (VOCAB, LANES), 1)
    frame_lanes = lax.broadcasted_iota(jnp.int32, (frames, LANES), 1)
    onehots = []
    for utterance in range(utterances):
        onehot = jnp.where(
            (vocab_ids == extended[utterance : utterance + 1, :]) & (lanes_wide < states), 1.0, 0.0
        )
        onehots.append(onehot)
        picked = jnp.dot(
            log_probs[utterance * frames : (utterance + 1) * frames, :],
            onehot,
            precision=lax.Precision.HIGHEST,
            preferred_element_type=jnp.float32,
        )
        emitted[:, utterance, :] = jnp.where(frame_lanes < states, picked, negative)

    def log_three(one, two, three):
        top = jnp.maximum(jnp.maximum(one, two), three)
        return top + jnp.log(jnp.exp(one - top) + jnp.exp(two - top) + jnp.exp(three - top))

    def ahead(values, count):
        return pltpu.roll(values, count, 1) if count else values

    def behind(values, count):
        return pltpu.roll(values, LANES - count, 1) if count else values

    skips = [ahead(skip_add, count) for count in range(3)]
    later_skips = [behind(later_add, count) for count in range(3)]
    finishes = [behind(finish, count) for count in range(3)]

    def advance(pair, carry):
        alpha, weighted = carry
        frame = 2 * pair
        back = frames - 1 - frame
        moved = [ahead(alpha, count) for count in range(5)]
        other = [behind(weighted, count) for count in range(5)]
        emit, emit_back = emitted[frame], emitted[back]
        ends_here = first_frame == back
        firsts, lasts = [], []
        for count in range(3):
            base = log_three(moved[count], moved[count + 1], moved[count + 2] + skips[count])
            rest = log_three(other[count], other[count + 1], other[count + 2] + later_skips[count])
            rest = jnp.where(ends_here, finishes[count], rest)
            if count == 0:
                alpha_rows[frame] = base
                beta_rows[back] = rest
            firsts.append(base + ahead(emit, count))
            lasts.append(rest + behind(emit_back, count))
        base = log_three(firsts[0], firsts[1], firsts[2] + skips[0])
        rest = log_three(lasts[0], lasts[1], lasts[2] + later_skips[0])
        rest = jnp.where(first_frame == back - 1, finish, rest)
        alpha_rows[frame + 1] = base
        beta_rows[back - 1] = rest
        return (base + emitted[frame + 1], rest + emitted[back - 1])

    nothing = jnp.full((8, LANES), negative, jnp.float32)
    start = jnp.where(lane_ids == 0, 0.0, negative)
    lax.fori_loop(0, frames // 2, advance, (start, nothing), unroll=8)

    frame_ids = lax.broadcasted_iota(jnp.int32, (frames, LANES), 0)
    for utterance in range(utterances):
        joint = (
            alpha_rows[:, utterance, :] + emitted[:, utterance, :] + beta_rows[:, utterance, :]
        )
        top = jnp.max(joint, axis=1, keepdims=True)
        mass = jnp.exp(joint - top)
        share = mass / jnp.sum(mass, axis=1, keepdims=True)
        occupancy = jnp.where(frame_ids < frame_lens[utterance], share, 0.0)
        gamma = dot_last(occupancy, onehots[utterance], lax.Precision.HIGHEST)
        rows = slice(utterance * frames, (utterance + 1) * frames)
        probs = jnp.exp(log_probs[rows, :])
        held = jnp.sum(occupancy, axis=1, keepdims=True)
        logit_grad[rows, :] = (loss_scale * (probs * held - gamma)).astype(jnp.bfloat16)


def grad_ff(logit_grad, out_mat, ff_grad):
    def body(rows):
        ff_grad[rows, :] = (
            0.5 * dot_last(logit_grad[rows, :], out_mat[...].reshape(D, VOCAB))
        ).astype(jnp.bfloat16)

    row_blocks(logit_grad.shape[0], body)


def grad_act(ff_grad, down_mat, activation, act_grad):
    def body(rows):
        act = activation[rows, :]
        sigmoid = 1.0 / (1.0 + jnp.exp(-act))
        slope = sigmoid * (1.0 + act * (1.0 - sigmoid))
        act_grad[rows, :] = (
            dot_last(ff_grad[rows, :], down_mat[...].reshape(FF, D)) * slope
        ).astype(jnp.bfloat16)

    row_blocks(ff_grad.shape[0], body)


def step_kernel(
    loss_scale,
    frame_lens,
    label_lens,
    features,
    labels,
    up_mat,
    down_mat,
    out_mat,
    grad_up,
    grad_down,
    grad_out,
    normalized,
    activation,
    hidden,
    block_out,
    log_probs,
    emitted,
    alpha_rows,
    beta_rows,
    logit_grad,
    ff_grad,
    act_grad,
):
    normalize(features, normalized)
    project_up(normalized, up_mat, activation, hidden)
    project_down(features, hidden, down_mat, out_mat, block_out, log_probs)
    ctc_grad(
        loss_scale, frame_lens, label_lens, labels, log_probs, emitted, alpha_rows, beta_rows,
        logit_grad,
    )
    grad_ff(logit_grad, out_mat, ff_grad)
    grad_act(ff_grad, down_mat, activation, act_grad)
    grad_up[...] = dot_first(normalized[...], act_grad[...])
    grad_down[...] = dot_first(hidden[...], ff_grad[...])
    grad_out[...] = dot_first(block_out[...], logit_grad[...])


def step_scratch(total, frames):
    return [
        pltpu.VMEM((total, D), jnp.bfloat16),
        pltpu.VMEM((total, FF), jnp.float32),
        pltpu.VMEM((total, FF), jnp.bfloat16),
        pltpu.VMEM((total, D), jnp.bfloat16),
        pltpu.VMEM((total, VOCAB), jnp.float32),
        pltpu.VMEM((frames, 8, LANES), jnp.float32),
        pltpu.VMEM((frames, 8, LANES), jnp.float32),
        pltpu.VMEM((frames, 8, LANES), jnp.float32),
        pltpu.VMEM((total, VOCAB), jnp.bfloat16),
        pltpu.VMEM((total, D), jnp.bfloat16),
        pltpu.VMEM((total, FF), jnp.bfloat16),
    ]


def local_step(loss_scale, frame_lens, label_lens, features, labels, up_mat, down_mat, out_mat):
    total = features.shape[0]
    frames = total // labels.shape[0]
    return pl.pallas_call(
        functools.partial(step_kernel, loss_scale),
        out_shape=[
            jax.ShapeDtypeStruct((D, FF), jnp.float32),
            jax.ShapeDtypeStruct((FF, D), jnp.float32),
            jax.ShapeDtypeStruct((D, VOCAB), jnp.float32),
        ],
        in_specs=[SMEM, SMEM] + [VMEM] * 5,
        out_specs=[VMEM] * 3,
        scratch_shapes=step_scratch(total, frames),
        compiler_params=pltpu.CompilerParams(vmem_limit_bytes=40 << 20),
        name="local_step",
    )(frame_lens, label_lens, features, labels, up_mat, down_mat, out_mat)


class Sum:
    def __init__(self, me, devices, grads, received, staged, send_sem, recv_sem):
        self.me, self.grads, self.received, self.staged = me, grads, received, staged
        self.send_sem, self.recv_sem = send_sem, recv_sem
        self.orders = [order[::-1] for order in bit_orders(devices)]
        self.steps = len(self.orders[0])
        self.copies = [{}, {}, {}]

    def sum_of(self, which, place, pattern, stage):
        value = self.grads[which][place]
        for bit in self.orders[which][:stage]:
            self.copies[which][pattern + bit].wait_recv()
            value = value + self.received[which][pattern + bit]
        return value

    def send(self, which, stage):
        order = self.orders[which]
        for offset in subsets(order[stage + 1 :][::-1])[::-1]:
            slot = offset + order[stage]
            place = place_with(self.me, order, slot)
            if stage == 0:
                source = self.grads[which].at[place]
            else:
                self.staged[which][slot] = self.sum_of(which, place, slot, stage)
                source = self.staged[which].at[slot]
            copy = pltpu.make_async_remote_copy(
                src_ref=source,
                dst_ref=self.received[which].at[slot],
                send_sem=self.send_sem.at[which, slot],
                recv_sem=self.recv_sem.at[which, slot],
                device_id=(flip(self.me, order[stage]),),
                device_id_type=MESH,
            )
            copy.start()
            self.copies[which][slot] = copy

    def finish(self, devices, reduced, squares, own_squares, small_send, small_recv):
        me = self.me
        own = jnp.zeros((1, LANES), jnp.float32)
        for which in (2, 1, 0):
            value = self.sum_of(which, me, 0, self.steps)
            rows, width = value.shape
            parts = width // LANES
            for part in range(parts):
                piece = value[:, part * LANES : (part + 1) * LANES]
                reduced[which][pl.ds(part, rows, stride=parts), :] = piece
                own = own + jnp.sum(piece * piece, axis=0, keepdims=True)
        own_squares[...] = own
        squares[0] = own

        def small_copy(shift):
            return pltpu.make_async_remote_copy(
                src_ref=own_squares,
                dst_ref=squares.at[shift],
                send_sem=small_send.at[shift],
                recv_sem=small_recv.at[shift],
                device_id=((me + shift) % devices,),
                device_id_type=MESH,
            )

        @pl.loop(1, devices)
        def _(shift):
            small_copy(shift).start()

        for copies in self.copies:
            for copy in copies.values():
                copy.wait_send()

        @pl.loop(1, devices)
        def _(shift):
            small_copy(shift).wait()


def chunks(blocks):
    if blocks >= 4:
        return [blocks // 4, blocks // 4, blocks // 2]
    return [1] * blocks


def sum_groups(steps):
    groups, sems = [], 0
    for stage in range(steps):
        sizes = chunks(1 << (steps - 1 - stage))
        groups.append((sems, sizes))
        sems += len(sizes)
    return groups, sems


class GroupSum:
    def __init__(self, me, devices, grads, received, staged, send_sem, recv_sem):
        self.me, self.devices = me, devices
        self.grads, self.received, self.staged = grads, received, staged
        self.send_sem, self.recv_sem = send_sem, recv_sem
        self.orders = [order[::-1] for order in bit_orders(devices)]
        self.steps = len(self.orders[0])
        self.groups, _ = sum_groups(self.steps)
        self.seen = set()

    def slots(self, which, stage):
        order = self.orders[which]
        return [
            offset + order[stage] for offset in subsets(order[stage + 1 :][::-1])[::-1]
        ]

    def sem_at(self, which, stage, slot):
        at = self.slots(which, stage).index(slot)
        sem, sizes = self.groups[stage]
        for size in sizes:
            if at < size:
                return sem, size
            at, sem = at - size, sem + 1

    def sum_of(self, which, place, pattern, stage):
        value = self.grads[which][place]
        for at, bit in enumerate(self.orders[which][:stage]):
            sem, size = self.sem_at(which, at, pattern + bit)
            if (which, sem) not in self.seen:
                self.seen.add((which, sem))
                drain(
                    self.received[which], size, self.send_sem.at[which],
                    self.recv_sem.at[which, sem], flip(self.me, bit),
                ).wait_recv()
            value = value + self.received[which][pattern + bit]
        return value

    def send(self, which, stage):
        order = self.orders[which]
        for slot in self.slots(which, stage):
            place = place_with(self.me, order, slot)
            if stage == 0:
                source = self.grads[which].at[place]
            else:
                self.staged[which][slot] = self.sum_of(which, place, slot, stage)
                source = self.staged[which].at[slot]
            pltpu.make_async_remote_copy(
                src_ref=source,
                dst_ref=self.received[which].at[slot],
                send_sem=self.send_sem.at[which],
                recv_sem=self.recv_sem.at[which, self.sem_at(which, stage, slot)[0]],
                device_id=(flip(self.me, order[stage]),),
                device_id_type=MESH,
            ).start()

    def finish(self, reduced, squares, own_squares, small_send, small_recv):
        me, devices = self.me, self.devices
        own = jnp.zeros((1, LANES), jnp.float32)
        for which in (2, 1, 0):
            value = self.sum_of(which, me, 0, self.steps)
            rows, width = value.shape
            parts = width // LANES
            for part in range(parts):
                piece = value[:, part * LANES : (part + 1) * LANES]
                reduced[which][pl.ds(part, rows, stride=parts), :] = piece
                own = own + jnp.sum(piece * piece, axis=0, keepdims=True)
        own_squares[...] = own
        squares[0] = own

        @pl.loop(1, devices)
        def _(shift):
            pltpu.make_async_remote_copy(
                src_ref=own_squares,
                dst_ref=squares.at[shift],
                send_sem=small_send,
                recv_sem=small_recv,
                device_id=((me + shift) % devices,),
                device_id_type=MESH,
            ).start()

        for which in range(3):
            drain(
                self.received[which], devices - 1, self.send_sem.at[which],
                self.recv_sem.at[which, 0], flip(me, 1),
            ).wait_send()
        small = drain(squares, devices - 1, small_send, small_recv, flip(me, 1))
        small.wait_send()
        small.wait_recv()


def sum_kernel(devices, *refs):
    grads, reduced, squares = refs[:3], refs[3:6], refs[6]
    received, staged = refs[7:10], refs[10:13]
    own_squares, send_sem, recv_sem, small_send, small_recv = refs[13:]
    me = lax.axis_index("dp")
    barrier = pltpu.get_barrier_semaphore()
    greet(me, devices, barrier)
    pl.semaphore_wait(barrier, devices - 1)
    total = Sum(me, devices, grads, received, staged, send_sem, recv_sem)
    for stage in range(total.steps):
        for which in range(3):
            total.send(which, stage)
    total.finish(devices, reduced, squares, own_squares, small_send, small_recv)


def fused_kernel(devices, loss_scale, *refs):
    frame_lens, label_lens, features, labels = refs[:4]
    shards, reduced, squares = refs[4:7], refs[7:10], refs[10]
    fulls, grads, received, staged = refs[11:14], refs[14:17], refs[17:20], refs[20:23]
    gather_send, gather_recv, own_squares, send_sem, recv_sem, small_send, small_recv = refs[23:30]
    normalized, activation, hidden, block_out, log_probs = refs[30:35]
    emitted, alpha_rows, beta_rows, logit_grad, ff_grad, act_grad = refs[35:41]
    held, load_sem = refs[41:45], refs[45]
    up_mat, down_mat, out_mat = fulls
    me = lax.axis_index("dp")
    loads = [
        pltpu.make_async_copy(source, target, load_sem.at[at])
        for at, (source, target) in enumerate(zip((*shards, features), held))
    ]
    for load in loads:
        load.start()
    shards, features = held[:3], held[3]
    barrier = pltpu.get_barrier_semaphore()
    greet_partners(me, devices, barrier)
    gather = GroupGather(me, devices, fulls, gather_send, gather_recv)
    for load in loads[:3]:
        load.wait()
    gather.fill(shards)
    loads[3].wait()
    normalize(features, normalized)
    pl.semaphore_wait(barrier, gather.steps)
    gather.pass_on()
    gather.arrive(0)
    project_up(normalized, up_mat, activation, hidden)
    gather.arrive(1)
    gather.arrive(2)
    project_down(features, hidden, down_mat, out_mat, block_out, log_probs)
    ctc_grad(
        loss_scale, frame_lens, label_lens, labels, log_probs, emitted, alpha_rows, beta_rows,
        logit_grad,
    )
    total = GroupSum(me, devices, grads, received, staged, send_sem, recv_sem)
    pending = [list(range(total.steps)) for _ in range(3)]

    def advance(*whiches):
        for which in whiches:
            if pending[which]:
                total.send(which, pending[which].pop(0))

    def put(which, value):
        grads[which][...] = value.reshape(grads[which].shape)

    grad_ff(logit_grad, out_mat, ff_grad)
    put(1, dot_first(hidden[...], ff_grad[...]))
    advance(1)
    grad_act(ff_grad, down_mat, activation, act_grad)
    advance(1)
    put(0, dot_first(normalized[...], act_grad[...]))
    advance(0)
    put(2, dot_first(block_out[...], logit_grad[...]))
    advance(2)
    while any(pending):
        advance(1, 0, 2)
    total.finish(reduced, squares, own_squares, small_send, small_recv)
    gather.close()


def fused_step(loss_scale, devices, frame_lens, label_lens, features, labels, weights):
    total = features.shape[0]
    frames = total // labels.shape[0]
    blocks = [
        (devices, weight.size // width, width)
        for weight, width in zip(weights, (FF, D, VOCAB))
    ]
    wide = [pltpu.VMEM(block, jnp.float32) for block in blocks]
    return pl.pallas_call(
        functools.partial(fused_kernel, devices, loss_scale),
        out_shape=[jax.ShapeDtypeStruct(weight.shape, jnp.float32) for weight in weights]
        + [jax.ShapeDtypeStruct((devices, 1, LANES), jnp.float32)],
        in_specs=[SMEM, SMEM, HBM, VMEM] + [HBM] * 3,
        out_specs=[VMEM] * 4,
        scratch_shapes=[pltpu.VMEM(block, jnp.bfloat16) for block in blocks]
        + wide * 3
        + [
            pltpu.SemaphoreType.DMA((3,)),
            pltpu.SemaphoreType.DMA((3, gather_sems(devices))),
            pltpu.VMEM((1, LANES), jnp.float32),
            pltpu.SemaphoreType.DMA((3,)),
            pltpu.SemaphoreType.DMA((3, sum_groups(devices.bit_length() - 1)[1])),
            pltpu.SemaphoreType.DMA,
            pltpu.SemaphoreType.DMA,
        ]
        + step_scratch(total, frames)
        + [pltpu.VMEM(array.shape, array.dtype) for array in (*weights, features)]
        + [pltpu.SemaphoreType.DMA((4,))],
        compiler_params=pltpu.CompilerParams(
            collective_id=2, has_side_effects=True, vmem_limit_bytes=67043328
        ),
        name="fused_step",
    )(frame_lens, label_lens, features, labels, *weights)


def sum_gradients(devices, grads):
    blocks = [grad.reshape(devices, grad.shape[0] // devices, grad.shape[1]) for grad in grads]
    shapes = [
        jax.ShapeDtypeStruct((block[0].size // LANES, LANES), jnp.float32) for block in blocks
    ]
    buffers = [pltpu.VMEM(block.shape, jnp.float32) for block in blocks]
    return pl.pallas_call(
        functools.partial(sum_kernel, devices),
        out_shape=shapes + [jax.ShapeDtypeStruct((devices, 1, LANES), jnp.float32)],
        in_specs=[VMEM] * 3,
        out_specs=[VMEM] * 4,
        scratch_shapes=buffers
        + buffers
        + [
            pltpu.VMEM((1, LANES), jnp.float32),
            pltpu.SemaphoreType.DMA((3, devices)),
            pltpu.SemaphoreType.DMA((3, devices)),
            pltpu.SemaphoreType.DMA((devices,)),
            pltpu.SemaphoreType.DMA((devices,)),
        ],
        compiler_params=pltpu.CompilerParams(
            collective_id=1, has_side_effects=True, vmem_limit_bytes=50 << 20
        ),
        name="sum_gradients",
    )(*blocks)


def adam_kernel(squares, *refs):
    weights, firsts, seconds, grads, outs = (refs[at : at + 3] for at in (0, 3, 6, 9, 12))
    new_firsts, new_seconds = refs[15:18], refs[18:21]
    total = jnp.sum(squares[...])
    clip = 1.0 / jnp.maximum(jnp.sqrt(jnp.full((1, LANES), total)), 1.0)
    for which in range(3):
        scaled = clip * grads[which][...]
        first = 0.9 * firsts[which][...] + 0.1 * scaled
        second = 0.999 * seconds[which][...] + 0.001 * scaled * scaled
        ratio = first / first_correction / (jnp.sqrt(second / second_correction) + 1e-08)
        outs[which][...] = weights[which][...] - 0.001 * ratio
        new_firsts[which][...] = first
        new_seconds[which][...] = second


def adam(squares, weights, firsts, seconds, grads):
    shapes = [jax.ShapeDtypeStruct(weight.shape, jnp.float32) for weight in weights]
    return pl.pallas_call(
        adam_kernel,
        out_shape=shapes * 3,
        in_specs=[VMEM] * 13,
        out_specs=[VMEM] * 9,
        compiler_params=pltpu.CompilerParams(vmem_limit_bytes=67043328),
        name="adam",
    )(squares, *weights, *firsts, *seconds, *grads)


def per_device(
    features,
    frame_lens,
    labels,
    label_lens,
    w_up,
    w_down,
    w_out,
    first_up,
    first_down,
    first_out,
    second_up,
    second_down,
    second_out,
):
    devices = lax.axis_size("dp")
    batch, frames, width = features.shape

    def lined(*arrays):
        return [array.reshape(array.shape[0] // LANES, LANES) for array in arrays]

    weights = lined(w_up, w_down, w_out)
    loss_scale = 1.0 / (batch * devices)
    rows_in = features.reshape(batch * frames, width)
    if w_up.size % (8 * FF) == 0 and w_out.size % (8 * VOCAB) == 0:
        *shares, squares = fused_step(
            loss_scale, devices, frame_lens, label_lens, rows_in, labels, weights
        )
    else:
        full_up, full_down, full_out = gather_weights(devices, *weights)
        grads = local_step(
            loss_scale,
            frame_lens,
            label_lens,
            rows_in,
            labels,
            full_up.reshape(D, FF),
            full_down.reshape(FF, D),
            full_out.reshape(D, VOCAB),
        )
        *shares, squares = sum_gradients(devices, grads)
    results = adam(
        squares,
        weights,
        lined(first_up, first_down, first_out),
        lined(second_up, second_down, second_out),
        shares,
    )
    return tuple(result.reshape(-1) for result in results)


def solution(mesh):
    flat = P("dp")
    return jax.shard_map(
        per_device,
        mesh=mesh,
        in_specs=(P("dp", None, None), flat, P("dp", None), flat) + (flat,) * 9,
        out_specs=(flat,) * 9,
        check_vma=False,
    )
```

```python
import functools

import jax
import jax.numpy as jnp
from jax import lax
from jax.experimental import pallas as pl
from jax.experimental.pallas import tpu as pltpu
from jax.sharding import PartitionSpec as P

D = 256
FF = 1024
VOCAB = 256
LANES = 128
MESH = pl.DeviceIdType.MESH

first_correction = 1.0 - (0.9**10) ** 10
second_correction = 1.0 - (0.999**10) ** 10
negative = -1e30
LOG2E = 1.4426950408889634
PARTS = 2
VMEM = pl.BlockSpec(memory_space=pltpu.VMEM)
SMEM = pl.BlockSpec(memory_space=pltpu.SMEM)
HBM = pl.BlockSpec(memory_space=pltpu.HBM)


def flip(me, bit):
    return me + bit - 2 * bit * ((me // bit) % 2)


def bit_orders(devices):
    bits = [1 << k for k in range(devices.bit_length() - 1)]
    core, rest = bits[:1], bits[1:]
    down = rest[::-1]
    swapped = down[:-2] + down[-2:][::-1]
    turned = down[-2:] + down[:-2]
    return (down + core, swapped + core, turned + core)


def subsets(bits):
    offsets = [0]
    for bit in bits:
        offsets = offsets + [offset + bit for offset in offsets]
    return offsets


def place_with(me, free, pattern):
    place = me
    for bit in free:
        if pattern & bit:
            place = flip(place, bit)
    return place


class Gather:
    def __init__(self, me, devices, fulls, send_sem, recv_sem):
        self.me, self.fulls = me, fulls
        self.send_sem, self.recv_sem = send_sem, recv_sem
        self.orders = bit_orders(devices)
        self.steps = len(self.orders[0])
        self.copies = [{}, {}, {}]

    def fill(self, shards):
        for shard, full in zip(shards, self.fulls):
            rows, width = full.shape[1:]
            parts = width // LANES
            for part in range(parts):
                full[self.me, :, part * LANES : (part + 1) * LANES] = shard[
                    pl.ds(part, rows, stride=parts), :
                ].astype(jnp.bfloat16)

    def send(self, which, pattern, stage):
        order, full = self.orders[which], self.fulls[which]
        owner = place_with(self.me, order[:stage], pattern)
        slot = pattern + order[stage]
        copy = pltpu.make_async_remote_copy(
            src_ref=full.at[owner],
            dst_ref=full.at[owner],
            send_sem=self.send_sem.at[which, slot],
            recv_sem=self.recv_sem.at[which, slot],
            device_id=(flip(self.me, order[stage]),),
            device_id_type=MESH,
        )
        copy.start()
        self.copies[which][slot] = copy

    def pass_on(self):
        for which in range(3):
            for stage in range(self.steps):
                self.send(which, 0, stage)
        for stage in range(self.steps - 1):
            for at in range(1 << stage):
                for which in range(3):
                    order = self.orders[which]
                    pattern = subsets(order[:stage])[at] + order[stage]
                    self.copies[which][pattern].wait_recv()
                    for later in range(stage + 1, self.steps):
                        self.send(which, pattern, later)

    def arrive(self, which):
        order = self.orders[which]
        for pattern in subsets(order[:-1]):
            self.copies[which][pattern + order[-1]].wait_recv()

    def close(self):
        for copies in self.copies:
            for copy in copies.values():
                copy.wait_send()


def drain(ref, blocks, send_sem, recv_sem, peer):
    return pltpu.make_async_remote_copy(
        src_ref=ref.at[pl.ds(0, blocks)],
        dst_ref=ref.at[pl.ds(0, blocks)],
        send_sem=send_sem,
        recv_sem=recv_sem,
        device_id=(peer,),
        device_id_type=MESH,
    )


class GroupGather:
    def __init__(self, me, devices, fulls, send_sem, recv_sem):
        self.me, self.devices, self.fulls = me, devices, fulls
        self.send_sem, self.recv_sem = send_sem, recv_sem
        self.orders = bit_orders(devices)
        self.steps = len(self.orders[0])

    def fill(self, shards):
        for shard, full in zip(shards, self.fulls):
            rows, width = full.shape[1:]
            parts = width // LANES
            for part in range(parts):
                full[self.me, :, part * LANES : (part + 1) * LANES] = shard[
                    pl.ds(part, rows, stride=parts), :
                ].astype(jnp.bfloat16)

    def sem_at(self, stage, group):
        return stage * (stage + 1) // 2 + (group if stage < self.steps - 1 else 0)

    def send(self, which, patterns, stage, group):
        order, full = self.orders[which], self.fulls[which]
        for pattern in patterns:
            owner = place_with(self.me, order[:stage], pattern)
            pltpu.make_async_remote_copy(
                src_ref=full.at[owner],
                dst_ref=full.at[owner],
                send_sem=self.send_sem.at[which],
                recv_sem=self.recv_sem.at[which, self.sem_at(stage, group)],
                device_id=(flip(self.me, order[stage]),),
                device_id_type=MESH,
            ).start()

    def drain(self, which, blocks, at):
        return drain(
            self.fulls[which], blocks, self.send_sem.at[which], self.recv_sem.at[which, at],
            flip(self.me, 1),
        )

    def pass_on(self):
        for which in range(3):
            for stage in range(self.steps):
                self.send(which, [0], stage, 0)
        for stage in range(self.steps - 1):
            for group in range(stage + 1):
                for which in range(3):
                    order = self.orders[which]
                    patterns = [0]
                    if group:
                        patterns = [at + order[group - 1] for at in subsets(order[: group - 1])]
                    self.drain(which, len(patterns), self.sem_at(stage, group)).wait_recv()
                    patterns = [pattern + order[stage] for pattern in patterns]
                    for later in range(stage + 1, self.steps):
                        self.send(which, patterns, later, stage + 1)

    def arrive(self, which):
        last = self.steps - 1
        self.drain(which, 1 << last, self.sem_at(last, 0)).wait_recv()

    def close(self):
        for which in range(3):
            self.drain(which, self.devices - 1, 0).wait_send()


def gather_sems(devices):
    steps = devices.bit_length() - 1
    return (steps - 1) * steps // 2 + 1


def greet_partners(me, devices, barrier):
    for step in range(devices.bit_length() - 1):
        pl.semaphore_signal(
            barrier, inc=1, device_id=(flip(me, 1 << step),), device_id_type=MESH
        )


def greet(me, devices, barrier):
    @pl.loop(1, devices)
    def _(shift):
        pl.semaphore_signal(
            barrier, inc=1, device_id=((me + shift) % devices,), device_id_type=MESH
        )


def gather_kernel(devices, w_up, w_down, w_out, full_up, full_down, full_out, send_sem, recv_sem):
    me = lax.axis_index("dp")
    barrier = pltpu.get_barrier_semaphore()
    greet(me, devices, barrier)
    gather = Gather(me, devices, (full_up, full_down, full_out), send_sem, recv_sem)
    gather.fill((w_up, w_down, w_out))
    pl.semaphore_wait(barrier, devices - 1)
    gather.pass_on()
    for which in range(3):
        gather.arrive(which)
    gather.close()


def gather_weights(devices, w_up, w_down, w_out):
    shapes = []
    for shard, width in ((w_up, FF), (w_down, D), (w_out, VOCAB)):
        shapes.append(
            jax.ShapeDtypeStruct((devices, shard.size // width, width), jnp.bfloat16)
        )
    return pl.pallas_call(
        functools.partial(gather_kernel, devices),
        out_shape=shapes,
        in_specs=[VMEM] * 3,
        out_specs=[VMEM] * 3,
        scratch_shapes=[
            pltpu.SemaphoreType.DMA((3, devices)),
            pltpu.SemaphoreType.DMA((3, devices)),
        ],
        compiler_params=pltpu.CompilerParams(collective_id=0, has_side_effects=True),
        name="gather_weights",
    )(w_up, w_down, w_out)


def dot_rows(left, right):
    return jnp.dot(left, right, preferred_element_type=jnp.float32)


def dot_last(left, right, precision=None):
    return lax.dot_general(
        left, right, (((1,), (1,)), ((), ())), precision=precision,
        preferred_element_type=jnp.float32,
    )


def dot_first(left, right):
    return lax.dot_general(
        left, right, (((0,), (0,)), ((), ())), preferred_element_type=jnp.float32
    )


def row_blocks(total, body):
    block = min(128, total)

    @pl.loop(0, total // block)
    def _(step):
        body(pl.ds(pl.multiple_of(step * block, block), block))


def normalize(features, normalized):
    def body(rows):
        flat_in = features[rows, :].astype(jnp.float32)
        centre = jnp.mean(flat_in, axis=1, keepdims=True)
        shifted = flat_in - centre
        spread = jnp.mean(shifted * shifted, axis=1, keepdims=True)
        normalized[rows, :] = (shifted * lax.rsqrt(spread + 1e-05)).astype(jnp.bfloat16)

    row_blocks(features.shape[0], body)


def project_up(normalized, up_mat, activation, hidden):
    def body(rows):
        act = dot_rows(normalized[rows, :], up_mat[...].reshape(D, FF))
        activation[rows, :] = act
        hidden[rows, :] = (act * (1.0 / (1.0 + jnp.exp(-act)))).astype(jnp.bfloat16)

    row_blocks(normalized.shape[0], body)


def project_down(features, hidden, down_mat, out_mat, block_out, log_probs):
    def body(rows):
        flat_in = features[rows, :].astype(jnp.float32)
        out_rows = (flat_in + 0.5 * dot_rows(hidden[rows, :], down_mat[...].reshape(FF, D))).astype(
            jnp.bfloat16
        )
        block_out[rows, :] = out_rows
        logits = dot_rows(out_rows, out_mat[...].reshape(D, VOCAB))
        top = jnp.max(logits, axis=1, keepdims=True)
        low = (logits - top) * LOG2E
        log_probs[rows, :] = low - jnp.log2(jnp.sum(jnp.exp2(low), axis=1, keepdims=True))

    row_blocks(features.shape[0], body)


def split_dot(dot, values, picks):
    high = values.astype(jnp.bfloat16)
    rest = values - high.astype(jnp.float32)
    middle = rest.astype(jnp.bfloat16)
    low = (rest - middle.astype(jnp.float32)).astype(jnp.bfloat16)
    return dot(high, picks) + (dot(middle, picks) + dot(low, picks))


def ctc_rows(frames):
    return [pltpu.VMEM((frames, 8, LANES), jnp.float32)] * 4 + [
        pltpu.VMEM((2 * frames, 8, LANES), jnp.float32)
    ] * 4


class Lattice:
    def __init__(self, parts, sign, skip):
        self.parts, self.sign = parts, sign
        self.row = 0 if sign > 0 else 7
        self.skips = [self.spread(skip, part) > 0.5 for part in range(parts)]

    def spread(self, values, part):
        if self.sign > 0:
            return pltpu.roll(values, part, 1, stride=self.parts, stride_axis=0)
        shift = LANES - part - 7 * self.parts
        return pltpu.roll(values, shift, 1, stride=self.parts, stride_axis=0)

    def begin(self, blank, label):
        def whole(values):
            return jnp.broadcast_to(values[self.row : self.row + 1], (8, LANES))

        blank, label = whole(blank), whole(label)
        self.blank = [self.spread(blank, part) for part in range(self.parts)]
        self.label = [self.spread(label, part) for part in range(self.parts + 1)]
        one = jnp.ones((8, LANES), jnp.float32)
        self.blank_mass, self.label_mass = [one] * self.parts, [one] * (self.parts + 1)

    def next_rows(self, values):
        return pltpu.roll(values, 7 if self.sign > 0 else 1, 0)

    def advance(self, emit_blank, emit_label, parts):
        blank, label, blank_mass, label_mass = [], [], [], []
        for part in range(parts):
            b, l, l1 = self.blank[part], self.label[part], self.label[part + 1]
            bm, lm, lm1 = self.blank_mass[part], self.label_mass[part], self.label_mass[part + 1]
            top = jnp.maximum(b, l1)
            mass = bm * jnp.exp2(b - top) + lm1 * jnp.exp2(l1 - top)
            above = jnp.where(self.skips[part], top, b)
            above_mass = jnp.where(self.skips[part], mass, bm)
            peak = jnp.maximum(l, above)
            peak_mass = lm * jnp.exp2(l - peak) + above_mass * jnp.exp2(above - peak)
            if part == 0:
                result = (top, mass, peak, peak_mass)
            blank.append(top + emit_blank)
            label.append(peak + self.spread(emit_label, part))
            blank_mass.append(mass)
            label_mass.append(peak_mass)
        if parts == self.parts:
            label.append(self.next_rows(label[0]))
            label_mass.append(self.next_rows(label_mass[0]))
        self.blank, self.label = blank, label
        self.blank_mass, self.label_mass = blank_mass, label_mass
        return result


def ctc_grad(
    loss_scale,
    frame_lens,
    label_lens,
    labels,
    log_probs,
    emitted,
    emitted_blank,
    alpha_rows,
    beta_rows,
    logit_grad,
):
    utterances, label_count = labels.shape
    frames = log_probs.shape[0] // utterances
    half = LANES // utterances
    depth = 8 * PARTS
    assert label_count + depth <= half and frames % depth == 0

    lane_row = lax.broadcasted_iota(jnp.int32, (8, LANES), 1)
    label_ids = lax.broadcasted_iota(jnp.int32, (label_count, LANES), 0)
    spread_lanes = lax.broadcasted_iota(jnp.int32, (label_count, LANES), 1)
    label_rows = jnp.concatenate(
        [
            labels[...].astype(jnp.float32),
            jnp.zeros((8 - utterances, label_count), jnp.float32),
        ],
        axis=0,
    ).astype(jnp.bfloat16)
    extended = jnp.zeros((8, LANES), jnp.float32)
    for utterance in range(utterances):
        spread = (spread_lanes == label_ids + half * utterance + 1).astype(jnp.bfloat16)
        placed = dot_rows(label_rows, spread)[utterance : utterance + 1]
        extended = extended + jnp.broadcast_to(placed, (8, LANES))
    skip = jnp.where(extended != pltpu.roll(extended, 1, 1), 1.0, 0.0)
    skip_back = pltpu.roll(skip, LANES - 1, 1)

    vocab_ids = lax.broadcasted_iota(jnp.int32, (VOCAB, LANES), 0).astype(jnp.float32)
    vocab_lanes = lax.broadcasted_iota(jnp.int32, (VOCAB, LANES), 1)
    frame_lanes = lax.broadcasted_iota(jnp.int32, (frames, LANES), 1)
    onehots = []
    picked = None
    blanks = None
    for utterance in range(utterances):
        rows = slice(utterance * frames, (utterance + 1) * frames)
        first = half * utterance + 1
        mine = (vocab_lanes >= first) & (vocab_lanes < first + label_count)
        onehot = jnp.where((vocab_ids == extended[0:1, :]) & mine, 1.0, 0.0).astype(jnp.bfloat16)
        onehots.append(onehot)
        picks = split_dot(dot_rows, log_probs[rows, :], onehot)
        blank = jnp.broadcast_to(log_probs[rows, 0:1], (frames, LANES))
        if utterance == 0:
            picked, blanks = picks, blank
        else:
            picked = jnp.where(frame_lanes < half * utterance, picked, picks)
            blanks = jnp.where(frame_lanes < half * utterance, blanks, blank)
    place = frame_lanes % half
    emitted[...] = jnp.where((place >= 1) & (place <= label_count), picked, negative)
    emitted_blank[...] = blanks

    forward = Lattice(PARTS, 1, skip)
    backward = Lattice(PARTS, -1, skip_back)
    start = jnp.full((8, LANES), negative, jnp.float32)
    start_back = start
    for utterance in range(utterances):
        first = half * utterance + 1
        start = jnp.where(lane_row == first, 0.0, start)
        start_back = jnp.where(
            lane_row == first + label_lens[utterance] - 1, 0.0, start_back
        )
    nothing = jnp.full((8, LANES), negative, jnp.float32)

    def row_of(ref, frame):
        return jnp.broadcast_to(ref[pl.ds(frame, 1), :], (8, LANES))

    def block(at, carry):
        forward.begin(*carry[:2])
        backward.begin(*carry[2:])
        for level in range(depth):
            frame = at * depth + level
            needed = min(PARTS, depth - level)
            result = forward.advance(row_of(emitted_blank, frame), row_of(emitted, frame), needed)
            for ref, value in zip(alpha_rows, result):
                ref[frame] = value
            emit = emit_blank = None
            for utterance in range(utterances):
                back = jnp.maximum(frame_lens[utterance] - 1 - frame, 0)
                mine, mine_blank = row_of(emitted, back), row_of(emitted_blank, back)
                if utterance == 0:
                    emit, emit_blank = mine, mine_blank
                else:
                    emit = jnp.where(lane_row < half * utterance, emit, mine)
                    emit_blank = jnp.where(lane_row < half * utterance, emit_blank, mine_blank)
            result = backward.advance(emit_blank, emit, needed)
            for ref, value in zip(beta_rows, result):
                ref[frames - 1 - frame] = value
        return tuple(
            values[0] + jnp.log2(mass[0])
            for lattice in (forward, backward)
            for values, mass in (
                (lattice.blank, lattice.blank_mass), (lattice.label, lattice.label_mass)
            )
        )

    lax.fori_loop(0, frames // depth, block, (start, nothing, start_back, nothing))

    frame_ids = lax.broadcasted_iota(jnp.int32, (frames, LANES), 0)
    alphas = [ref[:, forward.row, :] for ref in alpha_rows]
    betas, alive = [], None
    for ref in beta_rows:
        value = None
        for utterance in range(utterances):
            mine = ref[pl.ds(frames - frame_lens[utterance], frames), backward.row, :]
            value = mine if value is None else jnp.where(frame_lanes < half * utterance, value, mine)
        betas.append(value)
    betas[0], betas[1] = pltpu.roll(betas[0], 1, 1), pltpu.roll(betas[1], 1, 1)
    joint_blank = alphas[0] + emitted_blank[...] + betas[0]
    joint_label = alphas[2] + emitted[...] + betas[2]
    blank_mass, label_mass = alphas[1] * betas[1], alphas[3] * betas[3]
    both = jnp.maximum(joint_blank, joint_label)
    for utterance in range(utterances):
        rows = slice(utterance * frames, (utterance + 1) * frames)
        first = half * utterance
        mine = (frame_lanes >= first) & (frame_lanes < first + half)
        top = jnp.max(jnp.where(mine, both, negative), axis=1, keepdims=True)
        live = mine & (frame_ids < frame_lens[utterance])
        label = jnp.where(live, label_mass * jnp.exp2(joint_label - top), 0.0)
        blank = jnp.where(live, blank_mass * jnp.exp2(joint_blank - top), 0.0)
        blank_sum = jnp.sum(blank, axis=1, keepdims=True)
        total = jnp.sum(label, axis=1, keepdims=True) + blank_sum
        kept = frame_ids[:, 0:1] < frame_lens[utterance]
        scale = jnp.where(kept, 1.0 / jnp.where(kept, total, 1.0), 0.0)
        gamma = split_dot(dot_last, label * scale, onehots[utterance])
        vocab_at = lax.broadcasted_iota(jnp.int32, (frames, VOCAB), 1)
        gamma = gamma + jnp.where(vocab_at == 0, blank_sum * scale, 0.0)
        probs = jnp.exp2(log_probs[rows, :]) * jnp.where(kept, 1.0, 0.0)
        logit_grad[rows, :] = (loss_scale * (probs - gamma)).astype(jnp.bfloat16)


def grad_ff(logit_grad, out_mat, ff_grad):
    def body(rows):
        ff_grad[rows, :] = (
            0.5 * dot_last(logit_grad[rows, :], out_mat[...].reshape(D, VOCAB))
        ).astype(jnp.bfloat16)

    row_blocks(logit_grad.shape[0], body)


def grad_act(ff_grad, down_mat, activation, act_grad):
    def body(rows):
        act = activation[rows, :]
        sigmoid = 1.0 / (1.0 + jnp.exp(-act))
        slope = sigmoid * (1.0 + act * (1.0 - sigmoid))
        act_grad[rows, :] = (
            dot_last(ff_grad[rows, :], down_mat[...].reshape(FF, D)) * slope
        ).astype(jnp.bfloat16)

    row_blocks(ff_grad.shape[0], body)


def step_kernel(
    loss_scale,
    frame_lens,
    label_lens,
    features,
    labels,
    up_mat,
    down_mat,
    out_mat,
    grad_up,
    grad_down,
    grad_out,
    normalized,
    activation,
    hidden,
    block_out,
    log_probs,
    logit_grad,
    ff_grad,
    act_grad,
    emitted,
    emitted_blank,
    *lattice_rows,
):
    normalize(features, normalized)
    project_up(normalized, up_mat, activation, hidden)
    project_down(features, hidden, down_mat, out_mat, block_out, log_probs)
    ctc_grad(
        loss_scale, frame_lens, label_lens, labels, log_probs, emitted, emitted_blank,
        lattice_rows[:4], lattice_rows[4:], logit_grad,
    )
    grad_ff(logit_grad, out_mat, ff_grad)
    grad_act(ff_grad, down_mat, activation, act_grad)
    grad_up[...] = dot_first(normalized[...], act_grad[...])
    grad_down[...] = dot_first(hidden[...], ff_grad[...])
    grad_out[...] = dot_first(block_out[...], logit_grad[...])


def step_scratch(total, frames):
    return [
        pltpu.VMEM((total, D), jnp.bfloat16),
        pltpu.VMEM((total, FF), jnp.float32),
        pltpu.VMEM((total, FF), jnp.bfloat16),
        pltpu.VMEM((total, D), jnp.bfloat16),
        pltpu.VMEM((total, VOCAB), jnp.float32),
        pltpu.VMEM((total, VOCAB), jnp.bfloat16),
        pltpu.VMEM((total, D), jnp.bfloat16),
        pltpu.VMEM((total, FF), jnp.bfloat16),
        pltpu.VMEM((frames, LANES), jnp.float32),
        pltpu.VMEM((frames, LANES), jnp.float32),
    ] + ctc_rows(frames)


def local_step(loss_scale, frame_lens, label_lens, features, labels, up_mat, down_mat, out_mat):
    total = features.shape[0]
    frames = total // labels.shape[0]
    return pl.pallas_call(
        functools.partial(step_kernel, loss_scale),
        out_shape=[
            jax.ShapeDtypeStruct((D, FF), jnp.float32),
            jax.ShapeDtypeStruct((FF, D), jnp.float32),
            jax.ShapeDtypeStruct((D, VOCAB), jnp.float32),
        ],
        in_specs=[SMEM, SMEM] + [VMEM] * 5,
        out_specs=[VMEM] * 3,
        scratch_shapes=step_scratch(total, frames),
        compiler_params=pltpu.CompilerParams(vmem_limit_bytes=40 << 20),
        name="local_step",
    )(frame_lens, label_lens, features, labels, up_mat, down_mat, out_mat)


class Sum:
    def __init__(self, me, devices, grads, received, staged, send_sem, recv_sem):
        self.me, self.grads, self.received, self.staged = me, grads, received, staged
        self.send_sem, self.recv_sem = send_sem, recv_sem
        self.orders = [order[::-1] for order in bit_orders(devices)]
        self.steps = len(self.orders[0])
        self.copies = [{}, {}, {}]

    def sum_of(self, which, place, pattern, stage):
        value = self.grads[which][place]
        for bit in self.orders[which][:stage]:
            self.copies[which][pattern + bit].wait_recv()
            value = value + self.received[which][pattern + bit]
        return value

    def send(self, which, stage):
        order = self.orders[which]
        for offset in subsets(order[stage + 1 :][::-1])[::-1]:
            slot = offset + order[stage]
            place = place_with(self.me, order, slot)
            if stage == 0:
                source = self.grads[which].at[place]
            else:
                self.staged[which][slot] = self.sum_of(which, place, slot, stage)
                source = self.staged[which].at[slot]
            copy = pltpu.make_async_remote_copy(
                src_ref=source,
                dst_ref=self.received[which].at[slot],
                send_sem=self.send_sem.at[which, slot],
                recv_sem=self.recv_sem.at[which, slot],
                device_id=(flip(self.me, order[stage]),),
                device_id_type=MESH,
            )
            copy.start()
            self.copies[which][slot] = copy

    def finish(self, devices, reduced, squares, own_squares, small_send, small_recv):
        me = self.me
        own = jnp.zeros((1, LANES), jnp.float32)
        for which in (2, 1, 0):
            value = self.sum_of(which, me, 0, self.steps)
            rows, width = value.shape
            parts = width // LANES
            for part in range(parts):
                piece = value[:, part * LANES : (part + 1) * LANES]
                reduced[which][pl.ds(part, rows, stride=parts), :] = piece
                own = own + jnp.sum(piece * piece, axis=0, keepdims=True)
        own_squares[...] = own
        squares[0] = own

        def small_copy(shift):
            return pltpu.make_async_remote_copy(
                src_ref=own_squares,
                dst_ref=squares.at[shift],
                send_sem=small_send.at[shift],
                recv_sem=small_recv.at[shift],
                device_id=((me + shift) % devices,),
                device_id_type=MESH,
            )

        @pl.loop(1, devices)
        def _(shift):
            small_copy(shift).start()

        for copies in self.copies:
            for copy in copies.values():
                copy.wait_send()

        @pl.loop(1, devices)
        def _(shift):
            small_copy(shift).wait()


def chunks(blocks):
    if blocks >= 4:
        return [blocks // 4, blocks // 4, blocks // 2]
    return [1] * blocks


def sum_groups(steps):
    groups, sems = [], 0
    for stage in range(steps):
        sizes = chunks(1 << (steps - 1 - stage))
        groups.append((sems, sizes))
        sems += len(sizes)
    return groups, sems


class GroupSum:
    def __init__(self, me, devices, grads, received, staged, send_sem, recv_sem):
        self.me, self.devices = me, devices
        self.grads, self.received, self.staged = grads, received, staged
        self.send_sem, self.recv_sem = send_sem, recv_sem
        self.orders = [order[::-1] for order in bit_orders(devices)]
        self.steps = len(self.orders[0])
        self.groups, _ = sum_groups(self.steps)
        self.seen = set()

    def slots(self, which, stage):
        order = self.orders[which]
        return [
            offset + order[stage] for offset in subsets(order[stage + 1 :][::-1])[::-1]
        ]

    def sem_at(self, which, stage, slot):
        at = self.slots(which, stage).index(slot)
        sem, sizes = self.groups[stage]
        for size in sizes:
            if at < size:
                return sem, size
            at, sem = at - size, sem + 1

    def sum_of(self, which, place, pattern, stage):
        value = self.grads[which][place]
        for at, bit in enumerate(self.orders[which][:stage]):
            sem, size = self.sem_at(which, at, pattern + bit)
            if (which, sem) not in self.seen:
                self.seen.add((which, sem))
                drain(
                    self.received[which], size, self.send_sem.at[which],
                    self.recv_sem.at[which, sem], flip(self.me, bit),
                ).wait_recv()
            value = value + self.received[which][pattern + bit]
        return value

    def send(self, which, stage):
        order = self.orders[which]
        for slot in self.slots(which, stage):
            place = place_with(self.me, order, slot)
            if stage == 0:
                source = self.grads[which].at[place]
            else:
                self.staged[which][slot] = self.sum_of(which, place, slot, stage)
                source = self.staged[which].at[slot]
            pltpu.make_async_remote_copy(
                src_ref=source,
                dst_ref=self.received[which].at[slot],
                send_sem=self.send_sem.at[which],
                recv_sem=self.recv_sem.at[which, self.sem_at(which, stage, slot)[0]],
                device_id=(flip(self.me, order[stage]),),
                device_id_type=MESH,
            ).start()

    def finish(self, reduced, squares, own_squares, small_send, small_recv):
        me, devices = self.me, self.devices
        own = jnp.zeros((1, LANES), jnp.float32)
        for which in (2, 1, 0):
            value = self.sum_of(which, me, 0, self.steps)
            rows, width = value.shape
            parts = width // LANES
            for part in range(parts):
                piece = value[:, part * LANES : (part + 1) * LANES]
                reduced[which][pl.ds(part, rows, stride=parts), :] = piece
                own = own + jnp.sum(piece * piece, axis=0, keepdims=True)
        own_squares[...] = own
        squares[0] = own

        @pl.loop(1, devices)
        def _(shift):
            pltpu.make_async_remote_copy(
                src_ref=own_squares,
                dst_ref=squares.at[shift],
                send_sem=small_send,
                recv_sem=small_recv,
                device_id=((me + shift) % devices,),
                device_id_type=MESH,
            ).start()

        for which in range(3):
            drain(
                self.received[which], devices - 1, self.send_sem.at[which],
                self.recv_sem.at[which, 0], flip(me, 1),
            ).wait_send()
        small = drain(squares, devices - 1, small_send, small_recv, flip(me, 1))
        small.wait_send()
        small.wait_recv()


def sum_kernel(devices, *refs):
    grads, reduced, squares = refs[:3], refs[3:6], refs[6]
    received, staged = refs[7:10], refs[10:13]
    own_squares, send_sem, recv_sem, small_send, small_recv = refs[13:]
    me = lax.axis_index("dp")
    barrier = pltpu.get_barrier_semaphore()
    greet(me, devices, barrier)
    pl.semaphore_wait(barrier, devices - 1)
    total = Sum(me, devices, grads, received, staged, send_sem, recv_sem)
    for stage in range(total.steps):
        for which in range(3):
            total.send(which, stage)
    total.finish(devices, reduced, squares, own_squares, small_send, small_recv)


def fused_kernel(devices, loss_scale, *refs):
    frame_lens, label_lens, features, labels = refs[:4]
    shards, reduced, squares = refs[4:7], refs[7:10], refs[10]
    fulls, grads, received, staged = refs[11:14], refs[14:17], refs[17:20], refs[20:23]
    gather_send, gather_recv, own_squares, send_sem, recv_sem, small_send, small_recv = refs[23:30]
    normalized, activation, hidden, block_out, log_probs = refs[30:35]
    logit_grad, ff_grad, act_grad, emitted, emitted_blank = refs[35:40]
    alpha_rows, beta_rows = refs[40:44], refs[44:48]
    held, load_sem = refs[48:52], refs[52]
    up_mat, down_mat, out_mat = fulls
    me = lax.axis_index("dp")
    loads = [
        pltpu.make_async_copy(source, target, load_sem.at[at])
        for at, (source, target) in enumerate(zip((*shards, features), held))
    ]
    for load in loads:
        load.start()
    shards, features = held[:3], held[3]
    barrier = pltpu.get_barrier_semaphore()
    greet_partners(me, devices, barrier)
    gather = GroupGather(me, devices, fulls, gather_send, gather_recv)
    for load in loads[:3]:
        load.wait()
    gather.fill(shards)
    loads[3].wait()
    normalize(features, normalized)
    pl.semaphore_wait(barrier, gather.steps)
    gather.pass_on()
    gather.arrive(0)
    project_up(normalized, up_mat, activation, hidden)
    gather.arrive(1)
    gather.arrive(2)
    project_down(features, hidden, down_mat, out_mat, block_out, log_probs)
    ctc_grad(
        loss_scale, frame_lens, label_lens, labels, log_probs, emitted, emitted_blank, alpha_rows,
        beta_rows, logit_grad,
    )
    total = GroupSum(me, devices, grads, received, staged, send_sem, recv_sem)
    pending = [list(range(total.steps)) for _ in range(3)]

    def advance(*whiches):
        for which in whiches:
            if pending[which]:
                total.send(which, pending[which].pop(0))

    def put(which, value):
        grads[which][...] = value.reshape(grads[which].shape)

    grad_ff(logit_grad, out_mat, ff_grad)
    put(1, dot_first(hidden[...], ff_grad[...]))
    advance(1)
    grad_act(ff_grad, down_mat, activation, act_grad)
    advance(1)
    put(0, dot_first(normalized[...], act_grad[...]))
    advance(0)
    put(2, dot_first(block_out[...], logit_grad[...]))
    advance(2)
    while any(pending):
        advance(1, 0, 2)
    total.finish(reduced, squares, own_squares, small_send, small_recv)
    gather.close()


def fused_step(loss_scale, devices, frame_lens, label_lens, features, labels, weights):
    total = features.shape[0]
    frames = total // labels.shape[0]
    blocks = [
        (devices, weight.size // width, width)
        for weight, width in zip(weights, (FF, D, VOCAB))
    ]
    wide = [pltpu.VMEM(block, jnp.float32) for block in blocks]
    return pl.pallas_call(
        functools.partial(fused_kernel, devices, loss_scale),
        out_shape=[jax.ShapeDtypeStruct(weight.shape, jnp.float32) for weight in weights]
        + [jax.ShapeDtypeStruct((devices, 1, LANES), jnp.float32)],
        in_specs=[SMEM, SMEM, HBM, VMEM] + [HBM] * 3,
        out_specs=[VMEM] * 4,
        scratch_shapes=[pltpu.VMEM(block, jnp.bfloat16) for block in blocks]
        + wide * 3
        + [
            pltpu.SemaphoreType.DMA((3,)),
            pltpu.SemaphoreType.DMA((3, gather_sems(devices))),
            pltpu.VMEM((1, LANES), jnp.float32),
            pltpu.SemaphoreType.DMA((3,)),
            pltpu.SemaphoreType.DMA((3, sum_groups(devices.bit_length() - 1)[1])),
            pltpu.SemaphoreType.DMA,
            pltpu.SemaphoreType.DMA,
        ]
        + step_scratch(total, frames)
        + [pltpu.VMEM(array.shape, array.dtype) for array in (*weights, features)]
        + [pltpu.SemaphoreType.DMA((4,))],
        compiler_params=pltpu.CompilerParams(
            collective_id=2, has_side_effects=True, vmem_limit_bytes=67043328
        ),
        name="fused_step",
    )(frame_lens, label_lens, features, labels, *weights)


def sum_gradients(devices, grads):
    blocks = [grad.reshape(devices, grad.shape[0] // devices, grad.shape[1]) for grad in grads]
    shapes = [
        jax.ShapeDtypeStruct((block[0].size // LANES, LANES), jnp.float32) for block in blocks
    ]
    buffers = [pltpu.VMEM(block.shape, jnp.float32) for block in blocks]
    return pl.pallas_call(
        functools.partial(sum_kernel, devices),
        out_shape=shapes + [jax.ShapeDtypeStruct((devices, 1, LANES), jnp.float32)],
        in_specs=[VMEM] * 3,
        out_specs=[VMEM] * 4,
        scratch_shapes=buffers
        + buffers
        + [
            pltpu.VMEM((1, LANES), jnp.float32),
            pltpu.SemaphoreType.DMA((3, devices)),
            pltpu.SemaphoreType.DMA((3, devices)),
            pltpu.SemaphoreType.DMA((devices,)),
            pltpu.SemaphoreType.DMA((devices,)),
        ],
        compiler_params=pltpu.CompilerParams(
            collective_id=1, has_side_effects=True, vmem_limit_bytes=50 << 20
        ),
        name="sum_gradients",
    )(*blocks)


def adam_kernel(squares, *refs):
    weights, firsts, seconds, grads, outs = (refs[at : at + 3] for at in (0, 3, 6, 9, 12))
    new_firsts, new_seconds = refs[15:18], refs[18:21]
    total = jnp.sum(squares[...])
    clip = 1.0 / jnp.maximum(jnp.sqrt(jnp.full((1, LANES), total)), 1.0)
    for which in range(3):
        scaled = clip * grads[which][...]
        first = 0.9 * firsts[which][...] + 0.1 * scaled
        second = 0.999 * seconds[which][...] + 0.001 * scaled * scaled
        ratio = first / first_correction / (jnp.sqrt(second / second_correction) + 1e-08)
        outs[which][...] = weights[which][...] - 0.001 * ratio
        new_firsts[which][...] = first
        new_seconds[which][...] = second


def adam(squares, weights, firsts, seconds, grads):
    shapes = [jax.ShapeDtypeStruct(weight.shape, jnp.float32) for weight in weights]
    return pl.pallas_call(
        adam_kernel,
        out_shape=shapes * 3,
        in_specs=[VMEM] * 13,
        out_specs=[VMEM] * 9,
        compiler_params=pltpu.CompilerParams(vmem_limit_bytes=67043328),
        name="adam",
    )(squares, *weights, *firsts, *seconds, *grads)


def per_device(
    features,
    frame_lens,
    labels,
    label_lens,
    w_up,
    w_down,
    w_out,
    first_up,
    first_down,
    first_out,
    second_up,
    second_down,
    second_out,
):
    devices = lax.axis_size("dp")
    batch, frames, width = features.shape

    def lined(*arrays):
        return [array.reshape(array.shape[0] // LANES, LANES) for array in arrays]

    weights = lined(w_up, w_down, w_out)
    loss_scale = 1.0 / (batch * devices)
    rows_in = features.reshape(batch * frames, width)
    if w_up.size % (8 * FF) == 0 and w_out.size % (8 * VOCAB) == 0:
        *shares, squares = fused_step(
            loss_scale, devices, frame_lens, label_lens, rows_in, labels, weights
        )
    else:
        full_up, full_down, full_out = gather_weights(devices, *weights)
        grads = local_step(
            loss_scale,
            frame_lens,
            label_lens,
            rows_in,
            labels,
            full_up.reshape(D, FF),
            full_down.reshape(FF, D),
            full_out.reshape(D, VOCAB),
        )
        *shares, squares = sum_gradients(devices, grads)
    results = adam(
        squares,
        weights,
        lined(first_up, first_down, first_out),
        lined(second_up, second_down, second_out),
        shares,
    )
    return tuple(result.reshape(-1) for result in results)


def solution(mesh):
    flat = P("dp")
    return jax.shard_map(
        per_device,
        mesh=mesh,
        in_specs=(P("dp", None, None), flat, P("dp", None), flat) + (flat,) * 9,
        out_specs=(flat,) * 9,
        check_vma=False,
    )
```

```python
import functools

import jax
import jax.numpy as jnp
from jax import lax
from jax.experimental import pallas as pl
from jax.experimental.pallas import tpu as pltpu
from jax.sharding import PartitionSpec as P

D = 256
FF = 1024
VOCAB = 256
LANES = 128
MESH = pl.DeviceIdType.MESH

first_correction = 1.0 - (0.9**10) ** 10
second_correction = 1.0 - (0.999**10) ** 10
negative = -1e30
LOG2E = 1.4426950408889634
PARTS = 2
VMEM = pl.BlockSpec(memory_space=pltpu.VMEM)
SMEM = pl.BlockSpec(memory_space=pltpu.SMEM)
HBM = pl.BlockSpec(memory_space=pltpu.HBM)


def flip(me, bit):
    return me + bit - 2 * bit * ((me // bit) % 2)


def bit_orders(devices):
    bits = [1 << k for k in range(devices.bit_length() - 1)]
    core, rest = bits[:1], bits[1:]
    down = rest[::-1]
    swapped = down[:-2] + down[-2:][::-1]
    turned = down[-2:] + down[:-2]
    return (down + core, swapped + core, turned + core)


def subsets(bits):
    offsets = [0]
    for bit in bits:
        offsets = offsets + [offset + bit for offset in offsets]
    return offsets


def place_with(me, free, pattern):
    place = me
    for bit in free:
        if pattern & bit:
            place = flip(place, bit)
    return place


class Gather:
    def __init__(self, me, devices, fulls, send_sem, recv_sem):
        self.me, self.fulls = me, fulls
        self.send_sem, self.recv_sem = send_sem, recv_sem
        self.orders = bit_orders(devices)
        self.steps = len(self.orders[0])
        self.copies = [{}, {}, {}]

    def fill(self, shards):
        for shard, full in zip(shards, self.fulls):
            rows, width = full.shape[1:]
            parts = width // LANES
            for part in range(parts):
                full[self.me, :, part * LANES : (part + 1) * LANES] = shard[
                    pl.ds(part, rows, stride=parts), :
                ].astype(jnp.bfloat16)

    def send(self, which, pattern, stage):
        order, full = self.orders[which], self.fulls[which]
        owner = place_with(self.me, order[:stage], pattern)
        slot = pattern + order[stage]
        copy = pltpu.make_async_remote_copy(
            src_ref=full.at[owner],
            dst_ref=full.at[owner],
            send_sem=self.send_sem.at[which, slot],
            recv_sem=self.recv_sem.at[which, slot],
            device_id=(flip(self.me, order[stage]),),
            device_id_type=MESH,
        )
        copy.start()
        self.copies[which][slot] = copy

    def pass_on(self):
        for which in range(3):
            for stage in range(self.steps):
                self.send(which, 0, stage)
        for stage in range(self.steps - 1):
            for at in range(1 << stage):
                for which in range(3):
                    order = self.orders[which]
                    pattern = subsets(order[:stage])[at] + order[stage]
                    self.copies[which][pattern].wait_recv()
                    for later in range(stage + 1, self.steps):
                        self.send(which, pattern, later)

    def arrive(self, which):
        order = self.orders[which]
        for pattern in subsets(order[:-1]):
            self.copies[which][pattern + order[-1]].wait_recv()

    def close(self):
        for copies in self.copies:
            for copy in copies.values():
                copy.wait_send()


def drain(ref, blocks, send_sem, recv_sem, peer):
    return pltpu.make_async_remote_copy(
        src_ref=ref.at[pl.ds(0, blocks)],
        dst_ref=ref.at[pl.ds(0, blocks)],
        send_sem=send_sem,
        recv_sem=recv_sem,
        device_id=(peer,),
        device_id_type=MESH,
    )


def flat(stages):
    return [bit for stage in stages for bit in stage]


def move(me, offset, bits):
    return place_with(me, bits, offset)


class StagedGather:
    def __init__(self, me, plans, fulls, send_sem, recv_sem):
        self.me, self.plans, self.fulls = me, plans, fulls
        self.send_sem, self.recv_sem = send_sem, recv_sem
        self.units = [gather_units(plan) for plan in plans]

    def fill(self, shards):
        for shard, full in zip(shards, self.fulls):
            rows, width = full.shape[1:]
            parts = width // LANES
            for part in range(parts):
                full[self.me, :, part * LANES : (part + 1) * LANES] = shard[
                    pl.ds(part, rows, stride=parts), :
                ].astype(jnp.bfloat16)

    def send(self, which, source, first):
        plan, full = self.plans[which], self.fulls[which]
        for stage in range(first, len(plan)):
            for offset in subsets(plan[stage])[1:][::-1]:
                sem = self.units[which][1][stage, offset, source]
                peer = move(self.me, offset, plan[stage])
                for pattern in self.units[which][0][source][0] if source else [0]:
                    owner = move(self.me, pattern, flat(plan[:stage]))
                    pltpu.make_async_remote_copy(
                        src_ref=full.at[owner],
                        dst_ref=full.at[owner],
                        send_sem=self.send_sem.at[which],
                        recv_sem=self.recv_sem.at[which, sem],
                        device_id=(peer,),
                        device_id_type=MESH,
                    ).start()

    def drain(self, which, blocks, at):
        return drain(
            self.fulls[which], blocks, self.send_sem.at[which], self.recv_sem.at[which, at],
            flip(self.me, 1),
        )

    def pass_on(self):
        for which in range(3):
            self.send(which, None, 0)
        names = [list(units[0]) for units in self.units]
        for at in range(max(len(some) for some in names)):
            for which in range(3):
                if at < len(names[which]):
                    name = names[which][at]
                    patterns, sem = self.units[which][0][name]
                    self.drain(which, len(patterns), sem).wait_recv()
                    self.send(which, name, name[0] + 1)

    def arrive(self, which):
        before = 1 << len(flat(self.plans[which][:-1]))
        self.drain(which, before, self.units[which][2] - 1).wait_recv()

    def close(self):
        for which in range(3):
            before = 1 << len(flat(self.plans[which]))
            self.drain(which, before - 1, 0).wait_send()


def gather_units(plan):
    units, sems, count = {}, {}, 0
    for stage, bits in enumerate(plan):
        sources = {None: [0], **{name: patterns for name, (patterns, _) in units.items()}}
        for name, patterns in sources.items():
            for offset in subsets(bits)[1:]:
                sems[stage, offset, name] = count
                if stage < len(plan) - 1:
                    units[stage, offset, name] = ([offset + at for at in patterns], count)
                    count += 1
    return units, sems, count + 1


def greet_stages(me, plan, barrier):
    for bits in plan:
        for offset in subsets(bits)[1:]:
            pl.semaphore_signal(
                barrier, inc=1, device_id=(move(me, offset, bits),), device_id_type=MESH
            )


def stage_partners(plan):
    return sum((1 << len(bits)) - 1 for bits in plan)


def greet(me, devices, barrier):
    @pl.loop(1, devices)
    def _(shift):
        pl.semaphore_signal(
            barrier, inc=1, device_id=((me + shift) % devices,), device_id_type=MESH
        )


def gather_kernel(devices, w_up, w_down, w_out, full_up, full_down, full_out, send_sem, recv_sem):
    me = lax.axis_index("dp")
    barrier = pltpu.get_barrier_semaphore()
    greet(me, devices, barrier)
    gather = Gather(me, devices, (full_up, full_down, full_out), send_sem, recv_sem)
    gather.fill((w_up, w_down, w_out))
    pl.semaphore_wait(barrier, devices - 1)
    gather.pass_on()
    for which in range(3):
        gather.arrive(which)
    gather.close()


def gather_weights(devices, w_up, w_down, w_out):
    shapes = []
    for shard, width in ((w_up, FF), (w_down, D), (w_out, VOCAB)):
        shapes.append(
            jax.ShapeDtypeStruct((devices, shard.size // width, width), jnp.bfloat16)
        )
    return pl.pallas_call(
        functools.partial(gather_kernel, devices),
        out_shape=shapes,
        in_specs=[VMEM] * 3,
        out_specs=[VMEM] * 3,
        scratch_shapes=[
            pltpu.SemaphoreType.DMA((3, devices)),
            pltpu.SemaphoreType.DMA((3, devices)),
        ],
        compiler_params=pltpu.CompilerParams(collective_id=0, has_side_effects=True),
        name="gather_weights",
    )(w_up, w_down, w_out)


def dot_rows(left, right):
    return jnp.dot(left, right, preferred_element_type=jnp.float32)


def dot_last(left, right, precision=None):
    return lax.dot_general(
        left, right, (((1,), (1,)), ((), ())), precision=precision,
        preferred_element_type=jnp.float32,
    )


def dot_first(left, right):
    return lax.dot_general(
        left, right, (((0,), (0,)), ((), ())), preferred_element_type=jnp.float32
    )


def row_blocks(total, body):
    block = min(128, total)

    @pl.loop(0, total // block)
    def _(step):
        body(pl.ds(pl.multiple_of(step * block, block), block))


def normalize(features, normalized):
    def body(rows):
        flat_in = features[rows, :].astype(jnp.float32)
        centre = jnp.mean(flat_in, axis=1, keepdims=True)
        shifted = flat_in - centre
        spread = jnp.mean(shifted * shifted, axis=1, keepdims=True)
        normalized[rows, :] = (shifted * lax.rsqrt(spread + 1e-05)).astype(jnp.bfloat16)

    row_blocks(features.shape[0], body)


def project_up(normalized, up_mat, activation, hidden):
    def body(rows):
        act = dot_rows(normalized[rows, :], up_mat[...].reshape(D, FF))
        activation[rows, :] = act
        hidden[rows, :] = (act * (1.0 / (1.0 + jnp.exp(-act)))).astype(jnp.bfloat16)

    row_blocks(normalized.shape[0], body)


def project_down(features, hidden, down_mat, out_mat, block_out, log_probs):
    def body(rows):
        flat_in = features[rows, :].astype(jnp.float32)
        out_rows = (flat_in + 0.5 * dot_rows(hidden[rows, :], down_mat[...].reshape(FF, D))).astype(
            jnp.bfloat16
        )
        block_out[rows, :] = out_rows
        logits = dot_rows(out_rows, out_mat[...].reshape(D, VOCAB))
        top = jnp.max(logits, axis=1, keepdims=True)
        low = (logits - top) * LOG2E
        log_probs[rows, :] = low - jnp.log2(jnp.sum(jnp.exp2(low), axis=1, keepdims=True))

    row_blocks(features.shape[0], body)


def split_dot(dot, values, picks):
    high = values.astype(jnp.bfloat16)
    rest = values - high.astype(jnp.float32)
    middle = rest.astype(jnp.bfloat16)
    low = (rest - middle.astype(jnp.float32)).astype(jnp.bfloat16)
    return dot(high, picks) + (dot(middle, picks) + dot(low, picks))


def ctc_rows(frames):
    return [pltpu.VMEM((frames, 8, LANES), jnp.float32)] * 4 + [
        pltpu.VMEM((2 * frames, 8, LANES), jnp.float32)
    ] * 4


class Lattice:
    def __init__(self, parts, sign, skip):
        self.parts, self.sign = parts, sign
        self.row = 0 if sign > 0 else 7
        self.skips = [self.spread(skip, part) > 0.5 for part in range(parts)]

    def spread(self, values, part):
        if self.sign > 0:
            return pltpu.roll(values, part, 1, stride=self.parts, stride_axis=0)
        shift = LANES - part - 7 * self.parts
        return pltpu.roll(values, shift, 1, stride=self.parts, stride_axis=0)

    def begin(self, blank, label):
        def whole(values):
            return jnp.broadcast_to(values[self.row : self.row + 1], (8, LANES))

        blank, label = whole(blank), whole(label)
        self.blank = [self.spread(blank, part) for part in range(self.parts)]
        self.label = [self.spread(label, part) for part in range(self.parts + 1)]
        one = jnp.ones((8, LANES), jnp.float32)
        self.blank_mass, self.label_mass = [one] * self.parts, [one] * (self.parts + 1)

    def next_rows(self, values):
        return pltpu.roll(values, 7 if self.sign > 0 else 1, 0)

    def advance(self, emit_blank, emit_label, parts):
        blank, label, blank_mass, label_mass = [], [], [], []
        for part in range(parts):
            b, l, l1 = self.blank[part], self.label[part], self.label[part + 1]
            bm, lm, lm1 = self.blank_mass[part], self.label_mass[part], self.label_mass[part + 1]
            top = jnp.maximum(b, l1)
            mass = bm * jnp.exp2(b - top) + lm1 * jnp.exp2(l1 - top)
            above = jnp.where(self.skips[part], top, b)
            above_mass = jnp.where(self.skips[part], mass, bm)
            peak = jnp.maximum(l, above)
            peak_mass = lm * jnp.exp2(l - peak) + above_mass * jnp.exp2(above - peak)
            if part == 0:
                result = (top, mass, peak, peak_mass)
            blank.append(top + emit_blank)
            label.append(peak + self.spread(emit_label, part))
            blank_mass.append(mass)
            label_mass.append(peak_mass)
        if parts == self.parts:
            label.append(self.next_rows(label[0]))
            label_mass.append(self.next_rows(label_mass[0]))
        self.blank, self.label = blank, label
        self.blank_mass, self.label_mass = blank_mass, label_mass
        return result


def ctc_grad(
    loss_scale,
    frame_lens,
    label_lens,
    labels,
    log_probs,
    emitted,
    emitted_blank,
    alpha_rows,
    beta_rows,
    logit_grad,
):
    utterances, label_count = labels.shape
    frames = log_probs.shape[0] // utterances
    half = LANES // utterances
    depth = 8 * PARTS
    assert label_count + depth <= half and frames % depth == 0

    lane_row = lax.broadcasted_iota(jnp.int32, (8, LANES), 1)
    label_ids = lax.broadcasted_iota(jnp.int32, (label_count, LANES), 0)
    spread_lanes = lax.broadcasted_iota(jnp.int32, (label_count, LANES), 1)
    label_rows = jnp.concatenate(
        [
            labels[...].astype(jnp.float32),
            jnp.zeros((8 - utterances, label_count), jnp.float32),
        ],
        axis=0,
    ).astype(jnp.bfloat16)
    extended = jnp.zeros((8, LANES), jnp.float32)
    for utterance in range(utterances):
        spread = (spread_lanes == label_ids + half * utterance + 1).astype(jnp.bfloat16)
        placed = dot_rows(label_rows, spread)[utterance : utterance + 1]
        extended = extended + jnp.broadcast_to(placed, (8, LANES))
    skip = jnp.where(extended != pltpu.roll(extended, 1, 1), 1.0, 0.0)
    skip_back = pltpu.roll(skip, LANES - 1, 1)

    vocab_ids = lax.broadcasted_iota(jnp.int32, (VOCAB, LANES), 0).astype(jnp.float32)
    vocab_lanes = lax.broadcasted_iota(jnp.int32, (VOCAB, LANES), 1)
    frame_lanes = lax.broadcasted_iota(jnp.int32, (frames, LANES), 1)
    onehots = []
    picked = None
    blanks = None
    for utterance in range(utterances):
        rows = slice(utterance * frames, (utterance + 1) * frames)
        first = half * utterance + 1
        mine = (vocab_lanes >= first) & (vocab_lanes < first + label_count)
        onehot = jnp.where((vocab_ids == extended[0:1, :]) & mine, 1.0, 0.0).astype(jnp.bfloat16)
        onehots.append(onehot)
        picks = split_dot(dot_rows, log_probs[rows, :], onehot)
        blank = jnp.broadcast_to(log_probs[rows, 0:1], (frames, LANES))
        if utterance == 0:
            picked, blanks = picks, blank
        else:
            picked = jnp.where(frame_lanes < half * utterance, picked, picks)
            blanks = jnp.where(frame_lanes < half * utterance, blanks, blank)
    place = frame_lanes % half
    emitted[...] = jnp.where((place >= 1) & (place <= label_count), picked, negative)
    emitted_blank[...] = blanks

    forward = Lattice(PARTS, 1, skip)
    backward = Lattice(PARTS, -1, skip_back)
    start = jnp.full((8, LANES), negative, jnp.float32)
    start_back = start
    for utterance in range(utterances):
        first = half * utterance + 1
        start = jnp.where(lane_row == first, 0.0, start)
        start_back = jnp.where(
            lane_row == first + label_lens[utterance] - 1, 0.0, start_back
        )
    nothing = jnp.full((8, LANES), negative, jnp.float32)

    def row_of(ref, frame):
        return jnp.broadcast_to(ref[pl.ds(frame, 1), :], (8, LANES))

    def block(at, carry):
        forward.begin(*carry[:2])
        backward.begin(*carry[2:])
        for level in range(depth):
            frame = at * depth + level
            needed = min(PARTS, depth - level)
            result = forward.advance(row_of(emitted_blank, frame), row_of(emitted, frame), needed)
            for ref, value in zip(alpha_rows, result):
                ref[frame] = value
            emit = emit_blank = None
            for utterance in range(utterances):
                back = jnp.maximum(frame_lens[utterance] - 1 - frame, 0)
                mine, mine_blank = row_of(emitted, back), row_of(emitted_blank, back)
                if utterance == 0:
                    emit, emit_blank = mine, mine_blank
                else:
                    emit = jnp.where(lane_row < half * utterance, emit, mine)
                    emit_blank = jnp.where(lane_row < half * utterance, emit_blank, mine_blank)
            result = backward.advance(emit_blank, emit, needed)
            for ref, value in zip(beta_rows, result):
                ref[frames - 1 - frame] = value
        return tuple(
            values[0] + jnp.log2(mass[0])
            for lattice in (forward, backward)
            for values, mass in (
                (lattice.blank, lattice.blank_mass), (lattice.label, lattice.label_mass)
            )
        )

    lax.fori_loop(0, frames // depth, block, (start, nothing, start_back, nothing))

    frame_ids = lax.broadcasted_iota(jnp.int32, (frames, LANES), 0)
    alphas = [ref[:, forward.row, :] for ref in alpha_rows]
    betas, alive = [], None
    for ref in beta_rows:
        value = None
        for utterance in range(utterances):
            mine = ref[pl.ds(frames - frame_lens[utterance], frames), backward.row, :]
            value = mine if value is None else jnp.where(frame_lanes < half * utterance, value, mine)
        betas.append(value)
    betas[0], betas[1] = pltpu.roll(betas[0], 1, 1), pltpu.roll(betas[1], 1, 1)
    joint_blank = alphas[0] + emitted_blank[...] + betas[0]
    joint_label = alphas[2] + emitted[...] + betas[2]
    blank_mass, label_mass = alphas[1] * betas[1], alphas[3] * betas[3]
    both = jnp.maximum(joint_blank, joint_label)
    for utterance in range(utterances):
        rows = slice(utterance * frames, (utterance + 1) * frames)
        first = half * utterance
        mine = (frame_lanes >= first) & (frame_lanes < first + half)
        top = jnp.max(jnp.where(mine, both, negative), axis=1, keepdims=True)
        live = mine & (frame_ids < frame_lens[utterance])
        label = jnp.where(live, label_mass * jnp.exp2(joint_label - top), 0.0)
        blank = jnp.where(live, blank_mass * jnp.exp2(joint_blank - top), 0.0)
        blank_sum = jnp.sum(blank, axis=1, keepdims=True)
        total = jnp.sum(label, axis=1, keepdims=True) + blank_sum
        kept = frame_ids[:, 0:1] < frame_lens[utterance]
        scale = jnp.where(kept, 1.0 / jnp.where(kept, total, 1.0), 0.0)
        gamma = split_dot(dot_last, label * scale, onehots[utterance])
        vocab_at = lax.broadcasted_iota(jnp.int32, (frames, VOCAB), 1)
        gamma = gamma + jnp.where(vocab_at == 0, blank_sum * scale, 0.0)
        probs = jnp.exp2(log_probs[rows, :]) * jnp.where(kept, 1.0, 0.0)
        logit_grad[rows, :] = (loss_scale * (probs - gamma)).astype(jnp.bfloat16)


def grad_ff(logit_grad, out_mat, ff_grad):
    def body(rows):
        ff_grad[rows, :] = (
            0.5 * dot_last(logit_grad[rows, :], out_mat[...].reshape(D, VOCAB))
        ).astype(jnp.bfloat16)

    row_blocks(logit_grad.shape[0], body)


def grad_act(ff_grad, down_mat, activation, act_grad):
    def body(rows):
        act = activation[rows, :]
        sigmoid = 1.0 / (1.0 + jnp.exp(-act))
        slope = sigmoid * (1.0 + act * (1.0 - sigmoid))
        act_grad[rows, :] = (
            dot_last(ff_grad[rows, :], down_mat[...].reshape(FF, D)) * slope
        ).astype(jnp.bfloat16)

    row_blocks(ff_grad.shape[0], body)


def step_kernel(
    loss_scale,
    frame_lens,
    label_lens,
    features,
    labels,
    up_mat,
    down_mat,
    out_mat,
    grad_up,
    grad_down,
    grad_out,
    normalized,
    activation,
    hidden,
    block_out,
    log_probs,
    logit_grad,
    ff_grad,
    act_grad,
    emitted,
    emitted_blank,
    *lattice_rows,
):
    normalize(features, normalized)
    project_up(normalized, up_mat, activation, hidden)
    project_down(features, hidden, down_mat, out_mat, block_out, log_probs)
    ctc_grad(
        loss_scale, frame_lens, label_lens, labels, log_probs, emitted, emitted_blank,
        lattice_rows[:4], lattice_rows[4:], logit_grad,
    )
    grad_ff(logit_grad, out_mat, ff_grad)
    grad_act(ff_grad, down_mat, activation, act_grad)
    grad_up[...] = dot_first(normalized[...], act_grad[...])
    grad_down[...] = dot_first(hidden[...], ff_grad[...])
    grad_out[...] = dot_first(block_out[...], logit_grad[...])


def step_scratch(total, frames):
    return [
        pltpu.VMEM((total, D), jnp.bfloat16),
        pltpu.VMEM((total, FF), jnp.float32),
        pltpu.VMEM((total, FF), jnp.bfloat16),
        pltpu.VMEM((total, D), jnp.bfloat16),
        pltpu.VMEM((total, VOCAB), jnp.float32),
        pltpu.VMEM((total, VOCAB), jnp.bfloat16),
        pltpu.VMEM((total, D), jnp.bfloat16),
        pltpu.VMEM((total, FF), jnp.bfloat16),
        pltpu.VMEM((frames, LANES), jnp.float32),
        pltpu.VMEM((frames, LANES), jnp.float32),
    ] + ctc_rows(frames)


def local_step(loss_scale, frame_lens, label_lens, features, labels, up_mat, down_mat, out_mat):
    total = features.shape[0]
    frames = total // labels.shape[0]
    return pl.pallas_call(
        functools.partial(step_kernel, loss_scale),
        out_shape=[
            jax.ShapeDtypeStruct((D, FF), jnp.float32),
            jax.ShapeDtypeStruct((FF, D), jnp.float32),
            jax.ShapeDtypeStruct((D, VOCAB), jnp.float32),
        ],
        in_specs=[SMEM, SMEM] + [VMEM] * 5,
        out_specs=[VMEM] * 3,
        scratch_shapes=step_scratch(total, frames),
        compiler_params=pltpu.CompilerParams(vmem_limit_bytes=40 << 20),
        name="local_step",
    )(frame_lens, label_lens, features, labels, up_mat, down_mat, out_mat)


class Sum:
    def __init__(self, me, devices, grads, received, staged, send_sem, recv_sem):
        self.me, self.grads, self.received, self.staged = me, grads, received, staged
        self.send_sem, self.recv_sem = send_sem, recv_sem
        self.orders = [order[::-1] for order in bit_orders(devices)]
        self.steps = len(self.orders[0])
        self.copies = [{}, {}, {}]

    def sum_of(self, which, place, pattern, stage):
        value = self.grads[which][place]
        for bit in self.orders[which][:stage]:
            self.copies[which][pattern + bit].wait_recv()
            value = value + self.received[which][pattern + bit]
        return value

    def send(self, which, stage):
        order = self.orders[which]
        for offset in subsets(order[stage + 1 :][::-1])[::-1]:
            slot = offset + order[stage]
            place = place_with(self.me, order, slot)
            if stage == 0:
                source = self.grads[which].at[place]
            else:
                self.staged[which][slot] = self.sum_of(which, place, slot, stage)
                source = self.staged[which].at[slot]
            copy = pltpu.make_async_remote_copy(
                src_ref=source,
                dst_ref=self.received[which].at[slot],
                send_sem=self.send_sem.at[which, slot],
                recv_sem=self.recv_sem.at[which, slot],
                device_id=(flip(self.me, order[stage]),),
                device_id_type=MESH,
            )
            copy.start()
            self.copies[which][slot] = copy

    def finish(self, devices, reduced, squares, own_squares, small_send, small_recv):
        me = self.me
        own = jnp.zeros((1, LANES), jnp.float32)
        for which in (2, 1, 0):
            value = self.sum_of(which, me, 0, self.steps)
            rows, width = value.shape
            parts = width // LANES
            for part in range(parts):
                piece = value[:, part * LANES : (part + 1) * LANES]
                reduced[which][pl.ds(part, rows, stride=parts), :] = piece
                own = own + jnp.sum(piece * piece, axis=0, keepdims=True)
        own_squares[...] = own
        squares[0] = own

        def small_copy(shift):
            return pltpu.make_async_remote_copy(
                src_ref=own_squares,
                dst_ref=squares.at[shift],
                send_sem=small_send.at[shift],
                recv_sem=small_recv.at[shift],
                device_id=((me + shift) % devices,),
                device_id_type=MESH,
            )

        @pl.loop(1, devices)
        def _(shift):
            small_copy(shift).start()

        for copies in self.copies:
            for copy in copies.values():
                copy.wait_send()

        @pl.loop(1, devices)
        def _(shift):
            small_copy(shift).wait()


def sum_pieces(plan):
    pieces = {}
    for stage, bits in enumerate(plan):
        for offset in subsets(bits)[1:]:
            for after in subsets(plan[stage + 1]) if stage + 1 < len(plan) else [0]:
                pieces[stage, offset, after] = len(pieces)
    return pieces


class StagedSum:
    def __init__(self, me, plans, narrow, grads, received, staged, send_sem, recv_sem):
        self.me, self.plans, self.narrow = me, plans, narrow
        self.grads, self.received, self.staged = grads, received, staged
        self.send_sem, self.recv_sem = send_sem, recv_sem
        self.pieces = [sum_pieces(plan) for plan in plans]
        self.seen = set()

    def index(self, which, pattern):
        bits = flat(self.plans[which])
        return sum(1 << at for at, bit in enumerate(bits[::-1]) if pattern & bit)

    def wide(self, which, stage):
        return 3 * (stage in self.narrow[which]) + which

    def put(self, which, value):
        bits = flat(self.plans[which])[::-1]
        blocks, rows, width = self.grads[which].shape
        own = [(self.me // bit) % 2 for bit in bits]
        for block in range(blocks):
            slot = 0
            for at, bit in enumerate(bits):
                slot = slot + (1 << at) * (1 - own[at] if block & bit else own[at])
            self.grads[which][slot] = value[block * rows : (block + 1) * rows, :]

    def piece(self, which, stage, pattern):
        plan = self.plans[which]
        offset = sum(bit for bit in plan[stage] if pattern & bit)
        after = 0
        if stage + 1 < len(plan):
            after = sum(bit for bit in plan[stage + 1] if pattern & bit)
        return stage, offset, after

    def copy(self, which, name):
        stage, offset, after = name
        start = self.index(which, offset + after)
        blocks = pl.ds(start, 1 << len(flat(self.plans[which][stage + 2 :])))
        at = self.wide(which, stage)
        source = self.grads[which] if stage == 0 else self.staged[at]
        return pltpu.make_async_remote_copy(
            src_ref=source.at[blocks],
            dst_ref=self.received[at].at[blocks],
            send_sem=self.send_sem.at[at],
            recv_sem=self.recv_sem.at[which, self.pieces[which][name]],
            device_id=(move(self.me, offset, self.plans[which][stage]),),
            device_id_type=MESH,
        )

    def sum_of(self, which, pattern, stage):
        value = self.grads[which][self.index(which, pattern)]
        for earlier in range(stage):
            for offset in subsets(self.plans[which][earlier])[1:]:
                name = self.piece(which, earlier, pattern + offset)
                if (which, name) not in self.seen:
                    self.seen.add((which, name))
                    self.copy(which, name).wait_recv()
                slot = self.index(which, pattern + offset)
                value = value + self.received[self.wide(which, earlier)][slot].astype(jnp.float32)
        return value

    def send(self, which, stage):
        plan = self.plans[which]
        afters = subsets(plan[stage + 1])[::-1] if stage + 1 < len(plan) else [0]
        for after in afters:
            for offset in subsets(plan[stage])[1:][::-1]:
                if stage:
                    staged = self.staged[self.wide(which, stage)]
                    for later in subsets(flat(plan[stage + 2 :])):
                        pattern = offset + after + later
                        staged[self.index(which, pattern)] = self.sum_of(
                            which, pattern, stage
                        ).astype(staged.dtype)
                self.copy(which, (stage, offset, after)).start()

    def finish(self, devices, reduced, squares, own_squares, small_send, small_recv):
        me = self.me
        own = jnp.zeros((1, LANES), jnp.float32)
        for which in (2, 1, 0):
            value = self.sum_of(which, 0, len(self.plans[which]))
            rows, width = value.shape
            parts = width // LANES
            for part in range(parts):
                piece = value[:, part * LANES : (part + 1) * LANES]
                reduced[which][pl.ds(part, rows, stride=parts), :] = piece
                own = own + jnp.sum(piece * piece, axis=0, keepdims=True)
        own_squares[...] = own
        squares[0] = own

        @pl.loop(1, devices)
        def _(shift):
            pltpu.make_async_remote_copy(
                src_ref=own_squares,
                dst_ref=squares.at[shift],
                send_sem=small_send,
                recv_sem=small_recv,
                device_id=((me + shift) % devices,),
                device_id_type=MESH,
            ).start()

        for which, plan in enumerate(self.plans):
            sent = {}
            for stage, bits in enumerate(plan):
                blocks = ((1 << len(bits)) - 1) << len(flat(plan[stage + 1 :]))
                at = self.wide(which, stage)
                sent[at] = sent.get(at, 0) + blocks
            for at, blocks in sent.items():
                drain(
                    self.received[at], blocks, self.send_sem.at[at], self.recv_sem.at[which, 0],
                    flip(me, 1),
                ).wait_send()
        small = drain(squares, devices - 1, small_send, small_recv, flip(me, 1))
        small.wait_send()
        small.wait_recv()


def sum_kernel(devices, *refs):
    grads, reduced, squares = refs[:3], refs[3:6], refs[6]
    received, staged = refs[7:10], refs[10:13]
    own_squares, send_sem, recv_sem, small_send, small_recv = refs[13:]
    me = lax.axis_index("dp")
    barrier = pltpu.get_barrier_semaphore()
    greet(me, devices, barrier)
    pl.semaphore_wait(barrier, devices - 1)
    total = Sum(me, devices, grads, received, staged, send_sem, recv_sem)
    for stage in range(total.steps):
        for which in range(3):
            total.send(which, stage)
    total.finish(devices, reduced, squares, own_squares, small_send, small_recv)


def exchange_plans(devices):
    bits = [1 << k for k in range(devices.bit_length() - 1)]
    core, near, far = bits[:1], bits[1:3], bits[3:]
    gathers = ([far, near, core], [far, near, core], [near, far, core])
    sums = ([core, near, far], [core, near, far], [core, far, near])
    narrow = ((1, 2), (1,), (1,))
    return gathers, sums, narrow


def meet_plan(devices):
    bits = [1 << k for k in range(devices.bit_length() - 1)]
    core, near, far = bits[:1], bits[1:3], bits[3:]
    return [core, near, far]


def fused_kernel(devices, loss_scale, *refs):
    frame_lens, label_lens, features, labels = refs[:4]
    shards, reduced, squares = refs[4:7], refs[7:10], refs[10]
    fulls, grads, received, staged = refs[11:14], refs[14:17], refs[17:23], refs[23:29]
    gather_send, gather_recv, own_squares, send_sem, recv_sem, small_send, small_recv = refs[29:36]
    normalized, activation, hidden, block_out, log_probs = refs[36:41]
    logit_grad, ff_grad, act_grad, emitted, emitted_blank = refs[41:46]
    alpha_rows, beta_rows = refs[46:50], refs[50:54]
    held, load_sem = refs[54:58], refs[58]
    up_mat, down_mat, out_mat = fulls
    me = lax.axis_index("dp")
    loads = [
        pltpu.make_async_copy(source, target, load_sem.at[at])
        for at, (source, target) in enumerate(zip((*shards, features), held))
    ]
    for load in loads:
        load.start()
    shards, features = held[:3], held[3]
    barrier = pltpu.get_barrier_semaphore()
    gathers, sums, narrow = exchange_plans(devices)
    greet_stages(me, meet_plan(devices), barrier)
    gather = StagedGather(me, gathers, fulls, gather_send, gather_recv)
    for load in loads[:3]:
        load.wait()
    gather.fill(shards)
    loads[3].wait()
    normalize(features, normalized)
    pl.semaphore_wait(barrier, stage_partners(meet_plan(devices)))
    gather.pass_on()
    gather.arrive(0)
    project_up(normalized, up_mat, activation, hidden)
    gather.arrive(1)
    gather.arrive(2)
    project_down(features, hidden, down_mat, out_mat, block_out, log_probs)
    ctc_grad(
        loss_scale, frame_lens, label_lens, labels, log_probs, emitted, emitted_blank, alpha_rows,
        beta_rows, logit_grad,
    )
    total = StagedSum(me, sums, narrow, grads, received, staged, send_sem, recv_sem)
    pending = [list(range(len(plan))) for plan in sums]

    def advance(*whiches):
        for which in whiches:
            if pending[which]:
                total.send(which, pending[which].pop(0))

    grad_ff(logit_grad, out_mat, ff_grad)
    total.put(1, dot_first(hidden[...], ff_grad[...]))
    advance(1)
    grad_act(ff_grad, down_mat, activation, act_grad)
    advance(1)
    total.put(0, dot_first(normalized[...], act_grad[...]))
    advance(0)
    total.put(2, dot_first(block_out[...], logit_grad[...]))
    advance(2)
    while any(pending):
        advance(1, 0, 2)
    total.finish(devices, reduced, squares, own_squares, small_send, small_recv)
    gather.close()


def fused_step(loss_scale, devices, frame_lens, label_lens, features, labels, weights):
    total = features.shape[0]
    frames = total // labels.shape[0]
    blocks = [
        (devices, weight.size // width, width)
        for weight, width in zip(weights, (FF, D, VOCAB))
    ]
    gathers, sums, _ = exchange_plans(devices)
    wide = [pltpu.VMEM(block, jnp.float32) for block in blocks]
    both = wide + [pltpu.VMEM(block, jnp.bfloat16) for block in blocks]
    return pl.pallas_call(
        functools.partial(fused_kernel, devices, loss_scale),
        out_shape=[jax.ShapeDtypeStruct(weight.shape, jnp.float32) for weight in weights]
        + [jax.ShapeDtypeStruct((devices, 1, LANES), jnp.float32)],
        in_specs=[SMEM, SMEM, HBM, VMEM] + [HBM] * 3,
        out_specs=[VMEM] * 4,
        scratch_shapes=[pltpu.VMEM(block, jnp.bfloat16) for block in blocks]
        + wide
        + both * 2
        + [
            pltpu.SemaphoreType.DMA((3,)),
            pltpu.SemaphoreType.DMA((3, max(gather_units(plan)[2] for plan in gathers))),
            pltpu.VMEM((1, LANES), jnp.float32),
            pltpu.SemaphoreType.DMA((6,)),
            pltpu.SemaphoreType.DMA((3, max(len(sum_pieces(plan)) for plan in sums))),
            pltpu.SemaphoreType.DMA,
            pltpu.SemaphoreType.DMA,
        ]
        + step_scratch(total, frames)
        + [pltpu.VMEM(array.shape, array.dtype) for array in (*weights, features)]
        + [pltpu.SemaphoreType.DMA((4,))],
        compiler_params=pltpu.CompilerParams(
            collective_id=2, has_side_effects=True, vmem_limit_bytes=34 << 20
        ),
        name="fused_step",
    )(*(pltpu.with_memory_space_constraint(array, pltpu.HBM) for array in (frame_lens, label_lens, features, labels, *weights)))


def sum_gradients(devices, grads):
    blocks = [grad.reshape(devices, grad.shape[0] // devices, grad.shape[1]) for grad in grads]
    shapes = [
        jax.ShapeDtypeStruct((block[0].size // LANES, LANES), jnp.float32) for block in blocks
    ]
    buffers = [pltpu.VMEM(block.shape, jnp.float32) for block in blocks]
    return pl.pallas_call(
        functools.partial(sum_kernel, devices),
        out_shape=shapes + [jax.ShapeDtypeStruct((devices, 1, LANES), jnp.float32)],
        in_specs=[VMEM] * 3,
        out_specs=[VMEM] * 4,
        scratch_shapes=buffers
        + buffers
        + [
            pltpu.VMEM((1, LANES), jnp.float32),
            pltpu.SemaphoreType.DMA((3, devices)),
            pltpu.SemaphoreType.DMA((3, devices)),
            pltpu.SemaphoreType.DMA((devices,)),
            pltpu.SemaphoreType.DMA((devices,)),
        ],
        compiler_params=pltpu.CompilerParams(
            collective_id=1, has_side_effects=True, vmem_limit_bytes=50 << 20
        ),
        name="sum_gradients",
    )(*blocks)


def adam_kernel(squares, *refs):
    weights, firsts, seconds, grads, outs = (refs[at : at + 3] for at in (0, 3, 6, 9, 12))
    new_firsts, new_seconds = refs[15:18], refs[18:21]
    total = jnp.sum(squares[...])
    clip = 1.0 / jnp.maximum(jnp.sqrt(jnp.full((1, LANES), total)), 1.0)
    for which in range(3):
        scaled = clip * grads[which][...]
        first = 0.9 * firsts[which][...] + 0.1 * scaled
        second = 0.999 * seconds[which][...] + 0.001 * scaled * scaled
        ratio = first / first_correction / (jnp.sqrt(second / second_correction) + 1e-08)
        outs[which][...] = weights[which][...] - 0.001 * ratio
        new_firsts[which][...] = first
        new_seconds[which][...] = second


def adam(squares, weights, firsts, seconds, grads):
    shapes = [jax.ShapeDtypeStruct(weight.shape, jnp.float32) for weight in weights]
    return pl.pallas_call(
        adam_kernel,
        out_shape=shapes * 3,
        in_specs=[VMEM] * 13,
        out_specs=[VMEM] * 9,
        compiler_params=pltpu.CompilerParams(vmem_limit_bytes=4 << 20),
        name="adam",
    )(squares, *weights, *firsts, *seconds, *grads)


def per_device(
    features,
    frame_lens,
    labels,
    label_lens,
    w_up,
    w_down,
    w_out,
    first_up,
    first_down,
    first_out,
    second_up,
    second_down,
    second_out,
):
    devices = lax.axis_size("dp")
    batch, frames, width = features.shape

    def lined(*arrays):
        return [array.reshape(array.shape[0] // LANES, LANES) for array in arrays]

    weights = lined(w_up, w_down, w_out)
    loss_scale = 1.0 / (batch * devices)
    rows_in = features.reshape(batch * frames, width)
    if w_up.size % (8 * FF) == 0 and w_out.size % (8 * VOCAB) == 0:
        *shares, squares = fused_step(
            loss_scale, devices, frame_lens, label_lens, rows_in, labels, weights
        )
    else:
        full_up, full_down, full_out = gather_weights(devices, *weights)
        grads = local_step(
            loss_scale,
            frame_lens,
            label_lens,
            rows_in,
            labels,
            full_up.reshape(D, FF),
            full_down.reshape(FF, D),
            full_out.reshape(D, VOCAB),
        )
        *shares, squares = sum_gradients(devices, grads)
    results = adam(
        squares,
        weights,
        lined(first_up, first_down, first_out),
        lined(second_up, second_down, second_out),
        shares,
    )
    return tuple(result.reshape(-1) for result in results)


def solution(mesh):
    flat = P("dp")
    return jax.shard_map(
        per_device,
        mesh=mesh,
        in_specs=(P("dp", None, None), flat, P("dp", None), flat) + (flat,) * 9,
        out_specs=(flat,) * 9,
        check_vma=False,
    )
```

```python
import functools

import jax
import jax.numpy as jnp
from jax import lax
from jax.experimental import pallas as pl
from jax.experimental.pallas import tpu as pltpu
from jax.sharding import PartitionSpec as P

D = 256
FF = 1024
VOCAB = 256
LANES = 128
MESH = pl.DeviceIdType.MESH

first_correction = 1.0 - (0.9**10) ** 10
second_correction = 1.0 - (0.999**10) ** 10
negative = -1e30
LOG2E = 1.4426950408889634
PARTS = 2
VMEM = pl.BlockSpec(memory_space=pltpu.VMEM)
SMEM = pl.BlockSpec(memory_space=pltpu.SMEM)
HBM = pl.BlockSpec(memory_space=pltpu.HBM)


def flip(me, bit):
    return me + bit - 2 * bit * ((me // bit) % 2)


def bit_orders(devices):
    bits = [1 << k for k in range(devices.bit_length() - 1)]
    core, rest = bits[:1], bits[1:]
    down = rest[::-1]
    swapped = down[:-2] + down[-2:][::-1]
    turned = down[-2:] + down[:-2]
    return (down + core, swapped + core, turned + core)


def subsets(bits):
    offsets = [0]
    for bit in bits:
        offsets = offsets + [offset + bit for offset in offsets]
    return offsets


def place_with(me, free, pattern):
    place = me
    for bit in free:
        if pattern & bit:
            place = flip(place, bit)
    return place


class Gather:
    def __init__(self, me, devices, fulls, send_sem, recv_sem):
        self.me, self.fulls = me, fulls
        self.send_sem, self.recv_sem = send_sem, recv_sem
        self.orders = bit_orders(devices)
        self.steps = len(self.orders[0])
        self.copies = [{}, {}, {}]

    def fill(self, shards):
        for shard, full in zip(shards, self.fulls):
            rows, width = full.shape[1:]
            parts = width // LANES
            for part in range(parts):
                full[self.me, :, part * LANES : (part + 1) * LANES] = shard[
                    pl.ds(part, rows, stride=parts), :
                ].astype(jnp.bfloat16)

    def send(self, which, pattern, stage):
        order, full = self.orders[which], self.fulls[which]
        owner = place_with(self.me, order[:stage], pattern)
        slot = pattern + order[stage]
        copy = pltpu.make_async_remote_copy(
            src_ref=full.at[owner],
            dst_ref=full.at[owner],
            send_sem=self.send_sem.at[which, slot],
            recv_sem=self.recv_sem.at[which, slot],
            device_id=(flip(self.me, order[stage]),),
            device_id_type=MESH,
        )
        copy.start()
        self.copies[which][slot] = copy

    def pass_on(self):
        for which in range(3):
            for stage in range(self.steps):
                self.send(which, 0, stage)
        for stage in range(self.steps - 1):
            for at in range(1 << stage):
                for which in range(3):
                    order = self.orders[which]
                    pattern = subsets(order[:stage])[at] + order[stage]
                    self.copies[which][pattern].wait_recv()
                    for later in range(stage + 1, self.steps):
                        self.send(which, pattern, later)

    def arrive(self, which):
        order = self.orders[which]
        for pattern in subsets(order[:-1]):
            self.copies[which][pattern + order[-1]].wait_recv()

    def close(self):
        for copies in self.copies:
            for copy in copies.values():
                copy.wait_send()


def drain(ref, blocks, send_sem, recv_sem, peer):
    return pltpu.make_async_remote_copy(
        src_ref=ref.at[pl.ds(0, blocks)],
        dst_ref=ref.at[pl.ds(0, blocks)],
        send_sem=send_sem,
        recv_sem=recv_sem,
        device_id=(peer,),
        device_id_type=MESH,
    )


def flat(stages):
    return [bit for stage in stages for bit in stage]


def move(me, offset, bits):
    return place_with(me, bits, offset)


class StagedGather:
    def __init__(self, me, plans, fulls, send_sem, recv_sem):
        self.me, self.plans, self.fulls = me, plans, fulls
        self.send_sem, self.recv_sem = send_sem, recv_sem
        self.units = [gather_units(plan) for plan in plans]

    def fill(self, shards):
        for shard, full in zip(shards, self.fulls):
            rows, width = full.shape[1:]
            parts = width // LANES
            for part in range(parts):
                full[self.me, :, part * LANES : (part + 1) * LANES] = shard[
                    pl.ds(part, rows, stride=parts), :
                ].astype(jnp.bfloat16)

    def send(self, which, source, first):
        plan, full = self.plans[which], self.fulls[which]
        units, sems, _ = self.units[which]
        for stage in range(first, len(plan)):
            for offset in subsets(plan[stage])[1:][::-1]:
                peer = move(self.me, offset, plan[stage])
                for pattern in units[source][0] if source else [0]:
                    owner = move(self.me, pattern, flat(plan[:stage]))
                    pltpu.make_async_remote_copy(
                        src_ref=full.at[owner],
                        dst_ref=full.at[owner],
                        send_sem=self.send_sem.at[which],
                        recv_sem=self.recv_sem.at[which, sems[stage, offset, source]],
                        device_id=(peer,),
                        device_id_type=MESH,
                    ).start()

    def drain(self, which, blocks, at):
        return drain(
            self.fulls[which], blocks, self.send_sem.at[which], self.recv_sem.at[which, at],
            flip(self.me, 1),
        )

    def pass_on(self):
        for which in range(3):
            self.send(which, None, 0)
        names = [list(units[0]) for units in self.units]
        for at in range(max(len(some) for some in names)):
            for which in range(3):
                if at < len(names[which]):
                    name = names[which][at]
                    patterns, sem = self.units[which][0][name]
                    self.drain(which, len(patterns), sem).wait_recv()
                    self.send(which, name, name[0] + 1)

    def arrive(self, which):
        before = 1 << len(flat(self.plans[which][:-1]))
        self.drain(which, before, self.units[which][2] - 1).wait_recv()

    def close(self):
        for which in range(3):
            before = 1 << len(flat(self.plans[which]))
            self.drain(which, before - 1, 0).wait_send()


def gather_units(plan):
    units, sems, count = {}, {}, 0
    last = len(plan) - 1
    for stage, bits in enumerate(plan):
        offsets = subsets(bits)[1:]
        groups = [[offset] for offset in offsets] if stage + 1 < last else [offsets]
        sources = {None: [0], **{name: patterns for name, (patterns, _) in units.items()}}
        for name, patterns in sources.items():
            for group in groups:
                for offset in group:
                    sems[stage, offset, name] = count
                if stage < last:
                    arriving = [offset + at for offset in group for at in patterns]
                    units[stage, tuple(group), name] = (arriving, count)
                    count += 1
    return units, sems, count + 1


def greet_stages(me, plan, barrier):
    for bits in plan:
        for offset in subsets(bits)[1:]:
            pl.semaphore_signal(
                barrier, inc=1, device_id=(move(me, offset, bits),), device_id_type=MESH
            )


def stage_partners(plan):
    return sum((1 << len(bits)) - 1 for bits in plan)


def greet(me, devices, barrier):
    @pl.loop(1, devices)
    def _(shift):
        pl.semaphore_signal(
            barrier, inc=1, device_id=((me + shift) % devices,), device_id_type=MESH
        )


def gather_kernel(devices, w_up, w_down, w_out, full_up, full_down, full_out, send_sem, recv_sem):
    me = lax.axis_index("dp")
    barrier = pltpu.get_barrier_semaphore()
    greet(me, devices, barrier)
    gather = Gather(me, devices, (full_up, full_down, full_out), send_sem, recv_sem)
    gather.fill((w_up, w_down, w_out))
    pl.semaphore_wait(barrier, devices - 1)
    gather.pass_on()
    for which in range(3):
        gather.arrive(which)
    gather.close()


def gather_weights(devices, w_up, w_down, w_out):
    shapes = []
    for shard, width in ((w_up, FF), (w_down, D), (w_out, VOCAB)):
        shapes.append(
            jax.ShapeDtypeStruct((devices, shard.size // width, width), jnp.bfloat16)
        )
    return pl.pallas_call(
        functools.partial(gather_kernel, devices),
        out_shape=shapes,
        in_specs=[VMEM] * 3,
        out_specs=[VMEM] * 3,
        scratch_shapes=[
            pltpu.SemaphoreType.DMA((3, devices)),
            pltpu.SemaphoreType.DMA((3, devices)),
        ],
        compiler_params=pltpu.CompilerParams(collective_id=0, has_side_effects=True),
        name="gather_weights",
    )(w_up, w_down, w_out)


def dot_rows(left, right):
    return jnp.dot(left, right, preferred_element_type=jnp.float32)


def dot_last(left, right, precision=None):
    return lax.dot_general(
        left, right, (((1,), (1,)), ((), ())), precision=precision,
        preferred_element_type=jnp.float32,
    )


def dot_first(left, right):
    return lax.dot_general(
        left, right, (((0,), (0,)), ((), ())), preferred_element_type=jnp.float32
    )


def row_blocks(total, body):
    block = min(256, total)
    for step in range(total // block):
        body(pl.ds(step * block, block))


def normalize(features, normalized):
    def body(rows):
        flat_in = features[rows, :].astype(jnp.float32)
        centre = jnp.mean(flat_in, axis=1, keepdims=True)
        shifted = flat_in - centre
        spread = jnp.mean(shifted * shifted, axis=1, keepdims=True)
        normalized[rows, :] = (shifted * lax.rsqrt(spread + 1e-05)).astype(jnp.bfloat16)

    row_blocks(features.shape[0], body)


def project_up(normalized, up_mat, slopes, hidden):
    def body(rows):
        act = dot_rows(normalized[rows, :], up_mat[...].reshape(D, FF))
        sigmoid = 1.0 / (1.0 + jnp.exp(-act))
        slopes[rows, :] = sigmoid * (1.0 + act * (1.0 - sigmoid))
        hidden[rows, :] = (act * sigmoid).astype(jnp.bfloat16)

    row_blocks(normalized.shape[0], body)


def project_down(features, hidden, down_mat, out_mat, block_out, log_probs):
    def body(rows):
        flat_in = features[rows, :].astype(jnp.float32)
        out_rows = (flat_in + 0.5 * dot_rows(hidden[rows, :], down_mat[...].reshape(FF, D))).astype(
            jnp.bfloat16
        )
        block_out[rows, :] = out_rows
        logits = dot_rows(out_rows, out_mat[...].reshape(D, VOCAB))
        top = jnp.max(logits, axis=1, keepdims=True)
        low = (logits - top) * LOG2E
        log_probs[rows, :] = low - jnp.log2(jnp.sum(jnp.exp2(low), axis=1, keepdims=True))

    row_blocks(features.shape[0], body)


def split_dot(dot, values, picks):
    high = values.astype(jnp.bfloat16)
    rest = values - high.astype(jnp.float32)
    middle = rest.astype(jnp.bfloat16)
    low = (rest - middle.astype(jnp.float32)).astype(jnp.bfloat16)
    return dot(high, picks) + (dot(middle, picks) + dot(low, picks))


def ctc_rows(frames):
    return [pltpu.VMEM((frames, 8, LANES), jnp.float32)] * 4 + [
        pltpu.VMEM((2 * frames, 8, LANES), jnp.float32)
    ] * 4


class Lattice:
    def __init__(self, parts, sign, skip):
        self.parts, self.sign = parts, sign
        self.row = 0 if sign > 0 else 7
        self.skips = [self.spread(skip, part) > 0.5 for part in range(parts)]

    def spread(self, values, part):
        if self.sign > 0:
            return pltpu.roll(values, part, 1, stride=self.parts, stride_axis=0)
        shift = LANES - part - 7 * self.parts
        return pltpu.roll(values, shift, 1, stride=self.parts, stride_axis=0)

    def begin(self, blank, label):
        def whole(values):
            return jnp.broadcast_to(values[self.row : self.row + 1], (8, LANES))

        blank, label = whole(blank), whole(label)
        self.blank = [self.spread(blank, part) for part in range(self.parts)]
        self.label = [self.spread(label, part) for part in range(self.parts + 1)]
        one = jnp.ones((8, LANES), jnp.float32)
        self.blank_mass, self.label_mass = [one] * self.parts, [one] * (self.parts + 1)

    def next_rows(self, values):
        return pltpu.roll(values, 7 if self.sign > 0 else 1, 0)

    def advance(self, emit_blank, emit_label, parts):
        blank, label, blank_mass, label_mass = [], [], [], []
        for part in range(parts):
            b, l, l1 = self.blank[part], self.label[part], self.label[part + 1]
            bm, lm, lm1 = self.blank_mass[part], self.label_mass[part], self.label_mass[part + 1]
            top = jnp.maximum(b, l1)
            mass = bm * jnp.exp2(b - top) + lm1 * jnp.exp2(l1 - top)
            above = jnp.where(self.skips[part], top, b)
            above_mass = jnp.where(self.skips[part], mass, bm)
            peak = jnp.maximum(l, above)
            peak_mass = lm * jnp.exp2(l - peak) + above_mass * jnp.exp2(above - peak)
            if part == 0:
                result = (top, mass, peak, peak_mass)
            blank.append(top + emit_blank)
            label.append(peak + self.spread(emit_label, part))
            blank_mass.append(mass)
            label_mass.append(peak_mass)
        if parts == self.parts:
            label.append(self.next_rows(label[0]))
            label_mass.append(self.next_rows(label_mass[0]))
        self.blank, self.label = blank, label
        self.blank_mass, self.label_mass = blank_mass, label_mass
        return result


def ctc_grad(
    loss_scale,
    frame_lens,
    label_lens,
    labels,
    log_probs,
    emitted,
    emitted_blank,
    alpha_rows,
    beta_rows,
    logit_grad,
):
    utterances, label_count = labels.shape
    frames = log_probs.shape[0] // utterances
    half = LANES // utterances
    depth = 8 * PARTS
    assert label_count + depth <= half and frames % depth == 0

    lane_row = lax.broadcasted_iota(jnp.int32, (8, LANES), 1)
    label_ids = lax.broadcasted_iota(jnp.int32, (label_count, LANES), 0)
    spread_lanes = lax.broadcasted_iota(jnp.int32, (label_count, LANES), 1)
    label_rows = jnp.concatenate(
        [
            labels[...].astype(jnp.float32),
            jnp.zeros((8 - utterances, label_count), jnp.float32),
        ],
        axis=0,
    ).astype(jnp.bfloat16)
    extended = jnp.zeros((8, LANES), jnp.float32)
    for utterance in range(utterances):
        spread = (spread_lanes == label_ids + half * utterance + 1).astype(jnp.bfloat16)
        placed = dot_rows(label_rows, spread)[utterance : utterance + 1]
        extended = extended + jnp.broadcast_to(placed, (8, LANES))
    skip = jnp.where(extended != pltpu.roll(extended, 1, 1), 1.0, 0.0)
    skip_back = pltpu.roll(skip, LANES - 1, 1)

    vocab_ids = lax.broadcasted_iota(jnp.int32, (VOCAB, LANES), 0).astype(jnp.float32)
    vocab_lanes = lax.broadcasted_iota(jnp.int32, (VOCAB, LANES), 1)
    frame_lanes = lax.broadcasted_iota(jnp.int32, (frames, LANES), 1)
    onehots = []
    picked = None
    blanks = None
    for utterance in range(utterances):
        rows = slice(utterance * frames, (utterance + 1) * frames)
        first = half * utterance + 1
        mine = (vocab_lanes >= first) & (vocab_lanes < first + label_count)
        onehot = jnp.where((vocab_ids == extended[0:1, :]) & mine, 1.0, 0.0).astype(jnp.bfloat16)
        onehots.append(onehot)
        picks = split_dot(dot_rows, log_probs[rows, :], onehot)
        blank = jnp.broadcast_to(log_probs[rows, 0:1], (frames, LANES))
        if utterance == 0:
            picked, blanks = picks, blank
        else:
            picked = jnp.where(frame_lanes < half * utterance, picked, picks)
            blanks = jnp.where(frame_lanes < half * utterance, blanks, blank)
    place = frame_lanes % half
    emitted[...] = jnp.where((place >= 1) & (place <= label_count), picked, negative)
    emitted_blank[...] = blanks

    forward = Lattice(PARTS, 1, skip)
    backward = Lattice(PARTS, -1, skip_back)
    start = jnp.full((8, LANES), negative, jnp.float32)
    start_back = start
    for utterance in range(utterances):
        first = half * utterance + 1
        start = jnp.where(lane_row == first, 0.0, start)
        start_back = jnp.where(
            lane_row == first + label_lens[utterance] - 1, 0.0, start_back
        )
    nothing = jnp.full((8, LANES), negative, jnp.float32)

    def row_of(ref, frame):
        return jnp.broadcast_to(ref[pl.ds(frame, 1), :], (8, LANES))

    def block(at, carry):
        forward.begin(*carry[:2])
        backward.begin(*carry[2:])
        for level in range(depth):
            frame = at * depth + level
            needed = min(PARTS, depth - level)
            result = forward.advance(row_of(emitted_blank, frame), row_of(emitted, frame), needed)
            for ref, value in zip(alpha_rows, result):
                ref[frame] = value
            emit = emit_blank = None
            for utterance in range(utterances):
                back = jnp.maximum(frame_lens[utterance] - 1 - frame, 0)
                mine, mine_blank = row_of(emitted, back), row_of(emitted_blank, back)
                if utterance == 0:
                    emit, emit_blank = mine, mine_blank
                else:
                    emit = jnp.where(lane_row < half * utterance, emit, mine)
                    emit_blank = jnp.where(lane_row < half * utterance, emit_blank, mine_blank)
            result = backward.advance(emit_blank, emit, needed)
            for ref, value in zip(beta_rows, result):
                ref[frames - 1 - frame] = value
        return tuple(
            values[0] + jnp.log2(mass[0])
            for lattice in (forward, backward)
            for values, mass in (
                (lattice.blank, lattice.blank_mass), (lattice.label, lattice.label_mass)
            )
        )

    lax.fori_loop(0, frames // depth, block, (start, nothing, start_back, nothing))

    frame_ids = lax.broadcasted_iota(jnp.int32, (frames, LANES), 0)
    alphas = [ref[:, forward.row, :] for ref in alpha_rows]
    betas, alive = [], None
    for ref in beta_rows:
        value = None
        for utterance in range(utterances):
            mine = ref[pl.ds(frames - frame_lens[utterance], frames), backward.row, :]
            value = mine if value is None else jnp.where(frame_lanes < half * utterance, value, mine)
        betas.append(value)
    betas[0], betas[1] = pltpu.roll(betas[0], 1, 1), pltpu.roll(betas[1], 1, 1)
    joint_blank = alphas[0] + emitted_blank[...] + betas[0]
    joint_label = alphas[2] + emitted[...] + betas[2]
    blank_mass, label_mass = alphas[1] * betas[1], alphas[3] * betas[3]
    both = jnp.maximum(joint_blank, joint_label)
    for utterance in range(utterances):
        rows = slice(utterance * frames, (utterance + 1) * frames)
        first = half * utterance
        mine = (frame_lanes >= first) & (frame_lanes < first + half)
        top = jnp.max(jnp.where(mine, both, negative), axis=1, keepdims=True)
        live = mine & (frame_ids < frame_lens[utterance])
        label = jnp.where(live, label_mass * jnp.exp2(joint_label - top), 0.0)
        blank = jnp.where(live, blank_mass * jnp.exp2(joint_blank - top), 0.0)
        blank_sum = jnp.sum(blank, axis=1, keepdims=True)
        total = jnp.sum(label, axis=1, keepdims=True) + blank_sum
        kept = frame_ids[:, 0:1] < frame_lens[utterance]
        scale = jnp.where(kept, 1.0 / jnp.where(kept, total, 1.0), 0.0)
        gamma = split_dot(dot_last, label * scale, onehots[utterance])
        vocab_at = lax.broadcasted_iota(jnp.int32, (frames, VOCAB), 1)
        gamma = gamma + jnp.where(vocab_at == 0, blank_sum * scale, 0.0)
        probs = jnp.exp2(log_probs[rows, :]) * jnp.where(kept, 1.0, 0.0)
        logit_grad[rows, :] = (loss_scale * (probs - gamma)).astype(jnp.bfloat16)


def grad_ff(logit_grad, out_mat, ff_grad):
    def body(rows):
        ff_grad[rows, :] = (
            0.5 * dot_last(logit_grad[rows, :], out_mat[...].reshape(D, VOCAB))
        ).astype(jnp.bfloat16)

    row_blocks(logit_grad.shape[0], body)


def grad_act(ff_grad, down_mat, slopes, act_grad):
    def body(rows):
        act_grad[rows, :] = (
            dot_last(ff_grad[rows, :], down_mat[...].reshape(FF, D)) * slopes[rows, :]
        ).astype(jnp.bfloat16)

    row_blocks(ff_grad.shape[0], body)


def step_kernel(
    loss_scale,
    frame_lens,
    label_lens,
    features,
    labels,
    up_mat,
    down_mat,
    out_mat,
    grad_up,
    grad_down,
    grad_out,
    normalized,
    slopes,
    hidden,
    block_out,
    log_probs,
    logit_grad,
    ff_grad,
    act_grad,
    emitted,
    emitted_blank,
    *lattice_rows,
):
    normalize(features, normalized)
    project_up(normalized, up_mat, slopes, hidden)
    project_down(features, hidden, down_mat, out_mat, block_out, log_probs)
    ctc_grad(
        loss_scale, frame_lens, label_lens, labels, log_probs, emitted, emitted_blank,
        lattice_rows[:4], lattice_rows[4:], logit_grad,
    )
    grad_ff(logit_grad, out_mat, ff_grad)
    grad_act(ff_grad, down_mat, slopes, act_grad)
    grad_up[...] = dot_first(normalized[...], act_grad[...])
    grad_down[...] = dot_first(hidden[...], ff_grad[...])
    grad_out[...] = dot_first(block_out[...], logit_grad[...])


def step_scratch(total, frames):
    return [
        pltpu.VMEM((total, D), jnp.bfloat16),
        pltpu.VMEM((total, FF), jnp.float32),
        pltpu.VMEM((total, FF), jnp.bfloat16),
        pltpu.VMEM((total, D), jnp.bfloat16),
        pltpu.VMEM((total, VOCAB), jnp.float32),
        pltpu.VMEM((total, VOCAB), jnp.bfloat16),
        pltpu.VMEM((total, D), jnp.bfloat16),
        pltpu.VMEM((total, FF), jnp.bfloat16),
        pltpu.VMEM((frames, LANES), jnp.float32),
        pltpu.VMEM((frames, LANES), jnp.float32),
    ] + ctc_rows(frames)


def local_step(loss_scale, frame_lens, label_lens, features, labels, up_mat, down_mat, out_mat):
    total = features.shape[0]
    frames = total // labels.shape[0]
    return pl.pallas_call(
        functools.partial(step_kernel, loss_scale),
        out_shape=[
            jax.ShapeDtypeStruct((D, FF), jnp.float32),
            jax.ShapeDtypeStruct((FF, D), jnp.float32),
            jax.ShapeDtypeStruct((D, VOCAB), jnp.float32),
        ],
        in_specs=[SMEM, SMEM] + [VMEM] * 5,
        out_specs=[VMEM] * 3,
        scratch_shapes=step_scratch(total, frames),
        compiler_params=pltpu.CompilerParams(vmem_limit_bytes=40 << 20),
        name="local_step",
    )(frame_lens, label_lens, features, labels, up_mat, down_mat, out_mat)


class Sum:
    def __init__(self, me, devices, grads, received, staged, send_sem, recv_sem):
        self.me, self.grads, self.received, self.staged = me, grads, received, staged
        self.send_sem, self.recv_sem = send_sem, recv_sem
        self.orders = [order[::-1] for order in bit_orders(devices)]
        self.steps = len(self.orders[0])
        self.copies = [{}, {}, {}]

    def sum_of(self, which, place, pattern, stage):
        value = self.grads[which][place]
        for bit in self.orders[which][:stage]:
            self.copies[which][pattern + bit].wait_recv()
            value = value + self.received[which][pattern + bit]
        return value

    def send(self, which, stage):
        order = self.orders[which]
        for offset in subsets(order[stage + 1 :][::-1])[::-1]:
            slot = offset + order[stage]
            place = place_with(self.me, order, slot)
            if stage == 0:
                source = self.grads[which].at[place]
            else:
                self.staged[which][slot] = self.sum_of(which, place, slot, stage)
                source = self.staged[which].at[slot]
            copy = pltpu.make_async_remote_copy(
                src_ref=source,
                dst_ref=self.received[which].at[slot],
                send_sem=self.send_sem.at[which, slot],
                recv_sem=self.recv_sem.at[which, slot],
                device_id=(flip(self.me, order[stage]),),
                device_id_type=MESH,
            )
            copy.start()
            self.copies[which][slot] = copy

    def finish(self, devices, reduced, squares, own_squares, small_send, small_recv):
        me = self.me
        own = jnp.zeros((1, LANES), jnp.float32)
        for which in (2, 1, 0):
            value = self.sum_of(which, me, 0, self.steps)
            rows, width = value.shape
            parts = width // LANES
            for part in range(parts):
                piece = value[:, part * LANES : (part + 1) * LANES]
                reduced[which][pl.ds(part, rows, stride=parts), :] = piece
                own = own + jnp.sum(piece * piece, axis=0, keepdims=True)
        own_squares[...] = own
        squares[0] = own

        def small_copy(shift):
            return pltpu.make_async_remote_copy(
                src_ref=own_squares,
                dst_ref=squares.at[shift],
                send_sem=small_send.at[shift],
                recv_sem=small_recv.at[shift],
                device_id=((me + shift) % devices,),
                device_id_type=MESH,
            )

        @pl.loop(1, devices)
        def _(shift):
            small_copy(shift).start()

        for copies in self.copies:
            for copy in copies.values():
                copy.wait_send()

        @pl.loop(1, devices)
        def _(shift):
            small_copy(shift).wait()


def sum_pieces(plan):
    pieces = {}
    for stage in range(len(plan)):
        for after in subsets(plan[stage + 1]) if stage + 1 < len(plan) else [0]:
            pieces[stage, after] = len(pieces)
    return pieces


class StagedSum:
    def __init__(self, me, plans, narrow, grads, received, staged, send_sem, recv_sem):
        self.me, self.plans, self.narrow = me, plans, narrow
        self.grads, self.received, self.staged = grads, received, staged
        self.send_sem, self.recv_sem = send_sem, recv_sem
        self.pieces = [sum_pieces(plan) for plan in plans]
        self.seen = set()

    def index(self, which, pattern):
        bits = flat(self.plans[which])
        return sum(1 << at for at, bit in enumerate(bits[::-1]) if pattern & bit)

    def wide(self, which, stage):
        return 3 * (stage in self.narrow[which]) + which

    def put(self, which, value):
        bits = flat(self.plans[which])[::-1]
        blocks, rows, width = self.grads[which].shape
        own = [(self.me // bit) % 2 for bit in bits]
        for block in range(blocks):
            slot = 0
            for at, bit in enumerate(bits):
                slot = slot + (1 << at) * (1 - own[at] if block & bit else own[at])
            self.grads[which][slot] = value[block * rows : (block + 1) * rows, :]

    def copy(self, which, name):
        stage, offset, after = name
        start = self.index(which, offset + after)
        blocks = pl.ds(start, 1 << len(flat(self.plans[which][stage + 2 :])))
        at = self.wide(which, stage)
        source = self.grads[which] if stage == 0 else self.staged[at]
        return pltpu.make_async_remote_copy(
            src_ref=source.at[blocks],
            dst_ref=self.received[at].at[blocks],
            send_sem=self.send_sem.at[at],
            recv_sem=self.recv_sem.at[which, self.pieces[which][stage, after]],
            device_id=(move(self.me, offset, self.plans[which][stage]),),
            device_id_type=MESH,
        )

    def wait(self, which, stage, after):
        plan = self.plans[which]
        blocks = ((1 << len(plan[stage])) - 1) << len(flat(plan[stage + 2 :]))
        at = self.wide(which, stage)
        drain(
            self.received[at], blocks, self.send_sem.at[at],
            self.recv_sem.at[which, self.pieces[which][stage, after]], flip(self.me, 1),
        ).wait_recv()

    def sum_of(self, which, pattern, stage):
        value = self.grads[which][self.index(which, pattern)]
        for earlier in range(stage):
            after = 0
            if earlier + 1 < len(self.plans[which]):
                after = sum(bit for bit in self.plans[which][earlier + 1] if pattern & bit)
            if (which, earlier, after) not in self.seen:
                self.seen.add((which, earlier, after))
                self.wait(which, earlier, after)
            for offset in subsets(self.plans[which][earlier])[1:]:
                slot = self.index(which, pattern + offset)
                value = value + self.received[self.wide(which, earlier)][slot].astype(jnp.float32)
        return value

    def send(self, which, stage):
        plan = self.plans[which]
        afters = subsets(plan[stage + 1])[::-1] if stage + 1 < len(plan) else [0]
        for after in afters:
            for offset in subsets(plan[stage])[1:][::-1]:
                if stage:
                    staged = self.staged[self.wide(which, stage)]
                    for later in subsets(flat(plan[stage + 2 :])):
                        pattern = offset + after + later
                        staged[self.index(which, pattern)] = self.sum_of(
                            which, pattern, stage
                        ).astype(staged.dtype)
                self.copy(which, (stage, offset, after)).start()

    def finish(self, devices, reduced, squares, own_squares, small_send, small_recv):
        me = self.me
        own = jnp.zeros((1, LANES), jnp.float32)
        for which in (2, 1, 0):
            value = self.sum_of(which, 0, len(self.plans[which]))
            rows, width = value.shape
            parts = width // LANES
            for part in range(parts):
                piece = value[:, part * LANES : (part + 1) * LANES]
                reduced[which][pl.ds(part, rows, stride=parts), :] = piece
                own = own + jnp.sum(piece * piece, axis=0, keepdims=True)
        own_squares[...] = own
        squares[0] = own

        @pl.loop(1, devices)
        def _(shift):
            pltpu.make_async_remote_copy(
                src_ref=own_squares,
                dst_ref=squares.at[shift],
                send_sem=small_send,
                recv_sem=small_recv,
                device_id=((me + shift) % devices,),
                device_id_type=MESH,
            ).start()

        for which, plan in enumerate(self.plans):
            sent = {}
            for stage, bits in enumerate(plan):
                blocks = ((1 << len(bits)) - 1) << len(flat(plan[stage + 1 :]))
                at = self.wide(which, stage)
                sent[at] = sent.get(at, 0) + blocks
            for at, blocks in sent.items():
                drain(
                    self.received[at], blocks, self.send_sem.at[at], self.recv_sem.at[which, 0],
                    flip(me, 1),
                ).wait_send()
        small = drain(squares, devices - 1, small_send, small_recv, flip(me, 1))
        small.wait_send()
        small.wait_recv()


def sum_kernel(devices, *refs):
    grads, reduced, squares = refs[:3], refs[3:6], refs[6]
    received, staged = refs[7:10], refs[10:13]
    own_squares, send_sem, recv_sem, small_send, small_recv = refs[13:]
    me = lax.axis_index("dp")
    barrier = pltpu.get_barrier_semaphore()
    greet(me, devices, barrier)
    pl.semaphore_wait(barrier, devices - 1)
    total = Sum(me, devices, grads, received, staged, send_sem, recv_sem)
    for stage in range(total.steps):
        for which in range(3):
            total.send(which, stage)
    total.finish(devices, reduced, squares, own_squares, small_send, small_recv)


def exchange_plans(devices):
    bits = [1 << k for k in range(devices.bit_length() - 1)]
    core, near, far = bits[:1], bits[1:3], bits[3:]
    gathers = ([far, near, core], [far, near, core], [near, far, core])
    sums = ([core, near, far], [core, near, far], [core, far, near])
    narrow = ((1, 2), (1,), (1,))
    return gathers, sums, narrow


def meet_plan(devices):
    bits = [1 << k for k in range(devices.bit_length() - 1)]
    core, near, far = bits[:1], bits[1:3], bits[3:]
    return [core, near, far]


def fused_kernel(devices, loss_scale, *refs):
    frame_lens, label_lens, features, labels = refs[:4]
    shards, reduced, squares = refs[4:7], refs[7:10], refs[10]
    fulls, grads, received, staged = refs[11:14], refs[14:17], refs[17:23], refs[23:29]
    gather_send, gather_recv, own_squares, send_sem, recv_sem, small_send, small_recv = refs[29:36]
    normalized, slopes, hidden, block_out, log_probs = refs[36:41]
    logit_grad, ff_grad, act_grad, emitted, emitted_blank = refs[41:46]
    alpha_rows, beta_rows = refs[46:50], refs[50:54]
    held, load_sem = refs[54:58], refs[58]
    up_mat, down_mat, out_mat = fulls
    me = lax.axis_index("dp")
    loads = [
        pltpu.make_async_copy(source, target, load_sem.at[at])
        for at, (source, target) in enumerate(zip((*shards, features), held))
    ]
    for load in loads:
        load.start()
    shards, features = held[:3], held[3]
    barrier = pltpu.get_barrier_semaphore()
    gathers, sums, narrow = exchange_plans(devices)
    greet_stages(me, meet_plan(devices), barrier)
    gather = StagedGather(me, gathers, fulls, gather_send, gather_recv)
    for load in loads[:3]:
        load.wait()
    gather.fill(shards)
    loads[3].wait()
    normalize(features, normalized)
    pl.semaphore_wait(barrier, stage_partners(meet_plan(devices)))
    gather.pass_on()
    gather.arrive(0)
    project_up(normalized, up_mat, slopes, hidden)
    gather.arrive(1)
    gather.arrive(2)
    project_down(features, hidden, down_mat, out_mat, block_out, log_probs)
    ctc_grad(
        loss_scale, frame_lens, label_lens, labels, log_probs, emitted, emitted_blank, alpha_rows,
        beta_rows, logit_grad,
    )
    total = StagedSum(me, sums, narrow, grads, received, staged, send_sem, recv_sem)
    pending = [list(range(len(plan))) for plan in sums]

    def advance(*whiches):
        for which in whiches:
            if pending[which]:
                total.send(which, pending[which].pop(0))

    grad_ff(logit_grad, out_mat, ff_grad)
    total.put(1, dot_first(hidden[...], ff_grad[...]))
    advance(1)
    grad_act(ff_grad, down_mat, slopes, act_grad)
    advance(1)
    total.put(0, dot_first(normalized[...], act_grad[...]))
    advance(0)
    total.put(2, dot_first(block_out[...], logit_grad[...]))
    advance(2)
    while any(pending):
        advance(1, 0, 2)
    total.finish(devices, reduced, squares, own_squares, small_send, small_recv)
    gather.close()


def fused_step(loss_scale, devices, frame_lens, label_lens, features, labels, weights):
    total = features.shape[0]
    frames = total // labels.shape[0]
    blocks = [
        (devices, weight.size // width, width)
        for weight, width in zip(weights, (FF, D, VOCAB))
    ]
    gathers, sums, _ = exchange_plans(devices)
    wide = [pltpu.VMEM(block, jnp.float32) for block in blocks]
    both = wide + [pltpu.VMEM(block, jnp.bfloat16) for block in blocks]
    return pl.pallas_call(
        functools.partial(fused_kernel, devices, loss_scale),
        out_shape=[jax.ShapeDtypeStruct(weight.shape, jnp.float32) for weight in weights]
        + [jax.ShapeDtypeStruct((devices, 1, LANES), jnp.float32)],
        in_specs=[SMEM, SMEM, HBM, VMEM] + [HBM] * 3,
        out_specs=[VMEM] * 4,
        scratch_shapes=[pltpu.VMEM(block, jnp.bfloat16) for block in blocks]
        + wide
        + both * 2
        + [
            pltpu.SemaphoreType.DMA((3,)),
            pltpu.SemaphoreType.DMA((3, max(gather_units(plan)[2] for plan in gathers))),
            pltpu.VMEM((1, LANES), jnp.float32),
            pltpu.SemaphoreType.DMA((6,)),
            pltpu.SemaphoreType.DMA((3, max(len(sum_pieces(plan)) for plan in sums))),
            pltpu.SemaphoreType.DMA,
            pltpu.SemaphoreType.DMA,
        ]
        + step_scratch(total, frames)
        + [pltpu.VMEM(array.shape, array.dtype) for array in (*weights, features)]
        + [pltpu.SemaphoreType.DMA((4,))],
        compiler_params=pltpu.CompilerParams(
            collective_id=2, has_side_effects=True, vmem_limit_bytes=34 << 20
        ),
        name="fused_step",
    )(*(pltpu.with_memory_space_constraint(array, pltpu.HBM) for array in (frame_lens, label_lens, features, labels, *weights)))


def sum_gradients(devices, grads):
    blocks = [grad.reshape(devices, grad.shape[0] // devices, grad.shape[1]) for grad in grads]
    shapes = [
        jax.ShapeDtypeStruct((block[0].size // LANES, LANES), jnp.float32) for block in blocks
    ]
    buffers = [pltpu.VMEM(block.shape, jnp.float32) for block in blocks]
    return pl.pallas_call(
        functools.partial(sum_kernel, devices),
        out_shape=shapes + [jax.ShapeDtypeStruct((devices, 1, LANES), jnp.float32)],
        in_specs=[VMEM] * 3,
        out_specs=[VMEM] * 4,
        scratch_shapes=buffers
        + buffers
        + [
            pltpu.VMEM((1, LANES), jnp.float32),
            pltpu.SemaphoreType.DMA((3, devices)),
            pltpu.SemaphoreType.DMA((3, devices)),
            pltpu.SemaphoreType.DMA((devices,)),
            pltpu.SemaphoreType.DMA((devices,)),
        ],
        compiler_params=pltpu.CompilerParams(
            collective_id=1, has_side_effects=True, vmem_limit_bytes=50 << 20
        ),
        name="sum_gradients",
    )(*blocks)


def adam_kernel(squares, *refs):
    weights, firsts, seconds, grads, outs = (refs[at : at + 3] for at in (0, 3, 6, 9, 12))
    new_firsts, new_seconds = refs[15:18], refs[18:21]
    total = jnp.sum(squares[...])
    clip = 1.0 / jnp.maximum(jnp.sqrt(jnp.full((1, LANES), total)), 1.0)
    for which in range(3):
        scaled = clip * grads[which][...]
        first = 0.9 * firsts[which][...] + 0.1 * scaled
        second = 0.999 * seconds[which][...] + 0.001 * scaled * scaled
        ratio = first / first_correction / (jnp.sqrt(second / second_correction) + 1e-08)
        outs[which][...] = weights[which][...] - 0.001 * ratio
        new_firsts[which][...] = first
        new_seconds[which][...] = second


def adam(squares, weights, firsts, seconds, grads):
    shapes = [jax.ShapeDtypeStruct(weight.shape, jnp.float32) for weight in weights]
    return pl.pallas_call(
        adam_kernel,
        out_shape=shapes * 3,
        in_specs=[VMEM] * 13,
        out_specs=[VMEM] * 9,
        compiler_params=pltpu.CompilerParams(vmem_limit_bytes=4 << 20),
        name="adam",
    )(squares, *weights, *firsts, *seconds, *grads)


def per_device(
    features,
    frame_lens,
    labels,
    label_lens,
    w_up,
    w_down,
    w_out,
    first_up,
    first_down,
    first_out,
    second_up,
    second_down,
    second_out,
):
    devices = lax.axis_size("dp")
    batch, frames, width = features.shape

    def lined(*arrays):
        return [array.reshape(array.shape[0] // LANES, LANES) for array in arrays]

    weights = lined(w_up, w_down, w_out)
    loss_scale = 1.0 / (batch * devices)
    rows_in = features.reshape(batch * frames, width)
    if w_up.size % (8 * FF) == 0 and w_out.size % (8 * VOCAB) == 0:
        *shares, squares = fused_step(
            loss_scale, devices, frame_lens, label_lens, rows_in, labels, weights
        )
    else:
        full_up, full_down, full_out = gather_weights(devices, *weights)
        grads = local_step(
            loss_scale,
            frame_lens,
            label_lens,
            rows_in,
            labels,
            full_up.reshape(D, FF),
            full_down.reshape(FF, D),
            full_out.reshape(D, VOCAB),
        )
        *shares, squares = sum_gradients(devices, grads)
    results = adam(
        squares,
        weights,
        lined(first_up, first_down, first_out),
        lined(second_up, second_down, second_out),
        shares,
    )
    return tuple(result.reshape(-1) for result in results)


def solution(mesh):
    flat = P("dp")
    return jax.shard_map(
        per_device,
        mesh=mesh,
        in_specs=(P("dp", None, None), flat, P("dp", None), flat) + (flat,) * 9,
        out_specs=(flat,) * 9,
        check_vma=False,
    )
```

```python
import functools

import jax
import jax.numpy as jnp
from jax import lax
from jax.experimental import pallas as pl
from jax.experimental.pallas import tpu as pltpu
from jax.sharding import PartitionSpec as P

D = 256
FF = 1024
VOCAB = 256
LANES = 128
MESH = pl.DeviceIdType.MESH

first_correction = 1.0 - (0.9**10) ** 10
second_correction = 1.0 - (0.999**10) ** 10
negative = -1e30
LOG2E = 1.4426950408889634
PARTS = 2
VMEM = pl.BlockSpec(memory_space=pltpu.VMEM)
SMEM = pl.BlockSpec(memory_space=pltpu.SMEM)
HBM = pl.BlockSpec(memory_space=pltpu.HBM)


def flip(me, bit):
    return me + bit - 2 * bit * ((me // bit) % 2)


def bit_orders(devices):
    bits = [1 << k for k in range(devices.bit_length() - 1)]
    core, rest = bits[:1], bits[1:]
    down = rest[::-1]
    swapped = down[:-2] + down[-2:][::-1]
    turned = down[-2:] + down[:-2]
    return (down + core, swapped + core, turned + core)


def subsets(bits):
    offsets = [0]
    for bit in bits:
        offsets = offsets + [offset + bit for offset in offsets]
    return offsets


def place_with(me, free, pattern):
    place = me
    for bit in free:
        if pattern & bit:
            place = flip(place, bit)
    return place


class Gather:
    def __init__(self, me, devices, fulls, send_sem, recv_sem):
        self.me, self.fulls = me, fulls
        self.send_sem, self.recv_sem = send_sem, recv_sem
        self.orders = bit_orders(devices)
        self.steps = len(self.orders[0])
        self.copies = [{}, {}, {}]

    def fill(self, shards):
        for shard, full in zip(shards, self.fulls):
            rows, width = full.shape[1:]
            parts = width // LANES
            for part in range(parts):
                full[self.me, :, part * LANES : (part + 1) * LANES] = shard[
                    pl.ds(part, rows, stride=parts), :
                ].astype(jnp.bfloat16)

    def send(self, which, pattern, stage):
        order, full = self.orders[which], self.fulls[which]
        owner = place_with(self.me, order[:stage], pattern)
        slot = pattern + order[stage]
        copy = pltpu.make_async_remote_copy(
            src_ref=full.at[owner],
            dst_ref=full.at[owner],
            send_sem=self.send_sem.at[which, slot],
            recv_sem=self.recv_sem.at[which, slot],
            device_id=(flip(self.me, order[stage]),),
            device_id_type=MESH,
        )
        copy.start()
        self.copies[which][slot] = copy

    def pass_on(self):
        for which in range(3):
            for stage in range(self.steps):
                self.send(which, 0, stage)
        for stage in range(self.steps - 1):
            for at in range(1 << stage):
                for which in range(3):
                    order = self.orders[which]
                    pattern = subsets(order[:stage])[at] + order[stage]
                    self.copies[which][pattern].wait_recv()
                    for later in range(stage + 1, self.steps):
                        self.send(which, pattern, later)

    def arrive(self, which):
        order = self.orders[which]
        for pattern in subsets(order[:-1]):
            self.copies[which][pattern + order[-1]].wait_recv()

    def close(self):
        for copies in self.copies:
            for copy in copies.values():
                copy.wait_send()


def drain(ref, blocks, send_sem, recv_sem, peer):
    return pltpu.make_async_remote_copy(
        src_ref=ref.at[pl.ds(0, blocks)],
        dst_ref=ref.at[pl.ds(0, blocks)],
        send_sem=send_sem,
        recv_sem=recv_sem,
        device_id=(peer,),
        device_id_type=MESH,
    )


def flat(stages):
    return [bit for stage in stages for bit in stage]


def move(me, offset, bits):
    return place_with(me, bits, offset)


class StagedGather:
    def __init__(self, me, plans, fulls, send_sem, recv_sem):
        self.me, self.plans, self.fulls = me, plans, fulls
        self.send_sem, self.recv_sem = send_sem, recv_sem
        self.units = [gather_units(plan) for plan in plans]

    def fill(self, shards):
        for shard, full in zip(shards, self.fulls):
            rows, width = full.shape[1:]
            parts = width // LANES
            for part in range(parts):
                full[self.me, :, part * LANES : (part + 1) * LANES] = shard[
                    pl.ds(part, rows, stride=parts), :
                ].astype(jnp.bfloat16)

    def send(self, which, source, first):
        plan, full = self.plans[which], self.fulls[which]
        units, sems, _ = self.units[which]
        for stage in range(first, len(plan)):
            for offset in subsets(plan[stage])[1:][::-1]:
                peer = move(self.me, offset, plan[stage])
                for pattern in units[source][0] if source else [0]:
                    owner = move(self.me, pattern, flat(plan[:stage]))
                    pltpu.make_async_remote_copy(
                        src_ref=full.at[owner],
                        dst_ref=full.at[owner],
                        send_sem=self.send_sem.at[which],
                        recv_sem=self.recv_sem.at[which, sems[stage, offset, source]],
                        device_id=(peer,),
                        device_id_type=MESH,
                    ).start()

    def drain(self, which, blocks, at):
        return drain(
            self.fulls[which], blocks, self.send_sem.at[which], self.recv_sem.at[which, at],
            flip(self.me, 1),
        )

    def pass_on(self):
        for which in range(3):
            self.send(which, None, 0)
        names = [list(units[0]) for units in self.units]
        for at in range(max(len(some) for some in names)):
            for which in range(3):
                if at < len(names[which]):
                    name = names[which][at]
                    patterns, sem = self.units[which][0][name]
                    self.drain(which, len(patterns), sem).wait_recv()
                    self.send(which, name, name[0] + 1)

    def arrive(self, which):
        before = 1 << len(flat(self.plans[which][:-1]))
        self.drain(which, before, self.units[which][2] - 1).wait_recv()

    def close(self):
        for which in range(3):
            before = 1 << len(flat(self.plans[which]))
            self.drain(which, before - 1, 0).wait_send()


def gather_units(plan):
    units, sems, count = {}, {}, 0
    last = len(plan) - 1
    for stage, bits in enumerate(plan):
        offsets = subsets(bits)[1:]
        groups = [[offset] for offset in offsets] if stage + 1 < last else [offsets]
        sources = {None: [0], **{name: patterns for name, (patterns, _) in units.items()}}
        for name, patterns in sources.items():
            for group in groups:
                for offset in group:
                    sems[stage, offset, name] = count
                if stage < last:
                    arriving = [offset + at for offset in group for at in patterns]
                    units[stage, tuple(group), name] = (arriving, count)
                    count += 1
    return units, sems, count + 1


def greet_stages(me, plan, barrier):
    for bits in plan:
        for offset in subsets(bits)[1:]:
            pl.semaphore_signal(
                barrier, inc=1, device_id=(move(me, offset, bits),), device_id_type=MESH
            )


def stage_partners(plan):
    return sum((1 << len(bits)) - 1 for bits in plan)


def greet(me, devices, barrier):
    @pl.loop(1, devices)
    def _(shift):
        pl.semaphore_signal(
            barrier, inc=1, device_id=((me + shift) % devices,), device_id_type=MESH
        )


def gather_kernel(devices, w_up, w_down, w_out, full_up, full_down, full_out, send_sem, recv_sem):
    me = lax.axis_index("dp")
    barrier = pltpu.get_barrier_semaphore()
    greet(me, devices, barrier)
    gather = Gather(me, devices, (full_up, full_down, full_out), send_sem, recv_sem)
    gather.fill((w_up, w_down, w_out))
    pl.semaphore_wait(barrier, devices - 1)
    gather.pass_on()
    for which in range(3):
        gather.arrive(which)
    gather.close()


def gather_weights(devices, w_up, w_down, w_out):
    shapes = []
    for shard, width in ((w_up, FF), (w_down, D), (w_out, VOCAB)):
        shapes.append(
            jax.ShapeDtypeStruct((devices, shard.size // width, width), jnp.bfloat16)
        )
    return pl.pallas_call(
        functools.partial(gather_kernel, devices),
        out_shape=shapes,
        in_specs=[VMEM] * 3,
        out_specs=[VMEM] * 3,
        scratch_shapes=[
            pltpu.SemaphoreType.DMA((3, devices)),
            pltpu.SemaphoreType.DMA((3, devices)),
        ],
        compiler_params=pltpu.CompilerParams(collective_id=0, has_side_effects=True),
        name="gather_weights",
    )(w_up, w_down, w_out)


def dot_rows(left, right):
    return jnp.dot(left, right, preferred_element_type=jnp.float32)


def dot_last(left, right, precision=None):
    return lax.dot_general(
        left, right, (((1,), (1,)), ((), ())), precision=precision,
        preferred_element_type=jnp.float32,
    )


def dot_first(left, right):
    return lax.dot_general(
        left, right, (((0,), (0,)), ((), ())), preferred_element_type=jnp.float32
    )


def row_blocks(total, body):
    block = min(256, total)
    for step in range(total // block):
        body(pl.ds(step * block, block))


def normalize(features, normalized):
    def body(rows):
        flat_in = features[rows, :].astype(jnp.float32)
        centre = jnp.mean(flat_in, axis=1, keepdims=True)
        shifted = flat_in - centre
        spread = jnp.mean(shifted * shifted, axis=1, keepdims=True)
        normalized[rows, :] = (shifted * lax.rsqrt(spread + 1e-05)).astype(jnp.bfloat16)

    row_blocks(features.shape[0], body)


def project_up(normalized, up_mat, slopes, hidden):
    def body(rows):
        act = dot_rows(normalized[rows, :], up_mat[...].reshape(D, FF))
        sigmoid = 1.0 / (1.0 + jnp.exp(-act))
        slopes[rows, :] = sigmoid * (1.0 + act * (1.0 - sigmoid))
        hidden[rows, :] = (act * sigmoid).astype(jnp.bfloat16)

    row_blocks(normalized.shape[0], body)


def project_down(features, hidden, down_mat, out_mat, block_out, log_probs):
    def body(rows):
        flat_in = features[rows, :].astype(jnp.float32)
        out_rows = (flat_in + 0.5 * dot_rows(hidden[rows, :], down_mat[...].reshape(FF, D))).astype(
            jnp.bfloat16
        )
        block_out[rows, :] = out_rows
        logits = dot_rows(out_rows, out_mat[...].reshape(D, VOCAB))
        top = jnp.max(logits, axis=1, keepdims=True)
        low = (logits - top) * LOG2E
        log_probs[rows, :] = low - jnp.log2(jnp.sum(jnp.exp2(low), axis=1, keepdims=True))

    row_blocks(features.shape[0], body)


def split_dot(dot, values, picks):
    high = values.astype(jnp.bfloat16)
    rest = values - high.astype(jnp.float32)
    middle = rest.astype(jnp.bfloat16)
    low = (rest - middle.astype(jnp.float32)).astype(jnp.bfloat16)
    return dot(high, picks) + (dot(middle, picks) + dot(low, picks))


def ctc_rows(frames):
    return [pltpu.VMEM((8 * frames, LANES), jnp.float32)] * 4 + [
        pltpu.VMEM((16 * frames, LANES), jnp.float32)
    ] * 4


class Lattice:
    def __init__(self, parts, sign, skip):
        self.parts, self.sign = parts, sign
        self.row = 0 if sign > 0 else 7
        self.skips = [self.spread(skip, part) > 0.5 for part in range(parts)]

    def spread(self, values, part):
        if self.sign > 0:
            return pltpu.roll(values, part, 1, stride=self.parts, stride_axis=0)
        shift = LANES - part - 7 * self.parts
        return pltpu.roll(values, shift, 1, stride=self.parts, stride_axis=0)

    def begin(self, blank, label):
        def whole(values):
            return jnp.broadcast_to(values[self.row : self.row + 1], (8, LANES))

        blank, label = whole(blank), whole(label)
        return tuple(
            [self.spread(blank, part) for part in range(self.parts)]
            + [self.spread(label, part) for part in range(self.parts + 1)]
        )

    def enter(self, moved):
        self.blank, self.label = list(moved[: self.parts]), list(moved[self.parts :])
        one = jnp.ones((8, LANES), jnp.float32)
        self.blank_mass, self.label_mass = [one] * self.parts, [one] * (self.parts + 1)

    def next_rows(self, values):
        return pltpu.roll(values, 7 if self.sign > 0 else 1, 0)

    def advance(self, emit_blank, emit_label, parts):
        blank, label, blank_mass, label_mass = [], [], [], []
        for part in range(parts):
            b, l, l1 = self.blank[part], self.label[part], self.label[part + 1]
            bm, lm, lm1 = self.blank_mass[part], self.label_mass[part], self.label_mass[part + 1]
            top = jnp.maximum(b, l1)
            mass = bm * jnp.exp2(b - top) + lm1 * jnp.exp2(l1 - top)
            above = jnp.where(self.skips[part], top, b)
            above_mass = jnp.where(self.skips[part], mass, bm)
            peak = jnp.maximum(l, above)
            peak_mass = lm * jnp.exp2(l - peak) + above_mass * jnp.exp2(above - peak)
            if part == 0:
                result = (top, mass, peak, peak_mass)
            blank.append(top + emit_blank)
            label.append(peak + self.spread(emit_label, part))
            blank_mass.append(mass)
            label_mass.append(peak_mass)
        if parts == self.parts:
            label.append(self.next_rows(label[0]))
            label_mass.append(self.next_rows(label_mass[0]))
        self.blank, self.label = blank, label
        self.blank_mass, self.label_mass = blank_mass, label_mass
        return result


def ctc_grad(
    loss_scale,
    frame_lens,
    label_lens,
    labels,
    log_probs,
    emitted,
    emitted_blank,
    alpha_rows,
    beta_rows,
    logit_grad,
):
    utterances, label_count = labels.shape
    frames = log_probs.shape[0] // utterances
    half = LANES // utterances
    depth = 8 * PARTS
    assert label_count + depth <= half and frames % depth == 0

    lane_row = lax.broadcasted_iota(jnp.int32, (8, LANES), 1)
    label_ids = lax.broadcasted_iota(jnp.int32, (label_count, LANES), 0)
    spread_lanes = lax.broadcasted_iota(jnp.int32, (label_count, LANES), 1)
    label_rows = jnp.concatenate(
        [
            labels[...].astype(jnp.float32),
            jnp.zeros((8 - utterances, label_count), jnp.float32),
        ],
        axis=0,
    ).astype(jnp.bfloat16)
    extended = jnp.zeros((8, LANES), jnp.float32)
    for utterance in range(utterances):
        spread = (spread_lanes == label_ids + half * utterance + 1).astype(jnp.bfloat16)
        placed = dot_rows(label_rows, spread)[utterance : utterance + 1]
        extended = extended + jnp.broadcast_to(placed, (8, LANES))
    skip = jnp.where(extended != pltpu.roll(extended, 1, 1), 1.0, 0.0)
    skip_back = pltpu.roll(skip, LANES - 1, 1)

    vocab_ids = lax.broadcasted_iota(jnp.int32, (VOCAB, LANES), 0).astype(jnp.float32)
    vocab_lanes = lax.broadcasted_iota(jnp.int32, (VOCAB, LANES), 1)
    frame_lanes = lax.broadcasted_iota(jnp.int32, (frames, LANES), 1)
    onehots = []
    picked = None
    blanks = None
    for utterance in range(utterances):
        rows = slice(utterance * frames, (utterance + 1) * frames)
        first = half * utterance + 1
        mine = (vocab_lanes >= first) & (vocab_lanes < first + label_count)
        onehot = jnp.where((vocab_ids == extended[0:1, :]) & mine, 1.0, 0.0).astype(jnp.bfloat16)
        onehots.append(onehot)
        picks = split_dot(dot_rows, log_probs[rows, :], onehot)
        blank = jnp.broadcast_to(log_probs[rows, 0:1], (frames, LANES))
        if utterance == 0:
            picked, blanks = picks, blank
        else:
            picked = jnp.where(frame_lanes < half * utterance, picked, picks)
            blanks = jnp.where(frame_lanes < half * utterance, blanks, blank)
    place = frame_lanes % half
    emitted[...] = jnp.where((place >= 1) & (place <= label_count), picked, negative)
    emitted_blank[...] = blanks

    forward = Lattice(PARTS, 1, skip)
    backward = Lattice(PARTS, -1, skip_back)
    start = jnp.full((8, LANES), negative, jnp.float32)
    start_back = start
    for utterance in range(utterances):
        first = half * utterance + 1
        start = jnp.where(lane_row == first, 0.0, start)
        start_back = jnp.where(
            lane_row == first + label_lens[utterance] - 1, 0.0, start_back
        )
    nothing = jnp.full((8, LANES), negative, jnp.float32)

    def tile(frame):
        return pl.ds(pl.multiple_of(frame * 8, 8), 8)

    def row_of(ref, frame):
        return jnp.broadcast_to(ref[pl.ds(frame, 1), :], (8, LANES))

    def leave(lattice):
        return (
            lattice.blank[0] + jnp.log2(lattice.blank_mass[0]),
            lattice.label[0] + jnp.log2(lattice.label_mass[0]),
        )

    def step_back(at, level):
        frame = at * depth + level
        emit = emit_blank = None
        for utterance in range(utterances):
            back = jnp.maximum(frame_lens[utterance] - 1 - frame, 0)
            mine, mine_blank = row_of(emitted, back), row_of(emitted_blank, back)
            if utterance == 0:
                emit, emit_blank = mine, mine_blank
            else:
                emit = jnp.where(lane_row < half * utterance, emit, mine)
                emit_blank = jnp.where(lane_row < half * utterance, emit_blank, mine_blank)
        result = backward.advance(emit_blank, emit, min(PARTS, depth - level))
        for ref, value in zip(beta_rows, result):
            ref[tile(frames - 1 - frame), :] = value

    def step_ahead(at, level):
        frame = at * depth + level
        result = forward.advance(
            row_of(emitted_blank, frame), row_of(emitted, frame), min(PARTS, depth - level)
        )
        for ref, value in zip(alpha_rows, result):
            ref[tile(frame), :] = value

    def block(at, carry):
        forward.enter(forward.begin(*carry[:2]))
        backward.enter(backward.begin(*carry[2:]))
        for level in range(depth):
            step_ahead(at, level)
            step_back(at, level)
        return leave(forward) + leave(backward)

    lax.fori_loop(
        0, frames // depth, block, (start, nothing, start_back, nothing)
    )

    frame_ids = lax.broadcasted_iota(jnp.int32, (frames, LANES), 0)
    alphas = [ref[pl.ds(forward.row, frames, stride=8), :] for ref in alpha_rows]
    betas, alive = [], None
    for ref in beta_rows:
        value = None
        for utterance in range(utterances):
            first = 8 * (frames - frame_lens[utterance]) + backward.row
            mine = ref[pl.ds(first, frames, stride=8), :]
            value = mine if value is None else jnp.where(frame_lanes < half * utterance, value, mine)
        betas.append(value)
    betas[0], betas[1] = pltpu.roll(betas[0], 1, 1), pltpu.roll(betas[1], 1, 1)
    joint_blank = alphas[0] + emitted_blank[...] + betas[0]
    joint_label = alphas[2] + emitted[...] + betas[2]
    blank_mass, label_mass = alphas[1] * betas[1], alphas[3] * betas[3]
    both = jnp.maximum(joint_blank, joint_label)
    for utterance in range(utterances):
        rows = slice(utterance * frames, (utterance + 1) * frames)
        first = half * utterance
        mine = (frame_lanes >= first) & (frame_lanes < first + half)
        top = jnp.max(jnp.where(mine, both, negative), axis=1, keepdims=True)
        live = mine & (frame_ids < frame_lens[utterance])
        label = jnp.where(live, label_mass * jnp.exp2(joint_label - top), 0.0)
        blank = jnp.where(live, blank_mass * jnp.exp2(joint_blank - top), 0.0)
        blank_sum = jnp.sum(blank, axis=1, keepdims=True)
        total = jnp.sum(label, axis=1, keepdims=True) + blank_sum
        kept = frame_ids[:, 0:1] < frame_lens[utterance]
        scale = jnp.where(kept, 1.0 / jnp.where(kept, total, 1.0), 0.0)
        gamma = split_dot(dot_last, label * scale, onehots[utterance])
        vocab_at = lax.broadcasted_iota(jnp.int32, (frames, VOCAB), 1)
        gamma = gamma + jnp.where(vocab_at == 0, blank_sum * scale, 0.0)
        probs = jnp.exp2(log_probs[rows, :]) * jnp.where(kept, 1.0, 0.0)
        logit_grad[rows, :] = (loss_scale * (probs - gamma)).astype(jnp.bfloat16)


def grad_ff(logit_grad, out_mat, ff_grad):
    def body(rows):
        ff_grad[rows, :] = (
            0.5 * dot_last(logit_grad[rows, :], out_mat[...].reshape(D, VOCAB))
        ).astype(jnp.bfloat16)

    row_blocks(logit_grad.shape[0], body)


def grad_act(ff_grad, down_mat, slopes, act_grad):
    def body(rows):
        act_grad[rows, :] = (
            dot_last(ff_grad[rows, :], down_mat[...].reshape(FF, D)) * slopes[rows, :]
        ).astype(jnp.bfloat16)

    row_blocks(ff_grad.shape[0], body)


def step_kernel(
    loss_scale,
    frame_lens,
    label_lens,
    features,
    labels,
    up_mat,
    down_mat,
    out_mat,
    grad_up,
    grad_down,
    grad_out,
    normalized,
    slopes,
    hidden,
    block_out,
    log_probs,
    logit_grad,
    ff_grad,
    act_grad,
    emitted,
    emitted_blank,
    *lattice_rows,
):
    normalize(features, normalized)
    project_up(normalized, up_mat, slopes, hidden)
    project_down(features, hidden, down_mat, out_mat, block_out, log_probs)
    ctc_grad(
        loss_scale, frame_lens, label_lens, labels, log_probs, emitted, emitted_blank,
        lattice_rows[:4], lattice_rows[4:], logit_grad,
    )
    grad_ff(logit_grad, out_mat, ff_grad)
    grad_act(ff_grad, down_mat, slopes, act_grad)
    grad_up[...] = dot_first(normalized[...], act_grad[...])
    grad_down[...] = dot_first(hidden[...], ff_grad[...])
    grad_out[...] = dot_first(block_out[...], logit_grad[...])


def step_scratch(total, frames):
    return [
        pltpu.VMEM((total, D), jnp.bfloat16),
        pltpu.VMEM((total, FF), jnp.float32),
        pltpu.VMEM((total, FF), jnp.bfloat16),
        pltpu.VMEM((total, D), jnp.bfloat16),
        pltpu.VMEM((total, VOCAB), jnp.float32),
        pltpu.VMEM((total, VOCAB), jnp.bfloat16),
        pltpu.VMEM((total, D), jnp.bfloat16),
        pltpu.VMEM((total, FF), jnp.bfloat16),
        pltpu.VMEM((frames, LANES), jnp.float32),
        pltpu.VMEM((frames, LANES), jnp.float32),
    ] + ctc_rows(frames)


def local_step(loss_scale, frame_lens, label_lens, features, labels, up_mat, down_mat, out_mat):
    total = features.shape[0]
    frames = total // labels.shape[0]
    return pl.pallas_call(
        functools.partial(step_kernel, loss_scale),
        out_shape=[
            jax.ShapeDtypeStruct((D, FF), jnp.float32),
            jax.ShapeDtypeStruct((FF, D), jnp.float32),
            jax.ShapeDtypeStruct((D, VOCAB), jnp.float32),
        ],
        in_specs=[SMEM, SMEM] + [VMEM] * 5,
        out_specs=[VMEM] * 3,
        scratch_shapes=step_scratch(total, frames),
        compiler_params=pltpu.CompilerParams(vmem_limit_bytes=40 << 20),
        name="local_step",
    )(frame_lens, label_lens, features, labels, up_mat, down_mat, out_mat)


class Sum:
    def __init__(self, me, devices, grads, received, staged, send_sem, recv_sem):
        self.me, self.grads, self.received, self.staged = me, grads, received, staged
        self.send_sem, self.recv_sem = send_sem, recv_sem
        self.orders = [order[::-1] for order in bit_orders(devices)]
        self.steps = len(self.orders[0])
        self.copies = [{}, {}, {}]

    def sum_of(self, which, place, pattern, stage):
        value = self.grads[which][place]
        for bit in self.orders[which][:stage]:
            self.copies[which][pattern + bit].wait_recv()
            value = value + self.received[which][pattern + bit]
        return value

    def send(self, which, stage):
        order = self.orders[which]
        for offset in subsets(order[stage + 1 :][::-1])[::-1]:
            slot = offset + order[stage]
            place = place_with(self.me, order, slot)
            if stage == 0:
                source = self.grads[which].at[place]
            else:
                self.staged[which][slot] = self.sum_of(which, place, slot, stage)
                source = self.staged[which].at[slot]
            copy = pltpu.make_async_remote_copy(
                src_ref=source,
                dst_ref=self.received[which].at[slot],
                send_sem=self.send_sem.at[which, slot],
                recv_sem=self.recv_sem.at[which, slot],
                device_id=(flip(self.me, order[stage]),),
                device_id_type=MESH,
            )
            copy.start()
            self.copies[which][slot] = copy

    def finish(self, devices, reduced, squares, own_squares, small_send, small_recv):
        me = self.me
        own = jnp.zeros((1, LANES), jnp.float32)
        for which in (2, 1, 0):
            value = self.sum_of(which, me, 0, self.steps)
            rows, width = value.shape
            parts = width // LANES
            for part in range(parts):
                piece = value[:, part * LANES : (part + 1) * LANES]
                reduced[which][pl.ds(part, rows, stride=parts), :] = piece
                own = own + jnp.sum(piece * piece, axis=0, keepdims=True)
        own_squares[...] = own
        squares[0] = own

        def small_copy(shift):
            return pltpu.make_async_remote_copy(
                src_ref=own_squares,
                dst_ref=squares.at[shift],
                send_sem=small_send.at[shift],
                recv_sem=small_recv.at[shift],
                device_id=((me + shift) % devices,),
                device_id_type=MESH,
            )

        @pl.loop(1, devices)
        def _(shift):
            small_copy(shift).start()

        for copies in self.copies:
            for copy in copies.values():
                copy.wait_send()

        @pl.loop(1, devices)
        def _(shift):
            small_copy(shift).wait()


def sum_pieces(plan):
    pieces = {}
    for stage in range(len(plan)):
        for after in subsets(plan[stage + 1]) if stage + 1 < len(plan) else [0]:
            pieces[stage, after] = len(pieces)
    return pieces


def far_first(offset, bits):
    core, near, far = bits[:1], bits[1:3], bits[3:]
    weights = [1] * len(core) + [3] * len(near) + [3 << at for at in range(len(far))]
    return sum(weight for weight, bit in zip(weights, bits) if offset & bit)


class StagedSum:
    def __init__(self, me, plans, narrow, grads, received, staged, send_sem, recv_sem):
        self.me, self.plans, self.narrow = me, plans, narrow
        self.grads, self.received, self.staged = grads, received, staged
        self.send_sem, self.recv_sem = send_sem, recv_sem
        self.pieces = [sum_pieces(plan) for plan in plans]
        self.seen = set()

    def index(self, which, pattern):
        bits = flat(self.plans[which])
        return sum(1 << at for at, bit in enumerate(bits[::-1]) if pattern & bit)

    def wide(self, which, stage):
        return 3 * (stage in self.narrow[which]) + which

    def put(self, which, value):
        bits = flat(self.plans[which])[::-1]
        blocks, rows, width = self.grads[which].shape
        own = [(self.me // bit) % 2 for bit in bits]
        for block in range(blocks):
            slot = 0
            for at, bit in enumerate(bits):
                slot = slot + (1 << at) * (1 - own[at] if block & bit else own[at])
            self.grads[which][slot] = value[block * rows : (block + 1) * rows, :]

    def copy(self, which, name):
        stage, offset, after = name
        start = self.index(which, offset + after)
        blocks = pl.ds(start, 1 << len(flat(self.plans[which][stage + 2 :])))
        at = self.wide(which, stage)
        source = self.grads[which] if stage == 0 else self.staged[at]
        return pltpu.make_async_remote_copy(
            src_ref=source.at[blocks],
            dst_ref=self.received[at].at[blocks],
            send_sem=self.send_sem.at[at],
            recv_sem=self.recv_sem.at[which, self.pieces[which][stage, after]],
            device_id=(move(self.me, offset, self.plans[which][stage]),),
            device_id_type=MESH,
        )

    def wait(self, which, stage, after):
        plan = self.plans[which]
        blocks = ((1 << len(plan[stage])) - 1) << len(flat(plan[stage + 2 :]))
        at = self.wide(which, stage)
        drain(
            self.received[at], blocks, self.send_sem.at[at],
            self.recv_sem.at[which, self.pieces[which][stage, after]], flip(self.me, 1),
        ).wait_recv()

    def sum_of(self, which, pattern, stage):
        value = self.grads[which][self.index(which, pattern)]
        for earlier in range(stage):
            after = 0
            if earlier + 1 < len(self.plans[which]):
                after = sum(bit for bit in self.plans[which][earlier + 1] if pattern & bit)
            if (which, earlier, after) not in self.seen:
                self.seen.add((which, earlier, after))
                self.wait(which, earlier, after)
            for offset in subsets(self.plans[which][earlier])[1:]:
                slot = self.index(which, pattern + offset)
                value = value + self.received[self.wide(which, earlier)][slot].astype(jnp.float32)
        return value

    def send(self, which, stage):
        plan = self.plans[which]
        afters = subsets(plan[stage + 1])[::-1] if stage + 1 < len(plan) else [0]
        for after in afters:
            for offset in subsets(plan[stage])[1:][::-1]:
                if stage:
                    staged = self.staged[self.wide(which, stage)]
                    for later in subsets(flat(plan[stage + 2 :])):
                        pattern = offset + after + later
                        staged[self.index(which, pattern)] = self.sum_of(
                            which, pattern, stage
                        ).astype(staged.dtype)
                self.copy(which, (stage, offset, after)).start()

    def finish(self, devices, reduced, squares, own_squares, small_send, small_recv):
        me = self.me
        own = jnp.zeros((1, LANES), jnp.float32)
        for which in (2, 1, 0):
            value = self.sum_of(which, 0, len(self.plans[which]))
            rows, width = value.shape
            parts = width // LANES
            for part in range(parts):
                piece = value[:, part * LANES : (part + 1) * LANES]
                reduced[which][pl.ds(part, rows, stride=parts), :] = piece
                own = own + jnp.sum(piece * piece, axis=0, keepdims=True)
        own_squares[...] = own
        squares[0] = own

        bits = [1 << k for k in range(devices.bit_length() - 1)]
        for offset in sorted(subsets(bits)[1:], key=lambda at: -far_first(at, bits)):
            pltpu.make_async_remote_copy(
                src_ref=own_squares,
                dst_ref=squares.at[offset],
                send_sem=small_send,
                recv_sem=small_recv,
                device_id=(move(me, offset, bits),),
                device_id_type=MESH,
            ).start()

        for which, plan in enumerate(self.plans):
            sent = {}
            for stage, bits in enumerate(plan):
                blocks = ((1 << len(bits)) - 1) << len(flat(plan[stage + 1 :]))
                at = self.wide(which, stage)
                sent[at] = sent.get(at, 0) + blocks
            for at, blocks in sent.items():
                drain(
                    self.received[at], blocks, self.send_sem.at[at], self.recv_sem.at[which, 0],
                    flip(me, 1),
                ).wait_send()
        small = drain(squares, devices - 1, small_send, small_recv, flip(me, 1))
        small.wait_send()
        small.wait_recv()


def sum_kernel(devices, *refs):
    grads, reduced, squares = refs[:3], refs[3:6], refs[6]
    received, staged = refs[7:10], refs[10:13]
    own_squares, send_sem, recv_sem, small_send, small_recv = refs[13:]
    me = lax.axis_index("dp")
    barrier = pltpu.get_barrier_semaphore()
    greet(me, devices, barrier)
    pl.semaphore_wait(barrier, devices - 1)
    total = Sum(me, devices, grads, received, staged, send_sem, recv_sem)
    for stage in range(total.steps):
        for which in range(3):
            total.send(which, stage)
    total.finish(devices, reduced, squares, own_squares, small_send, small_recv)


def exchange_plans(devices):
    bits = [1 << k for k in range(devices.bit_length() - 1)]
    core, near, far = bits[:1], bits[1:3], bits[3:]
    gathers = ([far, near, core], [far, near, core], [near, far, core])
    sums = ([core, near, far], [core, near, far], [core, far, near])
    narrow = ((1, 2), (1,), (1,))
    return gathers, sums, narrow


def meet_plan(devices):
    bits = [1 << k for k in range(devices.bit_length() - 1)]
    core, near, far = bits[:1], bits[1:3], bits[3:]
    return [core, near, far]


def fused_kernel(devices, loss_scale, *refs):
    frame_lens, label_lens, features, labels = refs[:4]
    shards, reduced, squares = refs[4:7], refs[7:10], refs[10]
    fulls, grads, received, staged = refs[11:14], refs[14:17], refs[17:23], refs[23:29]
    gather_send, gather_recv, own_squares, send_sem, recv_sem, small_send, small_recv = refs[29:36]
    normalized, slopes, hidden, block_out, log_probs = refs[36:41]
    logit_grad, ff_grad, act_grad, emitted, emitted_blank = refs[41:46]
    alpha_rows, beta_rows = refs[46:50], refs[50:54]
    held, load_sem = refs[54:58], refs[58]
    up_mat, down_mat, out_mat = fulls
    me = lax.axis_index("dp")
    loads = [
        pltpu.make_async_copy(source, target, load_sem.at[at])
        for at, (source, target) in enumerate(zip((*shards, features), held))
    ]
    for load in loads:
        load.start()
    shards, features = held[:3], held[3]
    barrier = pltpu.get_barrier_semaphore()
    gathers, sums, narrow = exchange_plans(devices)
    greet_stages(me, meet_plan(devices), barrier)
    gather = StagedGather(me, gathers, fulls, gather_send, gather_recv)
    for load in loads[:3]:
        load.wait()
    gather.fill(shards)
    loads[3].wait()
    normalize(features, normalized)
    pl.semaphore_wait(barrier, stage_partners(meet_plan(devices)))
    gather.pass_on()
    gather.arrive(0)
    project_up(normalized, up_mat, slopes, hidden)
    gather.arrive(1)
    gather.arrive(2)
    project_down(features, hidden, down_mat, out_mat, block_out, log_probs)
    ctc_grad(
        loss_scale, frame_lens, label_lens, labels, log_probs, emitted, emitted_blank, alpha_rows,
        beta_rows, logit_grad,
    )
    total = StagedSum(me, sums, narrow, grads, received, staged, send_sem, recv_sem)
    pending = [list(range(len(plan))) for plan in sums]

    def advance(*whiches):
        for which in whiches:
            if pending[which]:
                total.send(which, pending[which].pop(0))

    grad_ff(logit_grad, out_mat, ff_grad)
    total.put(1, dot_first(hidden[...], ff_grad[...]))
    advance(1)
    grad_act(ff_grad, down_mat, slopes, act_grad)
    advance(1)
    total.put(2, dot_first(block_out[...], logit_grad[...]))
    advance(2)
    total.put(0, dot_first(normalized[...], act_grad[...]))
    advance(0)
    advance(2, 0, 1, 0, 2)
    total.finish(devices, reduced, squares, own_squares, small_send, small_recv)
    gather.close()


def fused_step(loss_scale, devices, frame_lens, label_lens, features, labels, weights):
    total = features.shape[0]
    frames = total // labels.shape[0]
    blocks = [
        (devices, weight.size // width, width)
        for weight, width in zip(weights, (FF, D, VOCAB))
    ]
    gathers, sums, _ = exchange_plans(devices)
    wide = [pltpu.VMEM(block, jnp.float32) for block in blocks]
    both = wide + [pltpu.VMEM(block, jnp.bfloat16) for block in blocks]
    return pl.pallas_call(
        functools.partial(fused_kernel, devices, loss_scale),
        out_shape=[jax.ShapeDtypeStruct(weight.shape, jnp.float32) for weight in weights]
        + [jax.ShapeDtypeStruct((devices, 1, LANES), jnp.float32)],
        in_specs=[SMEM, SMEM, HBM, VMEM] + [HBM] * 3,
        out_specs=[VMEM] * 4,
        scratch_shapes=[pltpu.VMEM(block, jnp.bfloat16) for block in blocks]
        + wide
        + both * 2
        + [
            pltpu.SemaphoreType.DMA((3,)),
            pltpu.SemaphoreType.DMA((3, max(gather_units(plan)[2] for plan in gathers))),
            pltpu.VMEM((1, LANES), jnp.float32),
            pltpu.SemaphoreType.DMA((6,)),
            pltpu.SemaphoreType.DMA((3, max(len(sum_pieces(plan)) for plan in sums))),
            pltpu.SemaphoreType.DMA,
            pltpu.SemaphoreType.DMA,
        ]
        + step_scratch(total, frames)
        + [pltpu.VMEM(array.shape, array.dtype) for array in (*weights, features)]
        + [pltpu.SemaphoreType.DMA((4,))],
        compiler_params=pltpu.CompilerParams(
            collective_id=2, has_side_effects=True, vmem_limit_bytes=34 << 20
        ),
        name="fused_step",
    )(*(pltpu.with_memory_space_constraint(array, pltpu.HBM) for array in (frame_lens, label_lens, features, labels, *weights)))


def sum_gradients(devices, grads):
    blocks = [grad.reshape(devices, grad.shape[0] // devices, grad.shape[1]) for grad in grads]
    shapes = [
        jax.ShapeDtypeStruct((block[0].size // LANES, LANES), jnp.float32) for block in blocks
    ]
    buffers = [pltpu.VMEM(block.shape, jnp.float32) for block in blocks]
    return pl.pallas_call(
        functools.partial(sum_kernel, devices),
        out_shape=shapes + [jax.ShapeDtypeStruct((devices, 1, LANES), jnp.float32)],
        in_specs=[VMEM] * 3,
        out_specs=[VMEM] * 4,
        scratch_shapes=buffers
        + buffers
        + [
            pltpu.VMEM((1, LANES), jnp.float32),
            pltpu.SemaphoreType.DMA((3, devices)),
            pltpu.SemaphoreType.DMA((3, devices)),
            pltpu.SemaphoreType.DMA((devices,)),
            pltpu.SemaphoreType.DMA((devices,)),
        ],
        compiler_params=pltpu.CompilerParams(
            collective_id=1, has_side_effects=True, vmem_limit_bytes=50 << 20
        ),
        name="sum_gradients",
    )(*blocks)


def adam_kernel(squares, *refs):
    weights, firsts, seconds, grads, outs = (refs[at : at + 3] for at in (0, 3, 6, 9, 12))
    new_firsts, new_seconds = refs[15:18], refs[18:21]
    total = jnp.sum(squares[...])
    clip = 1.0 / jnp.maximum(jnp.sqrt(jnp.full((1, LANES), total)), 1.0)
    for which in range(3):
        scaled = clip * grads[which][...]
        first = 0.9 * firsts[which][...] + 0.1 * scaled
        second = 0.999 * seconds[which][...] + 0.001 * scaled * scaled
        ratio = first / first_correction / (jnp.sqrt(second / second_correction) + 1e-08)
        outs[which][...] = weights[which][...] - 0.001 * ratio
        new_firsts[which][...] = first
        new_seconds[which][...] = second


def adam(squares, weights, firsts, seconds, grads):
    shapes = [jax.ShapeDtypeStruct(weight.shape, jnp.float32) for weight in weights]
    return pl.pallas_call(
        adam_kernel,
        out_shape=shapes * 3,
        in_specs=[VMEM] * 13,
        out_specs=[VMEM] * 9,
        compiler_params=pltpu.CompilerParams(vmem_limit_bytes=4 << 20),
        name="adam",
    )(squares, *weights, *firsts, *seconds, *grads)


def per_device(
    features,
    frame_lens,
    labels,
    label_lens,
    w_up,
    w_down,
    w_out,
    first_up,
    first_down,
    first_out,
    second_up,
    second_down,
    second_out,
):
    devices = lax.axis_size("dp")
    batch, frames, width = features.shape

    def lined(*arrays):
        return [array.reshape(array.shape[0] // LANES, LANES) for array in arrays]

    weights = lined(w_up, w_down, w_out)
    loss_scale = 1.0 / (batch * devices)
    rows_in = features.reshape(batch * frames, width)
    if w_up.size % (8 * FF) == 0 and w_out.size % (8 * VOCAB) == 0:
        *shares, squares = fused_step(
            loss_scale, devices, frame_lens, label_lens, rows_in, labels, weights
        )
    else:
        full_up, full_down, full_out = gather_weights(devices, *weights)
        grads = local_step(
            loss_scale,
            frame_lens,
            label_lens,
            rows_in,
            labels,
            full_up.reshape(D, FF),
            full_down.reshape(FF, D),
            full_out.reshape(D, VOCAB),
        )
        *shares, squares = sum_gradients(devices, grads)
    results = adam(
        squares,
        weights,
        lined(first_up, first_down, first_out),
        lined(second_up, second_down, second_out),
        shares,
    )
    return tuple(result.reshape(-1) for result in results)


def solution(mesh):
    flat = P("dp")
    return jax.shard_map(
        per_device,
        mesh=mesh,
        in_specs=(P("dp", None, None), flat, P("dp", None), flat) + (flat,) * 9,
        out_specs=(flat,) * 9,
        check_vma=False,
    )
```

```python
import functools

import jax
import jax.numpy as jnp
from jax import lax
from jax.experimental import pallas as pl
from jax.experimental.pallas import tpu as pltpu
from jax.sharding import PartitionSpec as P

D = 256
FF = 1024
VOCAB = 256
LANES = 128
MESH = pl.DeviceIdType.MESH

first_correction = 1.0 - (0.9**10) ** 10
second_correction = 1.0 - (0.999**10) ** 10
negative = -1e30
LOG2E = 1.4426950408889634
PARTS = 2
VMEM = pl.BlockSpec(memory_space=pltpu.VMEM)
SMEM = pl.BlockSpec(memory_space=pltpu.SMEM)
HBM = pl.BlockSpec(memory_space=pltpu.HBM)


def flip(me, bit):
    return me + bit - 2 * bit * ((me // bit) % 2)


def bit_orders(devices):
    bits = [1 << k for k in range(devices.bit_length() - 1)]
    core, rest = bits[:1], bits[1:]
    down = rest[::-1]
    swapped = down[:-2] + down[-2:][::-1]
    turned = down[-2:] + down[:-2]
    return (down + core, swapped + core, turned + core)


def subsets(bits):
    offsets = [0]
    for bit in bits:
        offsets = offsets + [offset + bit for offset in offsets]
    return offsets


def place_with(me, free, pattern):
    place = me
    for bit in free:
        if pattern & bit:
            place = flip(place, bit)
    return place


class Gather:
    def __init__(self, me, devices, fulls, send_sem, recv_sem):
        self.me, self.fulls = me, fulls
        self.send_sem, self.recv_sem = send_sem, recv_sem
        self.orders = bit_orders(devices)
        self.steps = len(self.orders[0])
        self.copies = [{}, {}, {}]

    def fill(self, shards):
        for shard, full in zip(shards, self.fulls):
            rows, width = full.shape[1:]
            parts = width // LANES
            for part in range(parts):
                full[self.me, :, part * LANES : (part + 1) * LANES] = shard[
                    pl.ds(part, rows, stride=parts), :
                ].astype(jnp.bfloat16)

    def send(self, which, pattern, stage):
        order, full = self.orders[which], self.fulls[which]
        owner = place_with(self.me, order[:stage], pattern)
        slot = pattern + order[stage]
        copy = pltpu.make_async_remote_copy(
            src_ref=full.at[owner],
            dst_ref=full.at[owner],
            send_sem=self.send_sem.at[which, slot],
            recv_sem=self.recv_sem.at[which, slot],
            device_id=(flip(self.me, order[stage]),),
            device_id_type=MESH,
        )
        copy.start()
        self.copies[which][slot] = copy

    def pass_on(self):
        for which in range(3):
            for stage in range(self.steps):
                self.send(which, 0, stage)
        for stage in range(self.steps - 1):
            for at in range(1 << stage):
                for which in range(3):
                    order = self.orders[which]
                    pattern = subsets(order[:stage])[at] + order[stage]
                    self.copies[which][pattern].wait_recv()
                    for later in range(stage + 1, self.steps):
                        self.send(which, pattern, later)

    def arrive(self, which):
        order = self.orders[which]
        for pattern in subsets(order[:-1]):
            self.copies[which][pattern + order[-1]].wait_recv()

    def close(self):
        for copies in self.copies:
            for copy in copies.values():
                copy.wait_send()


def drain(ref, blocks, send_sem, recv_sem, peer):
    return pltpu.make_async_remote_copy(
        src_ref=ref.at[pl.ds(0, blocks)],
        dst_ref=ref.at[pl.ds(0, blocks)],
        send_sem=send_sem,
        recv_sem=recv_sem,
        device_id=(peer,),
        device_id_type=MESH,
    )


def flat(stages):
    return [bit for stage in stages for bit in stage]


def move(me, offset, bits):
    return place_with(me, bits, offset)


class StagedGather:
    def __init__(self, me, plans, fulls, send_sem, recv_sem):
        self.me, self.plans, self.fulls = me, plans, fulls
        self.send_sem, self.recv_sem = send_sem, recv_sem
        self.units = [gather_units(plan) for plan in plans]

    def fill(self, shards):
        for shard, full in zip(shards, self.fulls):
            rows, width = full.shape[1:]
            parts = width // LANES
            for part in range(parts):
                full[self.me, :, part * LANES : (part + 1) * LANES] = shard[
                    pl.ds(part, rows, stride=parts), :
                ].astype(jnp.bfloat16)

    def send(self, which, source, first, end=None):
        plan, full = self.plans[which], self.fulls[which]
        units, sems, _ = self.units[which]
        for stage in range(first, end or len(plan)):
            for offset in subsets(plan[stage])[1:][::-1]:
                peer = move(self.me, offset, plan[stage])
                for pattern in units[source][0] if source else [0]:
                    owner = move(self.me, pattern, flat(plan[:stage]))
                    pltpu.make_async_remote_copy(
                        src_ref=full.at[owner],
                        dst_ref=full.at[owner],
                        send_sem=self.send_sem.at[which],
                        recv_sem=self.recv_sem.at[which, sems[stage, offset, source]],
                        device_id=(peer,),
                        device_id_type=MESH,
                    ).start()

    def drain(self, which, blocks, at):
        return drain(
            self.fulls[which], blocks, self.send_sem.at[which], self.recv_sem.at[which, at],
            flip(self.me, 1),
        )

    def pass_on(self):
        for stage in range(max(len(plan) for plan in self.plans)):
            for which in range(3):
                self.send(which, None, stage, stage + 1)
        names = [list(units[0]) for units in self.units]
        for at in range(max(len(some) for some in names)):
            for which in range(3):
                if at < len(names[which]):
                    name = names[which][at]
                    patterns, sem = self.units[which][0][name]
                    self.drain(which, len(patterns), sem).wait_recv()
                    self.send(which, name, name[0] + 1)

    def arrive(self, which):
        before = 1 << len(flat(self.plans[which][:-1]))
        self.drain(which, before, self.units[which][2] - 1).wait_recv()

    def close(self):
        for which in range(3):
            before = 1 << len(flat(self.plans[which]))
            self.drain(which, before - 1, 0).wait_send()


def gather_units(plan):
    units, sems, count = {}, {}, 0
    last = len(plan) - 1
    for stage, bits in enumerate(plan):
        offsets = subsets(bits)[1:]
        groups = [[offset] for offset in offsets] if stage + 1 < last else [offsets]
        sources = {None: [0], **{name: patterns for name, (patterns, _) in units.items()}}
        for name, patterns in sources.items():
            for group in groups:
                for offset in group:
                    sems[stage, offset, name] = count
                if stage < last:
                    arriving = [offset + at for offset in group for at in patterns]
                    units[stage, tuple(group), name] = (arriving, count)
                    count += 1
    return units, sems, count + 1


def greet_stages(me, plan, barrier):
    for bits in plan:
        for offset in subsets(bits)[1:]:
            pl.semaphore_signal(
                barrier, inc=1, device_id=(move(me, offset, bits),), device_id_type=MESH
            )


def stage_partners(plan):
    return sum((1 << len(bits)) - 1 for bits in plan)


def greet(me, devices, barrier):
    @pl.loop(1, devices)
    def _(shift):
        pl.semaphore_signal(
            barrier, inc=1, device_id=((me + shift) % devices,), device_id_type=MESH
        )


def gather_kernel(devices, w_up, w_down, w_out, full_up, full_down, full_out, send_sem, recv_sem):
    me = lax.axis_index("dp")
    barrier = pltpu.get_barrier_semaphore()
    greet(me, devices, barrier)
    gather = Gather(me, devices, (full_up, full_down, full_out), send_sem, recv_sem)
    gather.fill((w_up, w_down, w_out))
    pl.semaphore_wait(barrier, devices - 1)
    gather.pass_on()
    for which in range(3):
        gather.arrive(which)
    gather.close()


def gather_weights(devices, w_up, w_down, w_out):
    shapes = []
    for shard, width in ((w_up, FF), (w_down, D), (w_out, VOCAB)):
        shapes.append(
            jax.ShapeDtypeStruct((devices, shard.size // width, width), jnp.bfloat16)
        )
    return pl.pallas_call(
        functools.partial(gather_kernel, devices),
        out_shape=shapes,
        in_specs=[VMEM] * 3,
        out_specs=[VMEM] * 3,
        scratch_shapes=[
            pltpu.SemaphoreType.DMA((3, devices)),
            pltpu.SemaphoreType.DMA((3, devices)),
        ],
        compiler_params=pltpu.CompilerParams(collective_id=0, has_side_effects=True),
        name="gather_weights",
    )(w_up, w_down, w_out)


def dot_rows(left, right):
    return jnp.dot(left, right, preferred_element_type=jnp.float32)


def dot_last(left, right, precision=None):
    return lax.dot_general(
        left, right, (((1,), (1,)), ((), ())), precision=precision,
        preferred_element_type=jnp.float32,
    )


def dot_first(left, right):
    return lax.dot_general(
        left, right, (((0,), (0,)), ((), ())), preferred_element_type=jnp.float32
    )


def row_blocks(total, body):
    block = min(256, total)
    for step in range(total // block):
        body(pl.ds(step * block, block))


def normalize(features, normalized):
    def body(rows):
        flat_in = features[rows, :].astype(jnp.float32)
        centre = jnp.mean(flat_in, axis=1, keepdims=True)
        shifted = flat_in - centre
        spread = jnp.mean(shifted * shifted, axis=1, keepdims=True)
        normalized[rows, :] = (shifted * lax.rsqrt(spread + 1e-05)).astype(jnp.bfloat16)

    row_blocks(features.shape[0], body)


def project_up(normalized, up_mat, slopes, hidden):
    def body(rows):
        act = dot_rows(normalized[rows, :], up_mat[...].reshape(D, FF))
        sigmoid = 1.0 / (1.0 + jnp.exp(-act))
        slopes[rows, :] = sigmoid * (1.0 + act * (1.0 - sigmoid))
        hidden[rows, :] = (act * sigmoid).astype(jnp.bfloat16)

    row_blocks(normalized.shape[0], body)


def project_down(features, hidden, down_mat, out_mat, block_out, log_probs):
    def body(rows):
        flat_in = features[rows, :].astype(jnp.float32)
        out_rows = (flat_in + 0.5 * dot_rows(hidden[rows, :], down_mat[...].reshape(FF, D))).astype(
            jnp.bfloat16
        )
        block_out[rows, :] = out_rows
        logits = dot_rows(out_rows, out_mat[...].reshape(D, VOCAB))
        top = jnp.max(logits, axis=1, keepdims=True)
        low = (logits - top) * LOG2E
        log_probs[rows, :] = low - jnp.log2(jnp.sum(jnp.exp2(low), axis=1, keepdims=True))

    row_blocks(features.shape[0], body)


def split_dot(dot, values, picks):
    high = values.astype(jnp.bfloat16)
    rest = values - high.astype(jnp.float32)
    middle = rest.astype(jnp.bfloat16)
    low = (rest - middle.astype(jnp.float32)).astype(jnp.bfloat16)
    return dot(high, picks) + (dot(middle, picks) + dot(low, picks))


def ctc_rows(frames):
    return [pltpu.VMEM((8 * frames, LANES), jnp.float32)] * 4 + [
        pltpu.VMEM((16 * frames, LANES), jnp.float32)
    ] * 4


class Lattice:
    def __init__(self, parts, sign, skip):
        self.parts, self.sign = parts, sign
        self.row = 0 if sign > 0 else 7
        self.skips = [self.spread(skip, part) > 0.5 for part in range(parts)]

    def spread(self, values, part):
        if self.sign > 0:
            return pltpu.roll(values, part, 1, stride=self.parts, stride_axis=0)
        shift = LANES - part - 7 * self.parts
        return pltpu.roll(values, shift, 1, stride=self.parts, stride_axis=0)

    def begin(self, blank, label):
        def whole(values):
            return jnp.broadcast_to(values[self.row : self.row + 1], (8, LANES))

        blank, label = whole(blank), whole(label)
        return tuple(
            [self.spread(blank, part) for part in range(self.parts)]
            + [self.spread(label, part) for part in range(self.parts + 1)]
        )

    def enter(self, moved):
        self.blank, self.label = list(moved[: self.parts]), list(moved[self.parts :])
        one = jnp.ones((8, LANES), jnp.float32)
        self.blank_mass, self.label_mass = [one] * self.parts, [one] * (self.parts + 1)

    def next_rows(self, values):
        return pltpu.roll(values, 7 if self.sign > 0 else 1, 0)

    def advance(self, emit_blank, emit_label, parts):
        blank, label, blank_mass, label_mass = [], [], [], []
        for part in range(parts):
            b, l, l1 = self.blank[part], self.label[part], self.label[part + 1]
            bm, lm, lm1 = self.blank_mass[part], self.label_mass[part], self.label_mass[part + 1]
            top = jnp.maximum(b, l1)
            mass = bm * jnp.exp2(b - top) + lm1 * jnp.exp2(l1 - top)
            above = jnp.where(self.skips[part], top, b)
            above_mass = jnp.where(self.skips[part], mass, bm)
            peak = jnp.maximum(l, above)
            peak_mass = lm * jnp.exp2(l - peak) + above_mass * jnp.exp2(above - peak)
            if part == 0:
                result = (top, mass, peak, peak_mass)
            blank.append(top + emit_blank)
            label.append(peak + self.spread(emit_label, part))
            blank_mass.append(mass)
            label_mass.append(peak_mass)
        if parts == self.parts:
            label.append(self.next_rows(label[0]))
            label_mass.append(self.next_rows(label_mass[0]))
        self.blank, self.label = blank, label
        self.blank_mass, self.label_mass = blank_mass, label_mass
        return result


def ctc_grad(
    loss_scale,
    frame_lens,
    label_lens,
    labels,
    log_probs,
    emitted,
    emitted_blank,
    alpha_rows,
    beta_rows,
    logit_grad,
):
    utterances, label_count = labels.shape
    frames = log_probs.shape[0] // utterances
    half = LANES // utterances
    depth = 8 * PARTS
    assert label_count + depth <= half and frames % depth == 0

    lane_row = lax.broadcasted_iota(jnp.int32, (8, LANES), 1)
    label_ids = lax.broadcasted_iota(jnp.int32, (label_count, LANES), 0)
    spread_lanes = lax.broadcasted_iota(jnp.int32, (label_count, LANES), 1)
    label_rows = jnp.concatenate(
        [
            labels[...].astype(jnp.float32),
            jnp.zeros((8 - utterances, label_count), jnp.float32),
        ],
        axis=0,
    ).astype(jnp.bfloat16)
    extended = jnp.zeros((8, LANES), jnp.float32)
    for utterance in range(utterances):
        spread = (spread_lanes == label_ids + half * utterance + 1).astype(jnp.bfloat16)
        placed = dot_rows(label_rows, spread)[utterance : utterance + 1]
        extended = extended + jnp.broadcast_to(placed, (8, LANES))
    skip = jnp.where(extended != pltpu.roll(extended, 1, 1), 1.0, 0.0)
    skip_back = pltpu.roll(skip, LANES - 1, 1)

    vocab_ids = lax.broadcasted_iota(jnp.int32, (VOCAB, LANES), 0).astype(jnp.float32)
    vocab_lanes = lax.broadcasted_iota(jnp.int32, (VOCAB, LANES), 1)
    frame_lanes = lax.broadcasted_iota(jnp.int32, (frames, LANES), 1)
    onehots = []
    picked = None
    blanks = None
    for utterance in range(utterances):
        rows = slice(utterance * frames, (utterance + 1) * frames)
        first = half * utterance + 1
        mine = (vocab_lanes >= first) & (vocab_lanes < first + label_count)
        onehot = jnp.where((vocab_ids == extended[0:1, :]) & mine, 1.0, 0.0).astype(jnp.bfloat16)
        onehots.append(onehot)
        picks = split_dot(dot_rows, log_probs[rows, :], onehot)
        blank = jnp.broadcast_to(log_probs[rows, 0:1], (frames, LANES))
        if utterance == 0:
            picked, blanks = picks, blank
        else:
            picked = jnp.where(frame_lanes < half * utterance, picked, picks)
            blanks = jnp.where(frame_lanes < half * utterance, blanks, blank)
    place = frame_lanes % half
    emitted[...] = jnp.where((place >= 1) & (place <= label_count), picked, negative)
    emitted_blank[...] = blanks

    forward = Lattice(PARTS, 1, skip)
    backward = Lattice(PARTS, -1, skip_back)
    start = jnp.full((8, LANES), negative, jnp.float32)
    start_back = start
    for utterance in range(utterances):
        first = half * utterance + 1
        start = jnp.where(lane_row == first, 0.0, start)
        start_back = jnp.where(
            lane_row == first + label_lens[utterance] - 1, 0.0, start_back
        )
    nothing = jnp.full((8, LANES), negative, jnp.float32)

    def tile(frame):
        return pl.ds(pl.multiple_of(frame * 8, 8), 8)

    def row_of(ref, frame):
        return jnp.broadcast_to(ref[pl.ds(frame, 1), :], (8, LANES))

    def leave(lattice):
        return (
            lattice.blank[0] + jnp.log2(lattice.blank_mass[0]),
            lattice.label[0] + jnp.log2(lattice.label_mass[0]),
        )

    def step_back(at, level):
        frame = at * depth + level
        emit = emit_blank = None
        for utterance in range(utterances):
            back = jnp.maximum(frame_lens[utterance] - 1 - frame, 0)
            mine, mine_blank = row_of(emitted, back), row_of(emitted_blank, back)
            if utterance == 0:
                emit, emit_blank = mine, mine_blank
            else:
                emit = jnp.where(lane_row < half * utterance, emit, mine)
                emit_blank = jnp.where(lane_row < half * utterance, emit_blank, mine_blank)
        result = backward.advance(emit_blank, emit, min(PARTS, depth - level))
        for ref, value in zip(beta_rows, result):
            ref[tile(frames - 1 - frame), :] = value

    def step_ahead(at, level):
        frame = at * depth + level
        result = forward.advance(
            row_of(emitted_blank, frame), row_of(emitted, frame), min(PARTS, depth - level)
        )
        for ref, value in zip(alpha_rows, result):
            ref[tile(frame), :] = value

    def block(at, carry):
        forward.enter(forward.begin(*carry[:2]))
        backward.enter(backward.begin(*carry[2:]))
        for level in range(depth):
            step_ahead(at, level)
            step_back(at, level)
        return leave(forward) + leave(backward)

    lax.fori_loop(
        0, frames // depth, block, (start, nothing, start_back, nothing)
    )

    frame_ids = lax.broadcasted_iota(jnp.int32, (frames, LANES), 0)
    alphas = [ref[pl.ds(forward.row, frames, stride=8), :] for ref in alpha_rows]
    betas, alive = [], None
    for ref in beta_rows:
        value = None
        for utterance in range(utterances):
            first = 8 * (frames - frame_lens[utterance]) + backward.row
            mine = ref[pl.ds(first, frames, stride=8), :]
            value = mine if value is None else jnp.where(frame_lanes < half * utterance, value, mine)
        betas.append(value)
    betas[0], betas[1] = pltpu.roll(betas[0], 1, 1), pltpu.roll(betas[1], 1, 1)
    joint_blank = alphas[0] + emitted_blank[...] + betas[0]
    joint_label = alphas[2] + emitted[...] + betas[2]
    blank_mass, label_mass = alphas[1] * betas[1], alphas[3] * betas[3]
    both = jnp.maximum(joint_blank, joint_label)
    for utterance in range(utterances):
        rows = slice(utterance * frames, (utterance + 1) * frames)
        first = half * utterance
        mine = (frame_lanes >= first) & (frame_lanes < first + half)
        top = jnp.max(jnp.where(mine, both, negative), axis=1, keepdims=True)
        live = mine & (frame_ids < frame_lens[utterance])
        label = jnp.where(live, label_mass * jnp.exp2(joint_label - top), 0.0)
        blank = jnp.where(live, blank_mass * jnp.exp2(joint_blank - top), 0.0)
        blank_sum = jnp.sum(blank, axis=1, keepdims=True)
        total = jnp.sum(label, axis=1, keepdims=True) + blank_sum
        kept = frame_ids[:, 0:1] < frame_lens[utterance]
        scale = jnp.where(kept, 1.0 / jnp.where(kept, total, 1.0), 0.0)
        gamma = split_dot(dot_last, label * scale, onehots[utterance])
        vocab_at = lax.broadcasted_iota(jnp.int32, (frames, VOCAB), 1)
        gamma = gamma + jnp.where(vocab_at == 0, blank_sum * scale, 0.0)
        probs = jnp.exp2(log_probs[rows, :]) * jnp.where(kept, 1.0, 0.0)
        logit_grad[rows, :] = (loss_scale * (probs - gamma)).astype(jnp.bfloat16)


def grad_ff(logit_grad, out_mat, ff_grad):
    def body(rows):
        ff_grad[rows, :] = (
            0.5 * dot_last(logit_grad[rows, :], out_mat[...].reshape(D, VOCAB))
        ).astype(jnp.bfloat16)

    row_blocks(logit_grad.shape[0], body)


def grad_act(ff_grad, down_mat, slopes, act_grad):
    def body(rows):
        act_grad[rows, :] = (
            dot_last(ff_grad[rows, :], down_mat[...].reshape(FF, D)) * slopes[rows, :]
        ).astype(jnp.bfloat16)

    row_blocks(ff_grad.shape[0], body)


def step_kernel(
    loss_scale,
    frame_lens,
    label_lens,
    features,
    labels,
    up_mat,
    down_mat,
    out_mat,
    grad_up,
    grad_down,
    grad_out,
    normalized,
    slopes,
    hidden,
    block_out,
    log_probs,
    logit_grad,
    ff_grad,
    act_grad,
    emitted,
    emitted_blank,
    *lattice_rows,
):
    normalize(features, normalized)
    project_up(normalized, up_mat, slopes, hidden)
    project_down(features, hidden, down_mat, out_mat, block_out, log_probs)
    ctc_grad(
        loss_scale, frame_lens, label_lens, labels, log_probs, emitted, emitted_blank,
        lattice_rows[:4], lattice_rows[4:], logit_grad,
    )
    grad_ff(logit_grad, out_mat, ff_grad)
    grad_act(ff_grad, down_mat, slopes, act_grad)
    grad_up[...] = dot_first(normalized[...], act_grad[...])
    grad_down[...] = dot_first(hidden[...], ff_grad[...])
    grad_out[...] = dot_first(block_out[...], logit_grad[...])


def step_scratch(total, frames):
    return [
        pltpu.VMEM((total, D), jnp.bfloat16),
        pltpu.VMEM((total, FF), jnp.float32),
        pltpu.VMEM((total, FF), jnp.bfloat16),
        pltpu.VMEM((total, D), jnp.bfloat16),
        pltpu.VMEM((total, VOCAB), jnp.float32),
        pltpu.VMEM((total, VOCAB), jnp.bfloat16),
        pltpu.VMEM((total, D), jnp.bfloat16),
        pltpu.VMEM((total, FF), jnp.bfloat16),
        pltpu.VMEM((frames, LANES), jnp.float32),
        pltpu.VMEM((frames, LANES), jnp.float32),
    ] + ctc_rows(frames)


def local_step(loss_scale, frame_lens, label_lens, features, labels, up_mat, down_mat, out_mat):
    total = features.shape[0]
    frames = total // labels.shape[0]
    return pl.pallas_call(
        functools.partial(step_kernel, loss_scale),
        out_shape=[
            jax.ShapeDtypeStruct((D, FF), jnp.float32),
            jax.ShapeDtypeStruct((FF, D), jnp.float32),
            jax.ShapeDtypeStruct((D, VOCAB), jnp.float32),
        ],
        in_specs=[SMEM, SMEM] + [VMEM] * 5,
        out_specs=[VMEM] * 3,
        scratch_shapes=step_scratch(total, frames),
        compiler_params=pltpu.CompilerParams(vmem_limit_bytes=40 << 20),
        name="local_step",
    )(frame_lens, label_lens, features, labels, up_mat, down_mat, out_mat)


class Sum:
    def __init__(self, me, devices, grads, received, staged, send_sem, recv_sem):
        self.me, self.grads, self.received, self.staged = me, grads, received, staged
        self.send_sem, self.recv_sem = send_sem, recv_sem
        self.orders = [order[::-1] for order in bit_orders(devices)]
        self.steps = len(self.orders[0])
        self.copies = [{}, {}, {}]

    def sum_of(self, which, place, pattern, stage):
        value = self.grads[which][place]
        for bit in self.orders[which][:stage]:
            self.copies[which][pattern + bit].wait_recv()
            value = value + self.received[which][pattern + bit]
        return value

    def send(self, which, stage):
        order = self.orders[which]
        for offset in subsets(order[stage + 1 :][::-1])[::-1]:
            slot = offset + order[stage]
            place = place_with(self.me, order, slot)
            if stage == 0:
                source = self.grads[which].at[place]
            else:
                self.staged[which][slot] = self.sum_of(which, place, slot, stage)
                source = self.staged[which].at[slot]
            copy = pltpu.make_async_remote_copy(
                src_ref=source,
                dst_ref=self.received[which].at[slot],
                send_sem=self.send_sem.at[which, slot],
                recv_sem=self.recv_sem.at[which, slot],
                device_id=(flip(self.me, order[stage]),),
                device_id_type=MESH,
            )
            copy.start()
            self.copies[which][slot] = copy

    def finish(self, devices, reduced, squares, own_squares, small_send, small_recv):
        me = self.me
        own = jnp.zeros((1, LANES), jnp.float32)
        for which in (2, 1, 0):
            value = self.sum_of(which, me, 0, self.steps)
            rows, width = value.shape
            parts = width // LANES
            for part in range(parts):
                piece = value[:, part * LANES : (part + 1) * LANES]
                reduced[which][pl.ds(part, rows, stride=parts), :] = piece
                own = own + jnp.sum(piece * piece, axis=0, keepdims=True)
        own_squares[...] = own
        squares[0] = own

        def small_copy(shift):
            return pltpu.make_async_remote_copy(
                src_ref=own_squares,
                dst_ref=squares.at[shift],
                send_sem=small_send.at[shift],
                recv_sem=small_recv.at[shift],
                device_id=((me + shift) % devices,),
                device_id_type=MESH,
            )

        @pl.loop(1, devices)
        def _(shift):
            small_copy(shift).start()

        for copies in self.copies:
            for copy in copies.values():
                copy.wait_send()

        @pl.loop(1, devices)
        def _(shift):
            small_copy(shift).wait()


def sum_pieces(plan):
    pieces = {}
    for stage in range(len(plan)):
        for after in subsets(plan[stage + 1]) if stage + 1 < len(plan) else [0]:
            pieces[stage, after] = len(pieces)
    return pieces


def far_first(offset, bits):
    core, near, far = bits[:1], bits[1:3], bits[3:]
    weights = [1] * len(core) + [3] * len(near) + [3 << at for at in range(len(far))]
    return sum(weight for weight, bit in zip(weights, bits) if offset & bit)


class StagedSum:
    def __init__(self, me, plans, narrow, grads, received, staged, send_sem, recv_sem):
        self.me, self.plans, self.narrow = me, plans, narrow
        self.grads, self.received, self.staged = grads, received, staged
        self.send_sem, self.recv_sem = send_sem, recv_sem
        self.pieces = [sum_pieces(plan) for plan in plans]
        self.seen = set()

    def index(self, which, pattern):
        bits = flat(self.plans[which])
        return sum(1 << at for at, bit in enumerate(bits[::-1]) if pattern & bit)

    def wide(self, which, stage):
        return 3 * (stage in self.narrow[which]) + which

    def put(self, which, value):
        bits = flat(self.plans[which])[::-1]
        blocks, rows, width = self.grads[which].shape
        own = [(self.me // bit) % 2 for bit in bits]
        for block in range(blocks):
            slot = 0
            for at, bit in enumerate(bits):
                slot = slot + (1 << at) * (1 - own[at] if block & bit else own[at])
            self.grads[which][slot] = value[block * rows : (block + 1) * rows, :]

    def copy(self, which, name):
        stage, offset, after = name
        start = self.index(which, offset + after)
        blocks = pl.ds(start, 1 << len(flat(self.plans[which][stage + 2 :])))
        at = self.wide(which, stage)
        source = self.grads[which] if stage == 0 else self.staged[at]
        return pltpu.make_async_remote_copy(
            src_ref=source.at[blocks],
            dst_ref=self.received[at].at[blocks],
            send_sem=self.send_sem.at[at],
            recv_sem=self.recv_sem.at[which, self.pieces[which][stage, after]],
            device_id=(move(self.me, offset, self.plans[which][stage]),),
            device_id_type=MESH,
        )

    def wait(self, which, stage, after):
        plan = self.plans[which]
        blocks = ((1 << len(plan[stage])) - 1) << len(flat(plan[stage + 2 :]))
        at = self.wide(which, stage)
        drain(
            self.received[at], blocks, self.send_sem.at[at],
            self.recv_sem.at[which, self.pieces[which][stage, after]], flip(self.me, 1),
        ).wait_recv()

    def sum_of(self, which, pattern, stage):
        value = self.grads[which][self.index(which, pattern)]
        for earlier in range(stage):
            after = 0
            if earlier + 1 < len(self.plans[which]):
                after = sum(bit for bit in self.plans[which][earlier + 1] if pattern & bit)
            if (which, earlier, after) not in self.seen:
                self.seen.add((which, earlier, after))
                self.wait(which, earlier, after)
            for offset in subsets(self.plans[which][earlier])[1:]:
                slot = self.index(which, pattern + offset)
                value = value + self.received[self.wide(which, earlier)][slot].astype(jnp.float32)
        return value

    def send(self, which, stage):
        plan = self.plans[which]
        afters = subsets(plan[stage + 1])[::-1] if stage + 1 < len(plan) else [0]
        for after in afters:
            for offset in subsets(plan[stage])[1:][::-1]:
                if stage:
                    staged = self.staged[self.wide(which, stage)]
                    for later in subsets(flat(plan[stage + 2 :])):
                        pattern = offset + after + later
                        staged[self.index(which, pattern)] = self.sum_of(
                            which, pattern, stage
                        ).astype(staged.dtype)
                self.copy(which, (stage, offset, after)).start()

    def finish(self, devices, reduced, squares, own_squares, small_send, small_recv):
        me = self.me
        own = jnp.zeros((8, LANES), jnp.float32)
        values = {}
        for which in (2, 1, 0):
            value = self.sum_of(which, 0, len(self.plans[which]))
            values[which] = value
            rows, width = value.shape
            for row in range(0, rows, 8):
                for lane in range(0, width, LANES):
                    piece = value[row : row + 8, lane : lane + LANES]
                    own = own + piece * piece
        own = jnp.sum(own, axis=0, keepdims=True)
        own_squares[...] = own
        squares[0] = own

        bits = [1 << k for k in range(devices.bit_length() - 1)]
        for offset in sorted(subsets(bits)[1:], key=lambda at: -far_first(at, bits)):
            pltpu.make_async_remote_copy(
                src_ref=own_squares,
                dst_ref=squares.at[offset],
                send_sem=small_send,
                recv_sem=small_recv,
                device_id=(move(me, offset, bits),),
                device_id_type=MESH,
            ).start()

        for which, value in values.items():
            rows, width = value.shape
            parts = width // LANES
            for part in range(parts):
                reduced[which][pl.ds(part, rows, stride=parts), :] = value[
                    :, part * LANES : (part + 1) * LANES
                ]

        for which, plan in enumerate(self.plans):
            sent = {}
            for stage, bits in enumerate(plan):
                blocks = ((1 << len(bits)) - 1) << len(flat(plan[stage + 1 :]))
                at = self.wide(which, stage)
                sent[at] = sent.get(at, 0) + blocks
            for at, blocks in sent.items():
                drain(
                    self.received[at], blocks, self.send_sem.at[at], self.recv_sem.at[which, 0],
                    flip(me, 1),
                ).wait_send()
        small = drain(squares, devices - 1, small_send, small_recv, flip(me, 1))
        small.wait_send()
        small.wait_recv()


def sum_kernel(devices, *refs):
    grads, reduced, squares = refs[:3], refs[3:6], refs[6]
    received, staged = refs[7:10], refs[10:13]
    own_squares, send_sem, recv_sem, small_send, small_recv = refs[13:]
    me = lax.axis_index("dp")
    barrier = pltpu.get_barrier_semaphore()
    greet(me, devices, barrier)
    pl.semaphore_wait(barrier, devices - 1)
    total = Sum(me, devices, grads, received, staged, send_sem, recv_sem)
    for stage in range(total.steps):
        for which in range(3):
            total.send(which, stage)
    total.finish(devices, reduced, squares, own_squares, small_send, small_recv)


def exchange_plans(devices):
    bits = [1 << k for k in range(devices.bit_length() - 1)]
    core, near, far = bits[:1], bits[1:3], bits[3:]
    gathers = ([far, near, core], [far, near, core], [near, far, core])
    sums = ([core, near, far], [core, near, far], [core, far, near])
    narrow = ((1, 2), (1,), (1,))
    return gathers, sums, narrow


def meet_plan(devices):
    bits = [1 << k for k in range(devices.bit_length() - 1)]
    core, near, far = bits[:1], bits[1:3], bits[3:]
    return [core, near, far]


def fused_kernel(devices, loss_scale, *refs):
    frame_lens, label_lens, features, labels = refs[:4]
    shards, reduced, squares = refs[4:7], refs[7:10], refs[10]
    fulls, grads, received, staged = refs[11:14], refs[14:17], refs[17:23], refs[23:29]
    gather_send, gather_recv, own_squares, send_sem, recv_sem, small_send, small_recv = refs[29:36]
    normalized, slopes, hidden, block_out, log_probs = refs[36:41]
    logit_grad, ff_grad, act_grad, emitted, emitted_blank = refs[41:46]
    alpha_rows, beta_rows = refs[46:50], refs[50:54]
    held, load_sem = refs[54:58], refs[58]
    up_mat, down_mat, out_mat = fulls
    me = lax.axis_index("dp")
    loads = [
        pltpu.make_async_copy(source, target, load_sem.at[at])
        for at, (source, target) in enumerate(zip((*shards, features), held))
    ]
    for load in loads:
        load.start()
    shards, features = held[:3], held[3]
    barrier = pltpu.get_barrier_semaphore()
    gathers, sums, narrow = exchange_plans(devices)
    greet_stages(me, meet_plan(devices), barrier)
    gather = StagedGather(me, gathers, fulls, gather_send, gather_recv)
    for load in loads[:3]:
        load.wait()
    gather.fill(shards)
    loads[3].wait()
    normalize(features, normalized)
    pl.semaphore_wait(barrier, stage_partners(meet_plan(devices)))
    gather.pass_on()
    gather.arrive(0)
    project_up(normalized, up_mat, slopes, hidden)
    gather.arrive(1)
    gather.arrive(2)
    project_down(features, hidden, down_mat, out_mat, block_out, log_probs)
    ctc_grad(
        loss_scale, frame_lens, label_lens, labels, log_probs, emitted, emitted_blank, alpha_rows,
        beta_rows, logit_grad,
    )
    total = StagedSum(me, sums, narrow, grads, received, staged, send_sem, recv_sem)
    pending = [list(range(len(plan))) for plan in sums]

    def advance(*whiches):
        for which in whiches:
            if pending[which]:
                total.send(which, pending[which].pop(0))

    grad_ff(logit_grad, out_mat, ff_grad)
    total.put(1, dot_first(hidden[...], ff_grad[...]))
    advance(1)
    grad_act(ff_grad, down_mat, slopes, act_grad)
    advance(1)
    total.put(2, dot_first(block_out[...], logit_grad[...]))
    advance(2)
    total.put(0, dot_first(normalized[...], act_grad[...]))
    advance(0)
    advance(2, 0, 1, 0, 2)
    total.finish(devices, reduced, squares, own_squares, small_send, small_recv)
    gather.close()


def fused_step(loss_scale, devices, frame_lens, label_lens, features, labels, weights):
    total = features.shape[0]
    frames = total // labels.shape[0]
    blocks = [
        (devices, weight.size // width, width)
        for weight, width in zip(weights, (FF, D, VOCAB))
    ]
    gathers, sums, _ = exchange_plans(devices)
    wide = [pltpu.VMEM(block, jnp.float32) for block in blocks]
    both = wide + [pltpu.VMEM(block, jnp.bfloat16) for block in blocks]
    return pl.pallas_call(
        functools.partial(fused_kernel, devices, loss_scale),
        out_shape=[jax.ShapeDtypeStruct(weight.shape, jnp.float32) for weight in weights]
        + [jax.ShapeDtypeStruct((devices, 1, LANES), jnp.float32)],
        in_specs=[SMEM, SMEM, HBM, VMEM] + [HBM] * 3,
        out_specs=[VMEM] * 4,
        scratch_shapes=[pltpu.VMEM(block, jnp.bfloat16) for block in blocks]
        + wide
        + both * 2
        + [
            pltpu.SemaphoreType.DMA((3,)),
            pltpu.SemaphoreType.DMA((3, max(gather_units(plan)[2] for plan in gathers))),
            pltpu.VMEM((1, LANES), jnp.float32),
            pltpu.SemaphoreType.DMA((6,)),
            pltpu.SemaphoreType.DMA((3, max(len(sum_pieces(plan)) for plan in sums))),
            pltpu.SemaphoreType.DMA,
            pltpu.SemaphoreType.DMA,
        ]
        + step_scratch(total, frames)
        + [pltpu.VMEM(array.shape, array.dtype) for array in (*weights, features)]
        + [pltpu.SemaphoreType.DMA((4,))],
        compiler_params=pltpu.CompilerParams(
            collective_id=2, has_side_effects=True, vmem_limit_bytes=34 << 20
        ),
        name="fused_step",
    )(*(pltpu.with_memory_space_constraint(array, pltpu.HBM) for array in (frame_lens, label_lens, features, labels, *weights)))


def sum_gradients(devices, grads):
    blocks = [grad.reshape(devices, grad.shape[0] // devices, grad.shape[1]) for grad in grads]
    shapes = [
        jax.ShapeDtypeStruct((block[0].size // LANES, LANES), jnp.float32) for block in blocks
    ]
    buffers = [pltpu.VMEM(block.shape, jnp.float32) for block in blocks]
    return pl.pallas_call(
        functools.partial(sum_kernel, devices),
        out_shape=shapes + [jax.ShapeDtypeStruct((devices, 1, LANES), jnp.float32)],
        in_specs=[VMEM] * 3,
        out_specs=[VMEM] * 4,
        scratch_shapes=buffers
        + buffers
        + [
            pltpu.VMEM((1, LANES), jnp.float32),
            pltpu.SemaphoreType.DMA((3, devices)),
            pltpu.SemaphoreType.DMA((3, devices)),
            pltpu.SemaphoreType.DMA((devices,)),
            pltpu.SemaphoreType.DMA((devices,)),
        ],
        compiler_params=pltpu.CompilerParams(
            collective_id=1, has_side_effects=True, vmem_limit_bytes=50 << 20
        ),
        name="sum_gradients",
    )(*blocks)


def adam_kernel(squares, *refs):
    weights, firsts, seconds, grads, outs = (refs[at : at + 3] for at in (0, 3, 6, 9, 12))
    new_firsts, new_seconds = refs[15:18], refs[18:21]
    total = jnp.sum(squares[...])
    clip = 1.0 / jnp.maximum(jnp.sqrt(jnp.full((1, LANES), total)), 1.0)
    for which in range(3):
        scaled = clip * grads[which][...]
        first = 0.9 * firsts[which][...] + 0.1 * scaled
        second = 0.999 * seconds[which][...] + 0.001 * scaled * scaled
        ratio = first / first_correction / (jnp.sqrt(second / second_correction) + 1e-08)
        outs[which][...] = weights[which][...] - 0.001 * ratio
        new_firsts[which][...] = first
        new_seconds[which][...] = second


def adam(squares, weights, firsts, seconds, grads):
    shapes = [jax.ShapeDtypeStruct(weight.shape, jnp.float32) for weight in weights]
    return pl.pallas_call(
        adam_kernel,
        out_shape=shapes * 3,
        in_specs=[VMEM] * 13,
        out_specs=[VMEM] * 9,
        compiler_params=pltpu.CompilerParams(vmem_limit_bytes=4 << 20),
        name="adam",
    )(squares, *weights, *firsts, *seconds, *grads)


def per_device(
    features,
    frame_lens,
    labels,
    label_lens,
    w_up,
    w_down,
    w_out,
    first_up,
    first_down,
    first_out,
    second_up,
    second_down,
    second_out,
):
    devices = lax.axis_size("dp")
    batch, frames, width = features.shape

    def lined(*arrays):
        return [array.reshape(array.shape[0] // LANES, LANES) for array in arrays]

    weights = lined(w_up, w_down, w_out)
    loss_scale = 1.0 / (batch * devices)
    rows_in = features.reshape(batch * frames, width)
    if w_up.size % (8 * FF) == 0 and w_out.size % (8 * VOCAB) == 0:
        *shares, squares = fused_step(
            loss_scale, devices, frame_lens, label_lens, rows_in, labels, weights
        )
    else:
        full_up, full_down, full_out = gather_weights(devices, *weights)
        grads = local_step(
            loss_scale,
            frame_lens,
            label_lens,
            rows_in,
            labels,
            full_up.reshape(D, FF),
            full_down.reshape(FF, D),
            full_out.reshape(D, VOCAB),
        )
        *shares, squares = sum_gradients(devices, grads)
    results = adam(
        squares,
        weights,
        lined(first_up, first_down, first_out),
        lined(second_up, second_down, second_out),
        shares,
    )
    return tuple(result.reshape(-1) for result in results)


def solution(mesh):
    flat = P("dp")
    return jax.shard_map(
        per_device,
        mesh=mesh,
        in_specs=(P("dp", None, None), flat, P("dp", None), flat) + (flat,) * 9,
        out_specs=(flat,) * 9,
        check_vma=False,
    )
```
